64 devices in a mesh: dp: 4 (over x, y), ep: 16 (over z, core).
Axes of the slice: x: 2, y: 2, z: 8, core: 2. Of those that a mesh axis runs over, the one named last changes fastest.
The devices are a block of a 4x4x8 slice.
Arguments:
- x_rows: bfloat16 [32768, 768], P(('dp', 'ep')), parts along dimension 0
- logits: float32 [32768, 64], P(('dp', 'ep')), parts along dimension 0
- w_in: bfloat16 [64, 768, 3072], P('ep')
- w_out: bfloat16 [64, 3072, 768], P('ep')
Outputs:
- output: bfloat16 [32768, 768], P(('dp', 'ep')), parts along dimension 0
There are 4 independent parts. The reference program is written for one: setup_inputs(seed, part) draws one part's arguments, and reference() takes and returns one part's arrays. A program takes and returns all parts, laid end to end along the dimension named above; an argument that names none is the same for every part.
All inputs are finite; a program needn't handle non-finite values.
Results may differ from the reference program's by a relative error of at most 0.001.
Values are sent between devices in bfloat16 or wider.
A program may use at most 768 MiB of HBM per device.

```python
import math
import jax
import jax.numpy as jnp
from jax import lax

TOKENS = 8192
D_MODEL = 768
FF_HIDDEN = 3072
EXPERTS = 64
CAPACITY = 256
GROUP_DEV = 16
LOGIT_SHIFT = int(1024 * math.log(EXPERTS))


def draw_logits(route_key):
    sub_keys = jax.random.split(route_key, 5)
    tok_dev = TOKENS // GROUP_DEV
    mean_cnt = 2 * tok_dev // EXPERTS
    quarter = EXPERTS // 4
    exp_order = jax.random.permutation(sub_keys[0], EXPERTS)
    rot_bits = jax.random.randint(sub_keys[1], (GROUP_DEV,), 0, 2)
    tier_vals = jnp.array([2 * mean_cnt, mean_cnt, mean_cnt // 2, mean_cnt // 2], dtype=jnp.int32)
    tier_idx = (jnp.arange(EXPERTS)[None, :] // quarter + rot_bits[:, None]) % 4
    slot_ends = jnp.cumsum(tier_vals[tier_idx], axis=1)
    slot_ids = jnp.arange(2 * tok_dev)
    rank_pos = jnp.sum((slot_ends[:, None, :] <= slot_ids[None, :, None]).astype(jnp.int32), axis=2)
    pick_list = exp_order[rank_pos]
    perm_keys = jax.random.split(sub_keys[2], GROUP_DEV)
    tok_perm = jax.vmap(lambda perm_key: jax.random.permutation(perm_key, tok_dev))(perm_keys)
    first_pick = jnp.take_along_axis(pick_list[:, :tok_dev], tok_perm, axis=1).reshape(TOKENS)
    second_pick = jnp.take_along_axis(pick_list[:, tok_dev:], tok_perm, axis=1).reshape(TOKENS)
    expert_ids = jnp.arange(EXPERTS)
    chosen = (expert_ids[None, :] == first_pick[:, None]) | (expert_ids[None, :] == second_pick[:, None])
    base_val = jax.random.randint(sub_keys[3], (TOKENS, EXPERTS), 0, 2048)
    pick_val = jax.random.randint(sub_keys[4], (TOKENS, EXPERTS), 1024, 3072) + LOGIT_SHIFT
    score_int = jnp.where(chosen, pick_val, base_val) * EXPERTS + expert_ids[None, :]
    return score_int.astype(jnp.float32) / (1024.0 * EXPERTS)


def setup_inputs(seed: int = 0, part: int = 0) -> dict:
    part_key = jax.random.fold_in(jax.random.key(seed), part)
    sub_keys = jax.random.split(part_key, 2)
    w_keys = jax.random.split(jax.random.key(seed + 1), 2)
    x_rows = jax.random.normal(sub_keys[0], (TOKENS, D_MODEL), jnp.float32).astype(jnp.bfloat16)
    logits = draw_logits(sub_keys[1])
    w_in = (jax.random.normal(w_keys[0], (EXPERTS, D_MODEL, FF_HIDDEN), jnp.float32) * D_MODEL ** -0.5).astype(jnp.bfloat16)
    w_out = (jax.random.normal(w_keys[1], (EXPERTS, FF_HIDDEN, D_MODEL), jnp.float32) * (2.0 * FF_HIDDEN ** -0.5)).astype(jnp.bfloat16)
    return {'x_rows': x_rows, 'logits': logits, 'w_in': w_in, 'w_out': w_out}


def reference(x_rows, logits, w_in, w_out):
    gate_probs = jax.nn.softmax(logits, axis=-1)
    top_vals, top_ids = lax.top_k(logits, 2)
    chosen = (logits >= top_vals[:, 1:2]).astype(jnp.int32)
    before = jnp.cumsum(chosen, axis=0) - chosen
    pick_pos = jnp.take_along_axis(before, top_ids, axis=1)
    dest_row = jnp.where(pick_pos < CAPACITY, top_ids * CAPACITY + pick_pos, EXPERTS * CAPACITY)
    tok_ids = jnp.broadcast_to(jnp.arange(TOKENS, dtype=jnp.int32)[:, None], (TOKENS, 2))
    slot_tok = jnp.full((EXPERTS * CAPACITY,), TOKENS, jnp.int32).at[dest_row.reshape(-1)].set(tok_ids.reshape(-1), mode='drop')
    expert_rows = jnp.take(x_rows, slot_tok, axis=0, mode='fill', fill_value=0).reshape(EXPERTS, CAPACITY, D_MODEL)

    def expert_ffn(operands):
        rows_in, w_first, w_second = operands
        hidden = jax.nn.gelu(jnp.dot(rows_in, w_first, preferred_element_type=jnp.float32), approximate=True).astype(jnp.bfloat16)
        return jnp.dot(hidden, w_second, preferred_element_type=jnp.float32).astype(jnp.bfloat16)

    expert_out = lax.map(expert_ffn, (expert_rows, w_in, w_out)).reshape(EXPERTS * CAPACITY, D_MODEL)
    rows_back = jnp.take(expert_out, dest_row, axis=0, mode='fill', fill_value=0)
    pick_gate = jnp.take_along_axis(gate_probs, top_ids, axis=1)
    mix_sum = jnp.sum(pick_gate[:, :, None] * rows_back.astype(jnp.float32), axis=1)
    return (x_rows.astype(jnp.float32) + mix_sum).astype(jnp.bfloat16)
```

```python
import functools

import jax
import jax.numpy as jnp
from jax import lax
from jax.experimental import pallas as pl
from jax.experimental.pallas import tpu as pltpu
from jax.sharding import PartitionSpec as P

CAP_FACTOR = 2
HOP_ROWS = (512, 512, 512, 512)
FF_TILE = 512
BF = jnp.bfloat16
F32 = jnp.float32
MESH = pl.DeviceIdType.MESH


def top_two(vals, axis):
    best = jnp.max(vals, axis=axis, keepdims=True)
    first = vals == best
    rest = jnp.where(first, -jnp.inf, vals)
    runner = jnp.max(rest, axis=axis, keepdims=True)
    return best, runner, first, rest == runner


def as_one(mask):
    return jnp.where(mask, 1.0, 0.0)


def iota_f(shape, dim):
    return lax.broadcasted_iota(jnp.int32, shape, dim).astype(F32)


def dot(lhs, rhs):
    return jnp.dot(lhs, rhs, preferred_element_type=F32)


def moe_kernel(n_ep, n_dp, capacity, src_cap, x_ref, lg_ref, w1_hbm, w2_hbm, out_ref, flag_ref,
               w1_buf, w2_buf, blk, ring, mirror, px, meta_send, metas, acc, z_acc, skey, rkeys,
               ret, back, y_acc, flag_buf,
               w_sem, send_sem, recv_sem, mir_send, mir_recv, px_sem, meta_ssem, meta_rsem,
               ret_ssem, ret_rsem, flag_ssem, flag_rsem):
    tok, d_model = x_ref.shape
    experts = lg_ref.shape[1]
    exp_dev = experts // n_ep
    ff = w1_buf.shape[2]
    n_chip = n_ep // 2
    half = n_chip // 2
    me = lax.axis_index('ep')
    my_dp = lax.axis_index('dp')
    chip = lax.div(me, 2)
    core = lax.rem(me, 2)
    other = chip * 2 + 1 - core
    nxt = (lax.rem(chip + 1, n_chip) * 2 + core, lax.rem(chip + n_chip - 1, n_chip) * 2 + core)
    bounds = (0,) + HOP_ROWS[::-1]
    starts = [sum(HOP_ROWS[:h]) for h in range(half)]

    def weight_copies(el):
        slot = el % 2
        return (pltpu.make_async_copy(w1_hbm.at[el], w1_buf.at[slot], w_sem.at[slot, 0]),
                pltpu.make_async_copy(w2_hbm.at[el], w2_buf.at[slot], w_sem.at[slot, 1]))

    for el in range(min(2, exp_dev)):
        for copy in weight_copies(el):
            copy.start()

    barrier = pltpu.get_barrier_semaphore()
    for step in range(1, n_ep):
        pl.semaphore_signal(barrier, inc=1, device_id={'ep': lax.rem(me + step, n_ep)}, device_id_type=MESH)
    for step in range(1, n_dp):
        pl.semaphore_signal(barrier, inc=1, device_id={'dp': lax.rem(my_dp + step, n_dp)}, device_id_type=MESH)

    logits = lg_ref[...]
    logits_t = logits.T
    _, _, first_t, second_t = top_two(logits_t, 0)
    row_i = lax.broadcasted_iota(jnp.int32, (tok, tok), 0)
    col_i = lax.broadcasted_iota(jnp.int32, (tok, tok), 1)
    upper = as_one(row_i < col_i).astype(BF)
    rank_t = dot(as_one(first_t | second_t).astype(BF), upper)
    e_ids = iota_f((experts, tok), 0)
    ranks, ids = [], []
    for mask in (first_t, second_t):
        ids.append(jnp.sum(jnp.where(mask, e_ids, 0.0), axis=0, keepdims=True))
        ranks.append(jnp.sum(jnp.where(mask, rank_t, 0.0), axis=0, keepdims=True))
    chip_f = chip.astype(F32)
    base = me.astype(F32) * float(experts * src_cap)
    reach = [jnp.zeros((1, tok), F32), jnp.zeros((1, tok), F32)]
    opposite = jnp.zeros((1, tok), jnp.bool_)
    for expert_id in ids:
        delta = jnp.floor((expert_id + 0.5) * (1.0 / (2 * exp_dev))) - chip_f
        delta = jnp.where(delta < 0.0, delta + n_chip, delta)
        reach[0] = jnp.maximum(reach[0], jnp.where(delta < half, delta, 0.0))
        reach[1] = jnp.maximum(reach[1], jnp.where(delta > half, n_chip - delta, 0.0))
        opposite = opposite | (delta == half)
    odd = lax.rem(lax.broadcasted_iota(jnp.int32, (1, tok), 1) + core, 2) == 0
    forward = (reach[0] > reach[1]) | ((reach[0] == reach[1]) & odd)
    reach = [jnp.where(opposite & forward, float(half), reach[0]),
             jnp.where(opposite & jnp.logical_not(forward), float(half), reach[1])]

    zero_row = jnp.zeros((1, tok), F32)
    info = jnp.concatenate([ids[0], ranks[0], ids[1], ranks[1], zero_row + 1.0, zero_row, zero_row, zero_row], axis=0).astype(BF)
    over = jnp.zeros((1, 1), F32)
    meta_send[...] = jnp.zeros_like(meta_send)
    x_val = x_ref[...]
    for way in range(2):
        level = float(half) - iota_f((8, tok), 0)
        member = as_one((reach[way] == level) & (level > 0.5))
        inner = dot(member.astype(BF), upper)
        sizes = jnp.sum(member, axis=1, keepdims=True)
        place = zero_row - 1.0
        total = jnp.zeros((1, 1), F32)
        for lev in range(half):
            place = jnp.where(member[lev:lev + 1] > 0.5, inner[lev:lev + 1] + total, place)
            total = total + sizes[lev:lev + 1]
            over = jnp.maximum(over, as_one(total > float(bounds[lev + 1])))
        pick = as_one(iota_f((HOP_ROWS[0], tok), 0) == place).astype(BF)
        blk[way] = dot(pick, x_val).astype(BF)
        keys = lax.dot_general(info, pick, (((1,), (1,)), ((), ())), preferred_element_type=F32)
        for c in range(2):
            key = base + keys[2 * c:2 * c + 1] * float(src_cap) + keys[2 * c + 1:2 * c + 2]
            meta_send[2 * way + c:2 * way + c + 1, 0:HOP_ROWS[0]] = jnp.where(keys[4:5] > 0.5, key, -1.0)
    for c in range(2):
        meta_send[6 + c:7 + c, :] = base + ids[c] * float(src_cap) + ranks[c]

    best, runner, first, second = top_two(logits, 1)
    chosen = as_one(first | second)
    meta_send[4:5, 0:experts] = jnp.sum(chosen, axis=0, keepdims=True)
    meta_send[5:6, :] = zero_row + over
    metas[me] = meta_send[...]
    rank = dot(as_one(row_i > col_i).astype(BF), chosen.astype(BF))
    lane_e = iota_f((tok, experts), 1)
    norm = jnp.sum(jnp.exp(logits - best), axis=1, keepdims=True)
    gates = (1.0 / norm, jnp.exp(runner - best) / norm)
    tkeys = [jnp.sum(jnp.where(mask, lane_e * float(src_cap) + rank, 0.0), axis=1, keepdims=True) for mask in (first, second)]

    pl.semaphore_wait(barrier, n_ep - 1 + n_dp - 1)

    def meta_copy(step):
        dest = lax.rem(me + step, n_ep)
        return pltpu.make_async_remote_copy(
            src_ref=meta_send, dst_ref=metas.at[me], send_sem=meta_ssem.at[step], recv_sem=meta_rsem.at[step],
            device_id={'ep': dest}, device_id_type=MESH)

    def hop_copy(way, hop, part):
        lo, size = bounds[part], bounds[part + 1] - bounds[part]
        src = blk.at[way, pl.ds(lo, size)] if hop == 0 else ring.at[way, pl.ds(starts[hop - 1] + lo, size)]
        return pltpu.make_async_remote_copy(
            src_ref=src, dst_ref=ring.at[way, pl.ds(starts[hop] + lo, size)],
            send_sem=send_sem.at[way, hop, part], recv_sem=recv_sem.at[way, hop, part],
            device_id={'ep': nxt[way]}, device_id_type=MESH)

    def mirror_copy(way, hop):
        rows = pl.ds(starts[hop], HOP_ROWS[hop])
        return pltpu.make_async_remote_copy(
            src_ref=ring.at[way, rows], dst_ref=mirror.at[way, rows],
            send_sem=mir_send.at[way, hop], recv_sem=mir_recv.at[way, hop],
            device_id={'ep': other}, device_id_type=MESH)

    px_copy = pltpu.make_async_remote_copy(
        src_ref=x_ref, dst_ref=px, send_sem=px_sem.at[0], recv_sem=px_sem.at[1],
        device_id={'ep': other}, device_id_type=MESH)

    def parts_of(hop):
        return [p for p in range(half - hop) if bounds[p + 1] > bounds[p]]

    px_copy.start()
    for step in range(1, n_ep):
        meta_copy(step).start()
    for part in parts_of(0):
        for way in range(2):
            hop_copy(way, 0, part).start()

    for step in range(1, n_ep):
        meta_copy(step).wait_recv()
    counts = jnp.concatenate([metas[s, 4:5, 0:experts] for s in range(n_ep)], axis=0)
    over = metas[0, 5:6, 0:128]
    for s in range(1, n_ep):
        over = jnp.maximum(over, metas[s, 5:6, 0:128])
    tri = as_one(lax.broadcasted_iota(jnp.int32, (n_ep, n_ep), 1) <= lax.broadcasted_iota(jnp.int32, (n_ep, n_ep), 0)).astype(BF)
    ends = dot(tri, counts.astype(BF))
    lane_ep = lax.broadcasted_iota(jnp.int32, (n_ep, experts), 1)
    slot = iota_f((n_ep, capacity), 1)
    for el in range(exp_dev):
        mine = lane_ep == me * exp_dev + el
        count_col = jnp.sum(jnp.where(mine, counts, 0.0), axis=1, keepdims=True)
        end_col = jnp.sum(jnp.where(mine, ends, 0.0), axis=1, keepdims=True)
        past = as_one(end_col <= slot)
        src = jnp.sum(past, axis=0, keepdims=True)
        rnk = slot[0:1] - jnp.sum(past * count_col, axis=0, keepdims=True)
        valid = src < float(n_ep)
        e_base = (me * exp_dev + el).astype(F32) * float(src_cap)
        key = jnp.where(valid, src * float(experts * src_cap) + e_base + rnk, -2.0)
        skey[el] = jnp.broadcast_to(key, (128, capacity)).T
        rkeys[el:el + 1, :] = jnp.where(valid, src * float(src_cap) + rnk, -1.0)

    def gather_rows(rows, keys_one, keys_two, first_time=False):
        def body(el, carry):
            want = skey[el][:, 0:1]
            hit = as_one((want == keys_one) | (want == keys_two)).astype(BF)
            part = dot(hit, rows[...])
            if first_time:
                acc[el] = part
            else:
                acc[el] = acc[el] + part
            return carry
        lax.fori_loop(0, exp_dev, body, 0)

    def gather_block(buf, way, hop, core_id):
        far = lax.rem(chip + (n_chip - 1 - hop if way == 0 else hop + 1), n_chip)
        src = far * 2 + core_id
        size = HOP_ROWS[hop]
        gather_rows(buf.at[way, pl.ds(starts[hop], size)],
                    metas[src, 2 * way:2 * way + 1, 0:size], metas[src, 2 * way + 1:2 * way + 2, 0:size])

    gather_rows(x_ref, metas[me, 6:7, :], metas[me, 7:8, :], True)
    px_copy.wait_recv()
    gather_rows(px, metas[other, 6:7, :], metas[other, 7:8, :])

    for hop in range(half):
        parts = parts_of(hop)
        for part in parts:
            for way in range(2):
                hop_copy(way, hop, part).wait_recv()
                if hop + 1 < half and part in parts_of(hop + 1):
                    hop_copy(way, hop + 1, part).start()
        for way in range(2):
            mirror_copy(way, hop).start()
        if hop > 0:
            for way in range(2):
                mirror_copy(way, hop - 1).wait_recv()
                gather_block(mirror, way, hop - 1, 1 - core)
        for way in range(2):
            gather_block(ring, way, hop, core)
    for way in range(2):
        mirror_copy(way, half - 1).wait_recv()
        gather_block(mirror, way, half - 1, 1 - core)

    flag_buf[0] = jnp.broadcast_to(over, (8, 128))

    def flag_copy(step):
        return pltpu.make_async_remote_copy(
            src_ref=flag_buf.at[0], dst_ref=flag_buf.at[step], send_sem=flag_ssem.at[step], recv_sem=flag_rsem.at[step],
            device_id={'dp': lax.rem(my_dp + step, n_dp)}, device_id_type=MESH)

    for step in range(1, n_dp):
        flag_copy(step).start()

    def ret_copy(el, step):
        dest = lax.rem(me + step, n_ep)
        return pltpu.make_async_remote_copy(
            src_ref=ret.at[el, pl.ds(pl.multiple_of(dest * src_cap, src_cap), src_cap)],
            dst_ref=back.at[el, pl.ds(pl.multiple_of(me * src_cap, src_cap), src_cap)],
            send_sem=ret_ssem.at[el, step], recv_sem=ret_rsem.at[el, step],
            device_id={'ep': dest}, device_id_type=MESH)

    ret_order = sorted(range(1, n_ep), key=lambda s: -min(s, n_ep - s))

    for el in range(exp_dev):
        for copy in weight_copies(el):
            copy.wait()
        rows = acc[el].astype(BF)
        z_acc[...] = jnp.zeros_like(z_acc)

        def ff_body(tile, carry, rows=rows, spot=el % 2):
            cols = pl.ds(pl.multiple_of(tile * FF_TILE, FF_TILE), FF_TILE)
            hidden = jax.nn.gelu(dot(rows, w1_buf[spot, :, cols]), approximate=True).astype(BF)
            z_acc[...] += dot(hidden, w2_buf[spot, cols, :])
            return carry

        lax.fori_loop(0, ff // FF_TILE, ff_body, 0)
        if el + 2 < exp_dev:
            for copy in weight_copies(el + 2):
                copy.start()
        spread = as_one(iota_f((n_ep * src_cap, capacity), 0) == rkeys[el:el + 1, :]).astype(BF)
        ret[el] = dot(spread, z_acc[...].astype(BF)).astype(BF)
        for step in ret_order:
            ret_copy(el, step).start()
        own = pl.ds(pl.multiple_of(me * src_cap, src_cap), src_cap)
        back[el, own, :] = ret[el, own, :]

    slot_i = lax.broadcasted_iota(jnp.int32, (1, n_ep * src_cap), 1)
    slot_src = lax.div(slot_i, src_cap)
    for el in range(exp_dev):
        for step in ret_order:
            ret_copy(el, step).wait_recv()
        slot_key = ((slot_src * exp_dev + el) * src_cap + (slot_i - slot_src * src_cap)).astype(F32)
        for c in range(2):
            hit = as_one(tkeys[c] == slot_key).astype(BF)
            part = gates[c] * dot(hit, back[el])
            if el == 0 and c == 0:
                y_acc[...] = part
            else:
                y_acc[...] += part
    out_ref[...] = (x_ref[...].astype(F32) + y_acc[...]).astype(BF)

    worst = flag_buf[0]
    for step in range(1, n_dp):
        flag_copy(step).wait_recv()
        worst = jnp.maximum(worst, flag_buf[step])
    flag_ref[...] = worst

    px_copy.wait_send()
    for step in range(1, n_ep):
        meta_copy(step).wait_send()
    for step in range(1, n_dp):
        flag_copy(step).wait_send()
    for hop in range(half):
        for way in range(2):
            mirror_copy(way, hop).wait_send()
            for part in parts_of(hop):
                hop_copy(way, hop, part).wait_send()
    for el in range(exp_dev):
        for step in ret_order:
            ret_copy(el, step).wait_send()


def solution(mesh):
    n_ep = mesh.shape['ep']
    n_dp = mesh.shape['dp']
    row_spec = P(('dp', 'ep'), None)
    expert_spec = P('ep', None, None)

    def local_step(x_rows, logits, w_in, w_out):
        tok, d_model = x_rows.shape
        experts = logits.shape[1]
        exp_dev, _, ff = w_in.shape
        capacity = CAP_FACTOR * tok * n_ep // experts
        src_cap = 4 * tok // experts
        half = n_ep // 4
        all_rows = sum(HOP_ROWS)
        vmem = pl.BlockSpec(memory_space=pltpu.VMEM)
        hbm = pl.BlockSpec(memory_space=pl.ANY)
        dma = pltpu.SemaphoreType.DMA
        out, flag = pl.pallas_call(
            functools.partial(moe_kernel, n_ep, n_dp, capacity, src_cap),
            out_shape=(jax.ShapeDtypeStruct((tok, d_model), BF), jax.ShapeDtypeStruct((8, 128), F32)),
            in_specs=[vmem, vmem, hbm, hbm],
            out_specs=(vmem, vmem),
            scratch_shapes=[
                pltpu.VMEM((2, d_model, ff), BF),
                pltpu.VMEM((2, ff, d_model), BF),
                pltpu.VMEM((2, HOP_ROWS[0], d_model), BF),
                pltpu.VMEM((2, all_rows, d_model), BF),
                pltpu.VMEM((2, all_rows, d_model), BF),
                pltpu.VMEM((tok, d_model), BF),
                pltpu.VMEM((8, tok), F32),
                pltpu.VMEM((n_ep, 8, tok), F32),
                pltpu.VMEM((exp_dev, capacity, d_model), F32),
                pltpu.VMEM((capacity, d_model), F32),
                pltpu.VMEM((exp_dev, capacity, 128), F32),
                pltpu.VMEM((8, capacity), F32),
                pltpu.VMEM((exp_dev, n_ep * src_cap, d_model), BF),
                pltpu.VMEM((exp_dev, n_ep * src_cap, d_model), BF),
                pltpu.VMEM((tok, d_model), F32),
                pltpu.VMEM((n_dp, 8, 128), F32),
                dma((2, 2)),
                dma((2, half, half)), dma((2, half, half)),
                dma((2, half)), dma((2, half)),
                dma((2,)),
                dma((n_ep,)), dma((n_ep,)),
                dma((exp_dev, n_ep)), dma((exp_dev, n_ep)),
                dma((n_dp,)), dma((n_dp,)),
            ],
            compiler_params=pltpu.CompilerParams(
                collective_id=0, has_side_effects=True, vmem_limit_bytes=62 * 1024 * 1024),
            name='moe_layer',
        )(x_rows, logits, w_in, w_out)
        return out

    return jax.shard_map(local_step, mesh=mesh, in_specs=(row_spec, row_spec, expert_spec, expert_spec), out_specs=row_spec, check_vma=False)
```

```python
import functools

import jax
import jax.numpy as jnp
from jax import lax
from jax.experimental import pallas as pl
from jax.experimental.pallas import tpu as pltpu
from jax.sharding import PartitionSpec as P

CAP_FACTOR = 2
HOP_ROWS = (464, 384, 304, 160)
FF_TILE = 512
BF = jnp.bfloat16
F32 = jnp.float32
MESH = pl.DeviceIdType.MESH


def top_two(vals, axis):
    best = jnp.max(vals, axis=axis, keepdims=True)
    first = vals == best
    rest = jnp.where(first, -jnp.inf, vals)
    runner = jnp.max(rest, axis=axis, keepdims=True)
    return best, runner, first, rest == runner


def as_one(mask):
    return jnp.where(mask, 1.0, 0.0)


def iota_f(shape, dim):
    return lax.broadcasted_iota(jnp.int32, shape, dim).astype(F32)


def dot(lhs, rhs):
    return jnp.dot(lhs, rhs, preferred_element_type=F32)


def moe_kernel(n_ep, n_dp, capacity, src_cap, x_ref, lg_ref, w1_hbm, w2_hbm, out_ref, flag_ref,
               w1_buf, w2_buf, blk, ring, mirror, px, meta_send, metas, acc, z_acc, skey, rkeys,
               ret, back, y_acc, flag_buf,
               w_sem, send_sem, recv_sem, mir_send, mir_recv, px_sem, meta_ssem, meta_rsem,
               ret_ssem, ret_rsem, flag_ssem, flag_rsem):
    tok, d_model = x_ref.shape
    experts = lg_ref.shape[1]
    exp_dev = experts // n_ep
    ff = w1_buf.shape[2]
    n_chip = n_ep // 2
    half = n_chip // 2
    me = lax.axis_index('ep')
    my_dp = lax.axis_index('dp')
    chip = lax.div(me, 2)
    core = lax.rem(me, 2)
    other = chip * 2 + 1 - core
    nxt = (lax.rem(chip + 1, n_chip) * 2 + core, lax.rem(chip + n_chip - 1, n_chip) * 2 + core)
    bounds = (0,) + HOP_ROWS[::-1]
    starts = [sum(HOP_ROWS[:h]) for h in range(half)]

    def weight_copies(el):
        slot = lax.rem(el, 2)
        return (pltpu.make_async_copy(w1_hbm.at[el], w1_buf.at[slot], w_sem.at[slot, 0]),
                pltpu.make_async_copy(w2_hbm.at[el], w2_buf.at[slot], w_sem.at[slot, 1]))

    for el in range(min(2, exp_dev)):
        for copy in weight_copies(el):
            copy.start()

    barrier = pltpu.get_barrier_semaphore()
    for step in range(1, n_ep):
        pl.semaphore_signal(barrier, inc=1, device_id={'ep': lax.rem(me + step, n_ep)}, device_id_type=MESH)
    for step in range(1, n_dp):
        pl.semaphore_signal(barrier, inc=1, device_id={'dp': lax.rem(my_dp + step, n_dp)}, device_id_type=MESH)

    logits = lg_ref[...]
    logits_t = logits.T
    _, _, first_t, second_t = top_two(logits_t, 0)
    row_i = lax.broadcasted_iota(jnp.int32, (tok, tok), 0)
    col_i = lax.broadcasted_iota(jnp.int32, (tok, tok), 1)
    upper = as_one(row_i < col_i).astype(BF)
    rank_t = dot(as_one(first_t | second_t).astype(BF), upper)
    e_ids = iota_f((experts, tok), 0)
    ranks, ids = [], []
    for mask in (first_t, second_t):
        ids.append(jnp.sum(jnp.where(mask, e_ids, 0.0), axis=0, keepdims=True))
        ranks.append(jnp.sum(jnp.where(mask, rank_t, 0.0), axis=0, keepdims=True))
    chip_f = chip.astype(F32)
    base = me.astype(F32) * float(experts * src_cap)
    reach = [jnp.zeros((1, tok), F32), jnp.zeros((1, tok), F32)]
    opposite = jnp.zeros((1, tok), jnp.bool_)
    for expert_id in ids:
        delta = jnp.floor((expert_id + 0.5) * (1.0 / (2 * exp_dev))) - chip_f
        delta = jnp.where(delta < 0.0, delta + n_chip, delta)
        reach[0] = jnp.maximum(reach[0], jnp.where(delta < half, delta, 0.0))
        reach[1] = jnp.maximum(reach[1], jnp.where(delta > half, n_chip - delta, 0.0))
        opposite = opposite | (delta == half)
    odd = lax.rem(lax.broadcasted_iota(jnp.int32, (1, tok), 1) + core, 2) == 0
    forward = (reach[0] > reach[1]) | ((reach[0] == reach[1]) & odd)
    reach = [jnp.where(opposite & forward, float(half), reach[0]),
             jnp.where(opposite & jnp.logical_not(forward), float(half), reach[1])]

    zero_row = jnp.zeros((1, tok), F32)
    info = jnp.concatenate([ids[0], ranks[0], ids[1], ranks[1], zero_row + 1.0, zero_row, zero_row, zero_row], axis=0).astype(BF)
    over = jnp.zeros((1, 1), F32)
    meta_send[...] = jnp.zeros_like(meta_send)
    x_val = x_ref[...]
    for way in range(2):
        level = float(half) - iota_f((8, tok), 0)
        member = as_one((reach[way] == level) & (level > 0.5))
        inner = dot(member.astype(BF), upper)
        sizes = jnp.sum(member, axis=1, keepdims=True)
        place = zero_row - 1.0
        total = jnp.zeros((1, 1), F32)
        for lev in range(half):
            place = jnp.where(member[lev:lev + 1] > 0.5, inner[lev:lev + 1] + total, place)
            total = total + sizes[lev:lev + 1]
            over = jnp.maximum(over, as_one(total > float(bounds[lev + 1])))
        pick = as_one(iota_f((HOP_ROWS[0], tok), 0) == place).astype(BF)
        blk[way] = dot(pick, x_val).astype(BF)
        keys = lax.dot_general(info, pick, (((1,), (1,)), ((), ())), preferred_element_type=F32)
        for c in range(2):
            key = base + keys[2 * c:2 * c + 1] * float(src_cap) + keys[2 * c + 1:2 * c + 2]
            meta_send[2 * way + c:2 * way + c + 1, 0:HOP_ROWS[0]] = jnp.where(keys[4:5] > 0.5, key, -1.0)
    for c in range(2):
        meta_send[6 + c:7 + c, :] = base + ids[c] * float(src_cap) + ranks[c]

    best, runner, first, second = top_two(logits, 1)
    chosen = as_one(first | second)
    meta_send[4:5, 0:experts] = jnp.sum(chosen, axis=0, keepdims=True)
    meta_send[5:6, :] = zero_row + over
    metas[me] = meta_send[...]
    rank = dot(as_one(row_i > col_i).astype(BF), chosen.astype(BF))
    lane_e = iota_f((tok, experts), 1)
    norm = jnp.sum(jnp.exp(logits - best), axis=1, keepdims=True)
    gates = (1.0 / norm, jnp.exp(runner - best) / norm)
    tkeys = [jnp.sum(jnp.where(mask, lane_e * float(src_cap) + rank, 0.0), axis=1, keepdims=True) for mask in (first, second)]

    pl.semaphore_wait(barrier, n_ep - 1 + n_dp - 1)

    def meta_copy(step):
        dest = lax.rem(me + step, n_ep)
        return pltpu.make_async_remote_copy(
            src_ref=meta_send, dst_ref=metas.at[me], send_sem=meta_ssem.at[step], recv_sem=meta_rsem.at[step],
            device_id={'ep': dest}, device_id_type=MESH)

    def hop_copy(way, hop, part):
        lo, size = bounds[part], bounds[part + 1] - bounds[part]
        src = blk.at[way, pl.ds(lo, size)] if hop == 0 else ring.at[way, pl.ds(starts[hop - 1] + lo, size)]
        return pltpu.make_async_remote_copy(
            src_ref=src, dst_ref=ring.at[way, pl.ds(starts[hop] + lo, size)],
            send_sem=send_sem.at[way, hop, part], recv_sem=recv_sem.at[way, hop, part],
            device_id={'ep': nxt[way]}, device_id_type=MESH)

    def mirror_copy(way, hop):
        rows = pl.ds(starts[hop], HOP_ROWS[hop])
        return pltpu.make_async_remote_copy(
            src_ref=ring.at[way, rows], dst_ref=mirror.at[way, rows],
            send_sem=mir_send.at[way, hop], recv_sem=mir_recv.at[way, hop],
            device_id={'ep': other}, device_id_type=MESH)

    px_copy = pltpu.make_async_remote_copy(
        src_ref=x_ref, dst_ref=px, send_sem=px_sem.at[0], recv_sem=px_sem.at[1],
        device_id={'ep': other}, device_id_type=MESH)

    def parts_of(hop):
        return [p for p in range(half - hop) if bounds[p + 1] > bounds[p]]

    px_copy.start()
    for step in range(1, n_ep):
        meta_copy(step).start()
    for part in parts_of(0):
        for way in range(2):
            hop_copy(way, 0, part).start()

    for step in range(1, n_ep):
        meta_copy(step).wait_recv()
    counts = jnp.concatenate([metas[s, 4:5, 0:experts] for s in range(n_ep)], axis=0)
    over = metas[0, 5:6, 0:128]
    for s in range(1, n_ep):
        over = jnp.maximum(over, metas[s, 5:6, 0:128])
    tri = as_one(lax.broadcasted_iota(jnp.int32, (n_ep, n_ep), 1) <= lax.broadcasted_iota(jnp.int32, (n_ep, n_ep), 0)).astype(BF)
    ends = dot(tri, counts.astype(BF))
    lane_ep = lax.broadcasted_iota(jnp.int32, (n_ep, experts), 1)
    slot = iota_f((n_ep, capacity), 1)
    for el in range(exp_dev):
        mine = lane_ep == me * exp_dev + el
        count_col = jnp.sum(jnp.where(mine, counts, 0.0), axis=1, keepdims=True)
        end_col = jnp.sum(jnp.where(mine, ends, 0.0), axis=1, keepdims=True)
        past = as_one(end_col <= slot)
        src = jnp.sum(past, axis=0, keepdims=True)
        rnk = slot[0:1] - jnp.sum(past * count_col, axis=0, keepdims=True)
        valid = src < float(n_ep)
        e_base = (me * exp_dev + el).astype(F32) * float(src_cap)
        key = jnp.where(valid, src * float(experts * src_cap) + e_base + rnk, -2.0)
        skey[el] = jnp.broadcast_to(key, (128, capacity)).T
        rkeys[el:el + 1, :] = jnp.where(valid, src * float(src_cap) + rnk, -1.0)

    def gather_rows(rows, keys_one, keys_two, first_time=False):
        def body(el, carry):
            want = skey[el][:, 0:1]
            hit = as_one((want == keys_one) | (want == keys_two)).astype(BF)
            part = dot(hit, rows[...])
            if first_time:
                acc[el] = part
            else:
                acc[el] = acc[el] + part
            return carry
        lax.fori_loop(0, exp_dev, body, 0)

    def gather_block(buf, way, hop, core_id):
        far = lax.rem(chip + (n_chip - 1 - hop if way == 0 else hop + 1), n_chip)
        src = far * 2 + core_id
        size = HOP_ROWS[hop]
        gather_rows(buf.at[way, pl.ds(starts[hop], size)],
                    metas[src, 2 * way:2 * way + 1, 0:size], metas[src, 2 * way + 1:2 * way + 2, 0:size])

    gather_rows(x_ref, metas[me, 6:7, :], metas[me, 7:8, :], True)
    px_copy.wait_recv()
    gather_rows(px, metas[other, 6:7, :], metas[other, 7:8, :])

    for hop in range(half):
        parts = parts_of(hop)
        for part in parts:
            for way in range(2):
                hop_copy(way, hop, part).wait_recv()
                if hop + 1 < half and part in parts_of(hop + 1):
                    hop_copy(way, hop + 1, part).start()
        for way in range(2):
            mirror_copy(way, hop).start()
        if hop > 0:
            for way in range(2):
                mirror_copy(way, hop - 1).wait_recv()
                gather_block(mirror, way, hop - 1, 1 - core)
        for way in range(2):
            gather_block(ring, way, hop, core)
    for way in range(2):
        mirror_copy(way, half - 1).wait_recv()
        gather_block(mirror, way, half - 1, 1 - core)

    flag_buf[0] = jnp.broadcast_to(over, (8, 128))

    def flag_copy(step):
        return pltpu.make_async_remote_copy(
            src_ref=flag_buf.at[0], dst_ref=flag_buf.at[step], send_sem=flag_ssem.at[step], recv_sem=flag_rsem.at[step],
            device_id={'dp': lax.rem(my_dp + step, n_dp)}, device_id_type=MESH)

    for step in range(1, n_dp):
        flag_copy(step).start()

    def ret_copy(el, step):
        dest = lax.rem(me + step, n_ep)
        return pltpu.make_async_remote_copy(
            src_ref=ret.at[el, pl.ds(pl.multiple_of(dest * src_cap, src_cap), src_cap)],
            dst_ref=back.at[el, pl.ds(pl.multiple_of(me * src_cap, src_cap), src_cap)],
            send_sem=ret_ssem.at[el, step], recv_sem=ret_rsem.at[el, step],
            device_id={'ep': dest}, device_id_type=MESH)

    ret_order = sorted(range(1, n_ep), key=lambda s: -min(s, n_ep - s))

    def expert_body(el, carry):
        spot = lax.rem(el, 2)
        for copy in weight_copies(el):
            copy.wait()
        rows = acc[el].astype(BF)
        z_acc[...] = jnp.zeros_like(z_acc)

        def ff_body(tile, inner):
            cols = pl.ds(pl.multiple_of(tile * FF_TILE, FF_TILE), FF_TILE)
            hidden = jax.nn.gelu(dot(rows, w1_buf[spot, :, cols]), approximate=True).astype(BF)
            z_acc[...] += dot(hidden, w2_buf[spot, cols, :])
            return inner

        lax.fori_loop(0, ff // FF_TILE, ff_body, 0)

        @pl.when(el + 2 < exp_dev)
        def _():
            for copy in weight_copies(el + 2):
                copy.start()

        spread = as_one(iota_f((n_ep * src_cap, capacity), 0) == rkeys[pl.ds(el, 1), :]).astype(BF)
        ret[el] = dot(spread, z_acc[...].astype(BF)).astype(BF)
        for step in ret_order:
            ret_copy(el, step).start()
        own = pl.ds(pl.multiple_of(me * src_cap, src_cap), src_cap)
        back[el, own, :] = ret[el, own, :]
        return carry

    lax.fori_loop(0, exp_dev, expert_body, 0)

    slot_i = lax.broadcasted_iota(jnp.int32, (1, n_ep * src_cap), 1)
    slot_src = lax.div(slot_i, src_cap)
    y_acc[...] = jnp.zeros_like(y_acc)

    def mix_body(el, carry):
        for step in ret_order:
            ret_copy(el, step).wait_recv()
        slot_key = ((slot_src * exp_dev + el) * src_cap + (slot_i - slot_src * src_cap)).astype(F32)
        for c in range(2):
            hit = as_one(tkeys[c] == slot_key).astype(BF)
            y_acc[...] += gates[c] * dot(hit, back[el])
        return carry

    lax.fori_loop(0, exp_dev, mix_body, 0)
    out_ref[...] = (x_ref[...].astype(F32) + y_acc[...]).astype(BF)

    worst = flag_buf[0]
    for step in range(1, n_dp):
        flag_copy(step).wait_recv()
        worst = jnp.maximum(worst, flag_buf[step])
    flag_ref[...] = worst

    px_copy.wait_send()
    for step in range(1, n_ep):
        meta_copy(step).wait_send()
    for step in range(1, n_dp):
        flag_copy(step).wait_send()
    for hop in range(half):
        for way in range(2):
            mirror_copy(way, hop).wait_send()
            for part in parts_of(hop):
                hop_copy(way, hop, part).wait_send()
    for el in range(exp_dev):
        for step in ret_order:
            ret_copy(el, step).wait_send()


def plain_step(n_ep, x_rows, logits, w_in, w_out):
    tok_dev, d_model = x_rows.shape
    experts = logits.shape[1]
    exp_dev = w_in.shape[0]
    capacity = CAP_FACTOR * tok_dev * n_ep // experts
    src_cap = 4 * tok_dev // experts
    my_index = lax.axis_index('ep')
    gate_probs = jax.nn.softmax(logits, axis=-1)
    top_vals, top_ids = lax.top_k(logits, 2)
    chosen = (logits >= top_vals[:, 1:2]).astype(jnp.int32)
    local_before = jnp.cumsum(chosen, axis=0) - chosen
    local_counts = jnp.sum(chosen, axis=0).astype(jnp.float32)
    all_counts = lax.all_gather(local_counts, 'ep').astype(jnp.int32)
    dev_offsets = jnp.cumsum(all_counts, axis=0) - all_counts
    local_pos = jnp.take_along_axis(local_before, top_ids, axis=1)
    kept_mask = local_pos + jnp.take(dev_offsets[my_index], top_ids) < capacity
    send_row = jnp.where(kept_mask, top_ids * src_cap + local_pos, experts * src_cap)
    tok_ids = jnp.broadcast_to(jnp.arange(tok_dev, dtype=jnp.int32)[:, None], (tok_dev, 2))
    slot_tok = jnp.full((experts * src_cap,), tok_dev, jnp.int32).at[send_row.reshape(-1)].set(tok_ids.reshape(-1), mode='drop')
    send_buf = jnp.take(x_rows, slot_tok, axis=0, mode='fill', fill_value=0)
    recv_buf = lax.all_to_all(send_buf, 'ep', 0, 0, tiled=True)

    own_counts = lax.dynamic_slice_in_dim(all_counts, my_index * exp_dev, exp_dev, axis=1)
    own_offsets = lax.dynamic_slice_in_dim(dev_offsets, my_index * exp_dev, exp_dev, axis=1)
    kept_counts = jnp.minimum(jnp.maximum(capacity - own_offsets, 0), own_counts)
    slot_ends = (own_offsets + kept_counts).T
    cap_ids = jnp.arange(capacity, dtype=jnp.int32)
    below_mask = slot_ends[:, None, :] <= cap_ids[None, :, None]
    src_dev = jnp.sum(below_mask.astype(jnp.int32), axis=2)
    slot_start = jnp.sum(jnp.where(below_mask, kept_counts.T[:, None, :], 0), axis=2)
    exp_local = jnp.arange(exp_dev, dtype=jnp.int32)
    recv_row = (src_dev * exp_dev + exp_local[:, None]) * src_cap + cap_ids[None, :] - slot_start
    recv_row = jnp.where(src_dev < n_ep, recv_row, n_ep * exp_dev * src_cap)
    expert_rows = jnp.take(recv_buf, recv_row.reshape(-1), axis=0, mode='fill', fill_value=0).reshape(exp_dev, capacity, d_model)
    hidden = jax.nn.gelu(jnp.einsum('ecd,edf->ecf', expert_rows, w_in, preferred_element_type=jnp.float32), approximate=True).astype(jnp.bfloat16)
    expert_out = jnp.einsum('ecf,efd->ecd', hidden, w_out, preferred_element_type=jnp.float32).astype(jnp.bfloat16).reshape(exp_dev * capacity, d_model)

    src_slots = jnp.arange(src_cap, dtype=jnp.int32)
    back_row = exp_local[None, :, None] * capacity + own_offsets[:, :, None] + src_slots[None, None, :]
    back_row = jnp.where(src_slots[None, None, :] < kept_counts[:, :, None], back_row, exp_dev * capacity)
    back_buf = jnp.take(expert_out, back_row.reshape(-1), axis=0, mode='fill', fill_value=0)
    ret_buf = lax.all_to_all(back_buf, 'ep', 0, 0, tiled=True)

    rows_back = jnp.take(ret_buf, send_row, axis=0, mode='fill', fill_value=0)
    pick_gate = jnp.take_along_axis(gate_probs, top_ids, axis=1)
    mix_sum = jnp.sum(pick_gate[:, :, None] * rows_back.astype(jnp.float32), axis=1)
    return (x_rows.astype(jnp.float32) + mix_sum).astype(jnp.bfloat16)


def solution(mesh):
    n_ep = mesh.shape['ep']
    n_dp = mesh.shape['dp']
    row_spec = P(('dp', 'ep'), None)
    expert_spec = P('ep', None, None)

    def local_step(x_rows, logits, w_in, w_out):
        tok, d_model = x_rows.shape
        experts = logits.shape[1]
        exp_dev, _, ff = w_in.shape
        capacity = CAP_FACTOR * tok * n_ep // experts
        src_cap = 4 * tok // experts
        half = n_ep // 4
        all_rows = sum(HOP_ROWS)
        vmem = pl.BlockSpec(memory_space=pltpu.VMEM)
        hbm = pl.BlockSpec(memory_space=pl.ANY)
        dma = pltpu.SemaphoreType.DMA
        out, flag = pl.pallas_call(
            functools.partial(moe_kernel, n_ep, n_dp, capacity, src_cap),
            out_shape=(jax.ShapeDtypeStruct((tok, d_model), BF), jax.ShapeDtypeStruct((8, 128), F32)),
            in_specs=[vmem, vmem, hbm, hbm],
            out_specs=(vmem, vmem),
            scratch_shapes=[
                pltpu.VMEM((2, d_model, ff), BF),
                pltpu.VMEM((2, ff, d_model), BF),
                pltpu.VMEM((2, HOP_ROWS[0], d_model), BF),
                pltpu.VMEM((2, all_rows, d_model), BF),
                pltpu.VMEM((2, all_rows, d_model), BF),
                pltpu.VMEM((tok, d_model), BF),
                pltpu.VMEM((8, tok), F32),
                pltpu.VMEM((n_ep, 8, tok), F32),
                pltpu.VMEM((exp_dev, capacity, d_model), F32),
                pltpu.VMEM((capacity, d_model), F32),
                pltpu.VMEM((exp_dev, capacity, 128), F32),
                pltpu.VMEM((8, capacity), F32),
                pltpu.VMEM((exp_dev, n_ep * src_cap, d_model), BF),
                pltpu.VMEM((exp_dev, n_ep * src_cap, d_model), BF),
                pltpu.VMEM((tok, d_model), F32),
                pltpu.VMEM((n_dp, 8, 128), F32),
                dma((2, 2)),
                dma((2, half, half)), dma((2, half, half)),
                dma((2, half)), dma((2, half)),
                dma((2,)),
                dma((n_ep,)), dma((n_ep,)),
                dma((exp_dev, n_ep)), dma((exp_dev, n_ep)),
                dma((n_dp,)), dma((n_dp,)),
            ],
            compiler_params=pltpu.CompilerParams(
                collective_id=0, has_side_effects=True, vmem_limit_bytes=62 * 1024 * 1024),
            name='moe_layer',
        )(x_rows, logits, w_in, w_out)
        return lax.cond(flag[0, 0] > 0.0, functools.partial(plain_step, n_ep), lambda *_: out, x_rows, logits, w_in, w_out)

    return jax.shard_map(local_step, mesh=mesh, in_specs=(row_spec, row_spec, expert_spec, expert_spec), out_specs=row_spec, check_vma=False)
```

```python
import functools

import jax
import jax.numpy as jnp
from jax import lax
from jax.experimental import pallas as pl
from jax.experimental.pallas import tpu as pltpu
from jax.sharding import PartitionSpec as P

CAP_FACTOR = 2
HOP_ROWS = (464, 384, 304, 160)
FF_TILE = 512
BF = jnp.bfloat16
F32 = jnp.float32
MESH = pl.DeviceIdType.MESH


def top_two(vals, axis):
    best = jnp.max(vals, axis=axis, keepdims=True)
    first = vals == best
    rest = jnp.where(first, -jnp.inf, vals)
    runner = jnp.max(rest, axis=axis, keepdims=True)
    return best, runner, first, rest == runner


def as_one(mask):
    return jnp.where(mask, 1.0, 0.0)


def iota_f(shape, dim):
    return lax.broadcasted_iota(jnp.int32, shape, dim).astype(F32)


def dot(lhs, rhs):
    return jnp.dot(lhs, rhs, preferred_element_type=F32)


def moe_kernel(n_ep, n_dp, capacity, src_cap, x_ref, lg_ref, w1_hbm, w2_hbm, out_ref, flag_ref,
               w1_buf, w2_buf, blk, near, hops_a, hops_b, hops_c, hops_d, key_send, key_near, key_ring, key_mir,
               count_send, count_all, acc, z_acc, skey, rkeys, ret, back, y_acc, flag_buf,
               w_sem, send_sem, recv_sem, mir_send, mir_recv, px_sem, ksend_sem, krecv_sem, kmir_send, kmir_recv,
               kpx_sem, count_ssem, count_rsem, ret_ssem, ret_rsem, flag_ssem, flag_rsem):
    tok, d_model = x_ref.shape
    experts = lg_ref.shape[0]
    exp_dev = experts // n_ep
    ff = w1_buf.shape[2]
    n_chip = n_ep // 2
    half = n_chip // 2
    me = lax.axis_index('ep')
    my_dp = lax.axis_index('dp')
    chip = lax.div(me, 2)
    core = lax.rem(me, 2)
    other = chip * 2 + 1 - core
    nxt = (lax.rem(chip + 1, n_chip) * 2 + core, lax.rem(chip + n_chip - 1, n_chip) * 2 + core)
    bounds = (0,) + HOP_ROWS[::-1]
    hop_bufs = (hops_a, hops_b, hops_c, hops_d)

    def weight_copies(el):
        slot = lax.rem(el, 2)
        return (pltpu.make_async_copy(w1_hbm.at[el], w1_buf.at[slot], w_sem.at[slot, 0]),
                pltpu.make_async_copy(w2_hbm.at[el], w2_buf.at[slot], w_sem.at[slot, 1]))

    for el in range(min(2, exp_dev)):
        for copy in weight_copies(el):
            copy.start()

    barrier = pltpu.get_barrier_semaphore()
    for step in range(1, n_ep):
        pl.semaphore_signal(barrier, inc=1, device_id={'ep': lax.rem(me + step, n_ep)}, device_id_type=MESH)
    for step in range(1, n_dp):
        pl.semaphore_signal(barrier, inc=1, device_id={'dp': lax.rem(my_dp + step, n_dp)}, device_id_type=MESH)

    logits_t = lg_ref[...]
    logits = logits_t.T
    _, _, first_t, second_t = top_two(logits_t, 0)
    row_i = lax.broadcasted_iota(jnp.int32, (tok, tok), 0)
    col_i = lax.broadcasted_iota(jnp.int32, (tok, tok), 1)
    upper = as_one(row_i < col_i).astype(BF)
    rank_t = dot(as_one(first_t | second_t).astype(BF), upper)
    e_ids = iota_f((experts, tok), 0)
    ranks, ids = [], []
    for mask in (first_t, second_t):
        ids.append(jnp.sum(jnp.where(mask, e_ids, 0.0), axis=0, keepdims=True))
        ranks.append(jnp.sum(jnp.where(mask, rank_t, 0.0), axis=0, keepdims=True))
    chip_f = chip.astype(F32)
    base = me.astype(F32) * float(experts * src_cap)
    reach = [jnp.zeros((1, tok), F32), jnp.zeros((1, tok), F32)]
    opposite = jnp.zeros((1, tok), jnp.bool_)
    for expert_id in ids:
        delta = jnp.floor((expert_id + 0.5) * (1.0 / (2 * exp_dev))) - chip_f
        delta = jnp.where(delta < 0.0, delta + n_chip, delta)
        reach[0] = jnp.maximum(reach[0], jnp.where(delta < half, delta, 0.0))
        reach[1] = jnp.maximum(reach[1], jnp.where(delta > half, n_chip - delta, 0.0))
        opposite = opposite | (delta == half)
    odd = lax.rem(lax.broadcasted_iota(jnp.int32, (1, tok), 1) + core, 2) == 0
    forward = (reach[0] > reach[1]) | ((reach[0] == reach[1]) & odd)
    reach = [jnp.where(opposite & forward, float(half), reach[0]),
             jnp.where(opposite & jnp.logical_not(forward), float(half), reach[1])]

    zero_row = jnp.zeros((1, tok), F32)
    info = jnp.concatenate([ids[0], ranks[0], ids[1], ranks[1], zero_row + 1.0, zero_row, zero_row, zero_row], axis=0).astype(BF)
    over = jnp.zeros((1, 1), F32)
    x_val = x_ref[...]
    near[0:tok, :] = x_val
    for way in range(2):
        level = float(half) - iota_f((8, tok), 0)
        member = as_one((reach[way] == level) & (level > 0.5))
        inner = dot(member.astype(BF), upper)
        sizes = jnp.sum(member, axis=1, keepdims=True)
        place = zero_row - 1.0
        total = jnp.zeros((1, 1), F32)
        for lev in range(half):
            place = jnp.where(member[lev:lev + 1] > 0.5, inner[lev:lev + 1] + total, place)
            total = total + sizes[lev:lev + 1]
            over = jnp.maximum(over, as_one(total > float(bounds[lev + 1])))
        pick = as_one(iota_f((HOP_ROWS[0], tok), 0) == place).astype(BF)
        blk[way] = dot(pick, x_val).astype(BF)
        keys = lax.dot_general(info, pick, (((1,), (1,)), ((), ())), preferred_element_type=F32)
        for c in range(2):
            key = base + keys[2 * c:2 * c + 1] * float(src_cap) + keys[2 * c + 1:2 * c + 2]
            key_send[way, c:c + 1, 0:HOP_ROWS[0]] = jnp.where(keys[4:5] > 0.5, key, -1.0)
    for c in range(2):
        key_near[0, c:c + 1, :] = base + ids[c] * float(src_cap) + ranks[c]

    best, runner, first, second = top_two(logits, 1)
    chosen = as_one(first | second)
    lanes = 128
    count_send[...] = jnp.concatenate(
        [jnp.sum(chosen, axis=0, keepdims=True), jnp.zeros((1, lanes - experts), F32) + over], axis=1)
    count_all[me] = count_send[...]
    rank = dot(as_one(row_i > col_i).astype(BF), chosen.astype(BF))
    lane_e = iota_f((tok, experts), 1)
    norm = jnp.sum(jnp.exp(logits - best), axis=1, keepdims=True)
    gates = (1.0 / norm, jnp.exp(runner - best) / norm)
    tkeys = [jnp.sum(jnp.where(mask, lane_e * float(src_cap) + rank, 0.0), axis=1, keepdims=True) for mask in (first, second)]

    pl.semaphore_wait(barrier, n_ep - 1 + n_dp - 1)

    def remote(src, dst, send, recv, to):
        return pltpu.make_async_remote_copy(
            src_ref=src, dst_ref=dst, send_sem=send, recv_sem=recv, device_id=to, device_id_type=MESH)

    def count_copy(step):
        return remote(count_send, count_all.at[me], count_ssem.at[step], count_rsem.at[step],
                      {'ep': lax.rem(me + step, n_ep)})

    def ring_rows(way, hop, lo, size):
        return hop_bufs[hop].at[pl.ds(way * HOP_ROWS[hop] + lo, size)]

    def hop_copy(way, hop, part):
        lo, size = bounds[part], bounds[part + 1] - bounds[part]
        src = blk.at[way, pl.ds(lo, size)] if hop == 0 else ring_rows(way, hop - 1, lo, size)
        return remote(src, ring_rows(way, hop, lo, size), send_sem.at[way, hop, part], recv_sem.at[way, hop, part],
                      {'ep': nxt[way]})

    def key_copy(way, hop):
        src = key_send.at[way] if hop == 0 else key_ring.at[way, hop - 1]
        return remote(src, key_ring.at[way, hop], ksend_sem.at[way, hop], krecv_sem.at[way, hop], {'ep': nxt[way]})

    def mirror_copy(way, hop):
        return remote(ring_rows(way, hop, 0, HOP_ROWS[hop]), ring_rows(2 + way, hop, 0, HOP_ROWS[hop]),
                      mir_send.at[way, hop], mir_recv.at[way, hop], {'ep': other})

    def key_mirror(way, hop):
        return remote(key_ring.at[way, hop], key_mir.at[way, hop], kmir_send.at[way, hop], kmir_recv.at[way, hop],
                      {'ep': other})

    px_copy = remote(x_ref, near.at[pl.ds(tok, tok)], px_sem.at[0], px_sem.at[1], {'ep': other})
    kpx_copy = remote(key_near.at[0], key_near.at[1], kpx_sem.at[0], kpx_sem.at[1], {'ep': other})

    def parts_of(hop):
        return [p for p in range(half - hop) if bounds[p + 1] > bounds[p]]

    for way in range(2):
        hop_copy(way, 0, 0).start()
    for step in range(1, n_ep):
        count_copy(step).start()
    px_copy.start()
    kpx_copy.start()
    for way in range(2):
        key_copy(way, 0).start()
        for part in parts_of(0)[1:]:
            hop_copy(way, 0, part).start()

    for step in range(1, n_ep):
        count_copy(step).wait_recv()
    count_rows = jnp.concatenate([count_all[s] for s in range(n_ep)], axis=0)
    counts = count_rows[:, 0:experts]
    over = jnp.max(jnp.max(count_rows[:, experts:lanes], axis=1, keepdims=True), axis=0, keepdims=True)
    tri = as_one(lax.broadcasted_iota(jnp.int32, (n_ep, n_ep), 1) <= lax.broadcasted_iota(jnp.int32, (n_ep, n_ep), 0)).astype(BF)
    ends = dot(tri, counts.astype(BF))
    lane_ep = lax.broadcasted_iota(jnp.int32, (n_ep, experts), 1)
    slot = iota_f((n_ep, capacity), 1)
    for el in range(exp_dev):
        mine = lane_ep == me * exp_dev + el
        count_col = jnp.sum(jnp.where(mine, counts, 0.0), axis=1, keepdims=True)
        end_col = jnp.sum(jnp.where(mine, ends, 0.0), axis=1, keepdims=True)
        past = as_one(end_col <= slot)
        src = jnp.sum(past, axis=0, keepdims=True)
        rnk = slot[0:1] - jnp.sum(past * count_col, axis=0, keepdims=True)
        valid = src < float(n_ep)
        e_base = (me * exp_dev + el).astype(F32) * float(src_cap)
        key = jnp.where(valid, src * float(experts * src_cap) + e_base + rnk, -2.0)
        skey[el] = jnp.broadcast_to(key, (128, capacity)).T
        rkeys[el:el + 1, :] = jnp.where(valid, src * float(src_cap) + rnk, -1.0)

    def gather_rows(el, buf, keys, first_time=False):
        want = skey[el][:, 0:1]
        hit = as_one((want == keys[0:1]) | (want == keys[1:2])).astype(BF)
        part = dot(hit, buf[...])
        return part if first_time else acc[el] + part

    def gather_all(buf, keys, first_time=False):
        def body(el, carry):
            acc[el] = gather_rows(el, buf, keys, first_time)
            return carry
        lax.fori_loop(0, exp_dev, body, 0)

    def hop_keys(hop):
        for way in range(2):
            mirror_copy(way, hop).wait_recv()
            key_mirror(way, hop).wait_recv()
        size = HOP_ROWS[hop]
        return jnp.concatenate([keys[way, hop][:, 0:size] for keys in (key_ring, key_mir) for way in range(2)], axis=1)

    px_copy.wait_recv()
    kpx_copy.wait_recv()
    gather_all(near, jnp.concatenate([key_near[0], key_near[1]], axis=1), True)

    for hop in range(half):
        for part in parts_of(hop):
            for way in range(2):
                hop_copy(way, hop, part).wait_recv()
                onward = hop + 1 < half
                if onward and part in parts_of(hop + 1):
                    hop_copy(way, hop + 1, part).start()
                if part == 0:
                    key_copy(way, hop).wait_recv()
                    key_mirror(way, hop).start()
                    if onward:
                        key_copy(way, hop + 1).start()
        for way in range(2):
            mirror_copy(way, hop).start()
        if hop + 1 < half:
            gather_all(hop_bufs[hop], hop_keys(hop))
    last_keys = hop_keys(half - 1)

    flag_buf[0] = jnp.broadcast_to(over, (8, 128))

    def flag_copy(step):
        return pltpu.make_async_remote_copy(
            src_ref=flag_buf.at[0], dst_ref=flag_buf.at[step], send_sem=flag_ssem.at[step], recv_sem=flag_rsem.at[step],
            device_id={'dp': lax.rem(my_dp + step, n_dp)}, device_id_type=MESH)

    for step in range(1, n_dp):
        flag_copy(step).start()

    def ret_copy(el, step):
        dest = lax.rem(me + step, n_ep)
        return pltpu.make_async_remote_copy(
            src_ref=ret.at[el, pl.ds(pl.multiple_of(dest * src_cap, src_cap), src_cap)],
            dst_ref=back.at[el, pl.ds(pl.multiple_of(me * src_cap, src_cap), src_cap)],
            send_sem=ret_ssem.at[el, step], recv_sem=ret_rsem.at[el, step],
            device_id={'ep': dest}, device_id_type=MESH)

    ret_order = sorted(range(1, n_ep), key=lambda s: -min(s, n_ep - s))

    def expert_body(el, carry):
        spot = lax.rem(el, 2)
        for copy in weight_copies(el):
            copy.wait()
        rows = gather_rows(el, hop_bufs[half - 1], last_keys).astype(BF)
        z_acc[...] = jnp.zeros_like(z_acc)

        def ff_body(tile, inner):
            cols = pl.ds(pl.multiple_of(tile * FF_TILE, FF_TILE), FF_TILE)
            hidden = jax.nn.gelu(dot(rows, w1_buf[spot, :, cols]), approximate=True).astype(BF)
            z_acc[...] += dot(hidden, w2_buf[spot, cols, :])
            return inner

        lax.fori_loop(0, ff // FF_TILE, ff_body, 0)

        @pl.when(el + 2 < exp_dev)
        def _():
            for copy in weight_copies(el + 2):
                copy.start()

        spread = as_one(iota_f((n_ep * src_cap, capacity), 0) == rkeys[pl.ds(el, 1), :]).astype(BF)
        ret[el] = dot(spread, z_acc[...].astype(BF)).astype(BF)
        for step in ret_order:
            ret_copy(el, step).start()
        own = pl.ds(pl.multiple_of(me * src_cap, src_cap), src_cap)
        back[el, own, :] = ret[el, own, :]
        return carry

    lax.fori_loop(0, exp_dev, expert_body, 0)

    slot_i = lax.broadcasted_iota(jnp.int32, (1, n_ep * src_cap), 1)
    slot_src = lax.div(slot_i, src_cap)
    y_acc[...] = jnp.zeros_like(y_acc)

    def mix_body(el, carry):
        for step in ret_order:
            ret_copy(el, step).wait_recv()
        slot_key = ((slot_src * exp_dev + el) * src_cap + (slot_i - slot_src * src_cap)).astype(F32)
        for c in range(2):
            hit = as_one(tkeys[c] == slot_key).astype(BF)
            y_acc[...] += gates[c] * dot(hit, back[el])
        return carry

    lax.fori_loop(0, exp_dev, mix_body, 0)
    out_ref[...] = (x_ref[...].astype(F32) + y_acc[...]).astype(BF)

    worst = flag_buf[0]
    for step in range(1, n_dp):
        flag_copy(step).wait_recv()
        worst = jnp.maximum(worst, flag_buf[step])
    flag_ref[0] = jnp.max(worst)

    px_copy.wait_send()
    kpx_copy.wait_send()
    for step in range(1, n_ep):
        count_copy(step).wait_send()
    for step in range(1, n_dp):
        flag_copy(step).wait_send()
    for hop in range(half):
        for way in range(2):
            mirror_copy(way, hop).wait_send()
            key_mirror(way, hop).wait_send()
            key_copy(way, hop).wait_send()
            for part in parts_of(hop):
                hop_copy(way, hop, part).wait_send()
    for el in range(exp_dev):
        for step in ret_order:
            ret_copy(el, step).wait_send()


def plain_step(n_ep, x_rows, logits, w_in, w_out):
    tok_dev, d_model = x_rows.shape
    experts = logits.shape[1]
    exp_dev = w_in.shape[0]
    capacity = CAP_FACTOR * tok_dev * n_ep // experts
    src_cap = 4 * tok_dev // experts
    my_index = lax.axis_index('ep')
    gate_probs = jax.nn.softmax(logits, axis=-1)
    top_vals, top_ids = lax.top_k(logits, 2)
    chosen = (logits >= top_vals[:, 1:2]).astype(jnp.int32)
    local_before = jnp.cumsum(chosen, axis=0) - chosen
    local_counts = jnp.sum(chosen, axis=0).astype(jnp.float32)
    all_counts = lax.all_gather(local_counts, 'ep').astype(jnp.int32)
    dev_offsets = jnp.cumsum(all_counts, axis=0) - all_counts
    local_pos = jnp.take_along_axis(local_before, top_ids, axis=1)
    kept_mask = local_pos + jnp.take(dev_offsets[my_index], top_ids) < capacity
    send_row = jnp.where(kept_mask, top_ids * src_cap + local_pos, experts * src_cap)
    tok_ids = jnp.broadcast_to(jnp.arange(tok_dev, dtype=jnp.int32)[:, None], (tok_dev, 2))
    slot_tok = jnp.full((experts * src_cap,), tok_dev, jnp.int32).at[send_row.reshape(-1)].set(tok_ids.reshape(-1), mode='drop')
    send_buf = jnp.take(x_rows, slot_tok, axis=0, mode='fill', fill_value=0)
    recv_buf = lax.all_to_all(send_buf, 'ep', 0, 0, tiled=True)

    own_counts = lax.dynamic_slice_in_dim(all_counts, my_index * exp_dev, exp_dev, axis=1)
    own_offsets = lax.dynamic_slice_in_dim(dev_offsets, my_index * exp_dev, exp_dev, axis=1)
    kept_counts = jnp.minimum(jnp.maximum(capacity - own_offsets, 0), own_counts)
    slot_ends = (own_offsets + kept_counts).T
    cap_ids = jnp.arange(capacity, dtype=jnp.int32)
    below_mask = slot_ends[:, None, :] <= cap_ids[None, :, None]
    src_dev = jnp.sum(below_mask.astype(jnp.int32), axis=2)
    slot_start = jnp.sum(jnp.where(below_mask, kept_counts.T[:, None, :], 0), axis=2)
    exp_local = jnp.arange(exp_dev, dtype=jnp.int32)
    recv_row = (src_dev * exp_dev + exp_local[:, None]) * src_cap + cap_ids[None, :] - slot_start
    recv_row = jnp.where(src_dev < n_ep, recv_row, n_ep * exp_dev * src_cap)
    expert_rows = jnp.take(recv_buf, recv_row.reshape(-1), axis=0, mode='fill', fill_value=0).reshape(exp_dev, capacity, d_model)
    hidden = jax.nn.gelu(jnp.einsum('ecd,edf->ecf', expert_rows, w_in, preferred_element_type=jnp.float32), approximate=True).astype(jnp.bfloat16)
    expert_out = jnp.einsum('ecf,efd->ecd', hidden, w_out, preferred_element_type=jnp.float32).astype(jnp.bfloat16).reshape(exp_dev * capacity, d_model)

    src_slots = jnp.arange(src_cap, dtype=jnp.int32)
    back_row = exp_local[None, :, None] * capacity + own_offsets[:, :, None] + src_slots[None, None, :]
    back_row = jnp.where(src_slots[None, None, :] < kept_counts[:, :, None], back_row, exp_dev * capacity)
    back_buf = jnp.take(expert_out, back_row.reshape(-1), axis=0, mode='fill', fill_value=0)
    ret_buf = lax.all_to_all(back_buf, 'ep', 0, 0, tiled=True)

    rows_back = jnp.take(ret_buf, send_row, axis=0, mode='fill', fill_value=0)
    pick_gate = jnp.take_along_axis(gate_probs, top_ids, axis=1)
    mix_sum = jnp.sum(pick_gate[:, :, None] * rows_back.astype(jnp.float32), axis=1)
    return (x_rows.astype(jnp.float32) + mix_sum).astype(jnp.bfloat16)


def solution(mesh):
    n_ep = mesh.shape['ep']
    n_dp = mesh.shape['dp']
    row_spec = P(('dp', 'ep'), None)
    expert_spec = P('ep', None, None)

    def local_step(x_rows, logits, w_in, w_out):
        tok, d_model = x_rows.shape
        experts = logits.shape[1]
        exp_dev, _, ff = w_in.shape
        capacity = CAP_FACTOR * tok * n_ep // experts
        src_cap = 4 * tok // experts
        half = n_ep // 4
        vmem = pl.BlockSpec(memory_space=pltpu.VMEM)
        smem = pl.BlockSpec(memory_space=pltpu.SMEM)
        hbm = pl.BlockSpec(memory_space=pl.ANY)
        dma = pltpu.SemaphoreType.DMA
        out, flag = pl.pallas_call(
            functools.partial(moe_kernel, n_ep, n_dp, capacity, src_cap),
            out_shape=(jax.ShapeDtypeStruct((tok, d_model), BF), jax.ShapeDtypeStruct((1,), F32)),
            in_specs=[vmem, vmem, hbm, hbm],
            out_specs=(vmem, smem),
            scratch_shapes=[
                pltpu.VMEM((2, d_model, ff), BF),
                pltpu.VMEM((2, ff, d_model), BF),
                pltpu.VMEM((2, HOP_ROWS[0], d_model), BF),
                pltpu.VMEM((2 * tok, d_model), BF),
                *[pltpu.VMEM((4 * rows, d_model), BF) for rows in HOP_ROWS],
                pltpu.VMEM((2, 2, tok), F32),
                pltpu.VMEM((2, 2, tok), F32),
                pltpu.VMEM((2, half, 2, tok), F32),
                pltpu.VMEM((2, half, 2, tok), F32),
                pltpu.VMEM((1, 128), F32),
                pltpu.VMEM((n_ep, 1, 128), F32),
                pltpu.VMEM((exp_dev, capacity, d_model), F32),
                pltpu.VMEM((capacity, d_model), F32),
                pltpu.VMEM((exp_dev, capacity, 128), F32),
                pltpu.VMEM((8, capacity), F32),
                pltpu.VMEM((exp_dev, n_ep * src_cap, d_model), BF),
                pltpu.VMEM((exp_dev, n_ep * src_cap, d_model), BF),
                pltpu.VMEM((tok, d_model), F32),
                pltpu.VMEM((n_dp, 8, 128), F32),
                dma((2, 2)),
                dma((2, half, half)), dma((2, half, half)),
                dma((2, half)), dma((2, half)),
                dma((2,)),
                dma((2, half)), dma((2, half)), dma((2, half)), dma((2, half)),
                dma((2,)),
                dma((n_ep,)), dma((n_ep,)),
                dma((exp_dev, n_ep)), dma((exp_dev, n_ep)),
                dma((n_dp,)), dma((n_dp,)),
            ],
            compiler_params=pltpu.CompilerParams(
                collective_id=0, has_side_effects=True, vmem_limit_bytes=62 * 1024 * 1024),
            name='moe_layer',
        )(x_rows, logits.T, w_in, w_out)
        return lax.cond(flag[0] > 0.0, functools.partial(plain_step, n_ep), lambda *_: out, x_rows, logits, w_in, w_out)

    return jax.shard_map(local_step, mesh=mesh, in_specs=(row_spec, row_spec, expert_spec, expert_spec), out_specs=row_spec, check_vma=False)
```

```python
import functools

import jax
import jax.numpy as jnp
from jax import lax
from jax.experimental import pallas as pl
from jax.experimental.pallas import tpu as pltpu
from jax.sharding import PartitionSpec as P

CAP_FACTOR = 2
HOP_ROWS = (464, 384, 304, 160)
FF_TILE = 512
BF = jnp.bfloat16
F32 = jnp.float32
MESH = pl.DeviceIdType.MESH


def top_two(vals, axis):
    best = jnp.max(vals, axis=axis, keepdims=True)
    first = vals == best
    rest = jnp.where(first, -jnp.inf, vals)
    runner = jnp.max(rest, axis=axis, keepdims=True)
    return best, runner, first, rest == runner


def as_one(mask):
    return jnp.where(mask, 1.0, 0.0)


def iota_f(shape, dim):
    return lax.broadcasted_iota(jnp.int32, shape, dim).astype(F32)


def dot(lhs, rhs):
    return jnp.dot(lhs, rhs, preferred_element_type=F32)


def moe_kernel(n_ep, n_dp, capacity, src_cap, x_ref, lg_ref, w1_hbm, w2_hbm, out_ref, flag_ref,
               w1_buf, w2_buf, blk, near, hops_a, hops_b, hops_c, hops_d, key_send, key_near, key_ring, key_mir,
               count_send, count_all, acc, z_acc, skey, rkeys, ret, back, flag_buf,
               w_sem, send_sem, recv_sem, mir_send, mir_recv, px_sem, ksend_sem, krecv_sem, kmir_send, kmir_recv,
               kpx_sem, count_ssem, count_rsem, ret_ssem, ret_rsem, flag_ssem, flag_rsem):
    tok, d_model = x_ref.shape
    experts = lg_ref.shape[0]
    exp_dev = experts // n_ep
    ff = w1_buf.shape[2]
    n_chip = n_ep // 2
    half = n_chip // 2
    me = lax.axis_index('ep')
    my_dp = lax.axis_index('dp')
    chip = lax.div(me, 2)
    core = lax.rem(me, 2)
    other = chip * 2 + 1 - core
    nxt = (lax.rem(chip + 1, n_chip) * 2 + core, lax.rem(chip + n_chip - 1, n_chip) * 2 + core)
    bounds = (0,) + HOP_ROWS[::-1]
    hop_bufs = (hops_a, hops_b, hops_c, hops_d)

    def weight_copies(el):
        slot = lax.rem(el, 2)
        return (pltpu.make_async_copy(w1_hbm.at[el], w1_buf.at[slot], w_sem.at[slot, 0]),
                pltpu.make_async_copy(w2_hbm.at[el], w2_buf.at[slot], w_sem.at[slot, 1]))

    for el in range(min(2, exp_dev)):
        for copy in weight_copies(el):
            copy.start()

    barrier = pltpu.get_barrier_semaphore()
    for step in range(1, n_ep):
        pl.semaphore_signal(barrier, inc=1, device_id={'ep': lax.rem(me + step, n_ep)}, device_id_type=MESH)
    for step in range(1, n_dp):
        pl.semaphore_signal(barrier, inc=1, device_id={'dp': lax.rem(my_dp + step, n_dp)}, device_id_type=MESH)

    logits_t = lg_ref[...]
    logits = logits_t.T
    _, _, first_t, second_t = top_two(logits_t, 0)
    row_i = lax.broadcasted_iota(jnp.int32, (tok, tok), 0)
    col_i = lax.broadcasted_iota(jnp.int32, (tok, tok), 1)
    upper = as_one(row_i < col_i).astype(BF)
    e_ids = iota_f((experts, tok), 0)
    ids = [jnp.sum(jnp.where(mask, e_ids, 0.0), axis=0, keepdims=True) for mask in (first_t, second_t)]
    chip_f = chip.astype(F32)
    base = me.astype(F32) * float(experts * src_cap)
    reach = [jnp.zeros((1, tok), F32), jnp.zeros((1, tok), F32)]
    opposite = jnp.zeros((1, tok), jnp.bool_)
    for expert_id in ids:
        delta = jnp.floor((expert_id + 0.5) * (1.0 / (2 * exp_dev))) - chip_f
        delta = jnp.where(delta < 0.0, delta + n_chip, delta)
        reach[0] = jnp.maximum(reach[0], jnp.where(delta < half, delta, 0.0))
        reach[1] = jnp.maximum(reach[1], jnp.where(delta > half, n_chip - delta, 0.0))
        opposite = opposite | (delta == half)
    odd = lax.rem(lax.broadcasted_iota(jnp.int32, (1, tok), 1) + core, 2) == 0
    forward = (reach[0] > reach[1]) | ((reach[0] == reach[1]) & odd)
    reach = [jnp.where(opposite & forward, float(half), reach[0]),
             jnp.where(opposite & jnp.logical_not(forward), float(half), reach[1])]

    zero_row = jnp.zeros((1, tok), F32)
    over = jnp.zeros((1, 1), F32)
    places = []
    for way in range(2):
        level = float(half) - iota_f((8, tok), 0)
        member = as_one((reach[way] == level) & (level > 0.5))
        inner = dot(member.astype(BF), upper)
        sizes = jnp.sum(member, axis=1, keepdims=True)
        place = zero_row - 1.0
        total = jnp.zeros((1, 1), F32)
        for lev in range(half):
            place = jnp.where(member[lev:lev + 1] > 0.5, inner[lev:lev + 1] + total, place)
            total = total + sizes[lev:lev + 1]
            over = jnp.maximum(over, as_one(total > float(bounds[lev + 1])))
        places.append(place)

    x_val = x_ref[...]

    def pick_rows(way, lo, size):
        return as_one(iota_f((size, tok), 0) + float(lo) == places[way]).astype(BF)

    def pack_rows(way, lo, size):
        blk[way, lo:lo + size, :] = dot(pick_rows(way, lo, size), x_val).astype(BF)

    for way in range(2):
        pack_rows(way, 0, bounds[1])

    def remote(src, dst, send, recv, to):
        return pltpu.make_async_remote_copy(
            src_ref=src, dst_ref=dst, send_sem=send, recv_sem=recv, device_id=to, device_id_type=MESH)

    def count_copy(step):
        return remote(count_send, count_all.at[me], count_ssem.at[step], count_rsem.at[step],
                      {'ep': lax.rem(me + step, n_ep)})

    def ring_rows(way, hop, lo, size):
        return hop_bufs[hop].at[pl.ds(way * HOP_ROWS[hop] + lo, size)]

    def hop_copy(way, hop, part):
        lo, size = bounds[part], bounds[part + 1] - bounds[part]
        src = blk.at[way, pl.ds(lo, size)] if hop == 0 else ring_rows(way, hop - 1, lo, size)
        return remote(src, ring_rows(way, hop, lo, size), send_sem.at[way, hop, part], recv_sem.at[way, hop, part],
                      {'ep': nxt[way]})

    def key_copy(way, hop):
        src = key_send.at[way] if hop == 0 else key_ring.at[way, hop - 1]
        return remote(src, key_ring.at[way, hop], ksend_sem.at[way, hop], krecv_sem.at[way, hop], {'ep': nxt[way]})

    def mirror_copy(way, hop):
        return remote(ring_rows(way, hop, 0, HOP_ROWS[hop]), ring_rows(2 + way, hop, 0, HOP_ROWS[hop]),
                      mir_send.at[way, hop], mir_recv.at[way, hop], {'ep': other})

    def key_mirror(way, hop):
        return remote(key_ring.at[way, hop], key_mir.at[way, hop], kmir_send.at[way, hop], kmir_recv.at[way, hop],
                      {'ep': other})

    px_copy = remote(x_ref, near.at[pl.ds(tok, tok)], px_sem.at[0], px_sem.at[1], {'ep': other})
    kpx_copy = remote(key_near.at[0], key_near.at[1], kpx_sem.at[0], kpx_sem.at[1], {'ep': other})

    def parts_of(hop):
        return [p for p in range(half - hop) if bounds[p + 1] > bounds[p]]

    pl.semaphore_wait(barrier, n_ep - 1 + n_dp - 1)
    for way in range(2):
        hop_copy(way, 0, 0).start()
    px_copy.start()

    rank_t = dot(as_one(first_t | second_t).astype(BF), upper)
    ranks = [jnp.sum(jnp.where(mask, rank_t, 0.0), axis=0, keepdims=True) for mask in (first_t, second_t)]
    info = jnp.concatenate([ids[0], ranks[0], ids[1], ranks[1], zero_row + 1.0, zero_row, zero_row, zero_row], axis=0).astype(BF)
    for way in range(2):
        keys = lax.dot_general(info, pick_rows(way, 0, HOP_ROWS[0]), (((1,), (1,)), ((), ())), preferred_element_type=F32)
        for c in range(2):
            key = base + keys[2 * c:2 * c + 1] * float(src_cap) + keys[2 * c + 1:2 * c + 2]
            key_send[way, c:c + 1, 0:HOP_ROWS[0]] = jnp.where(keys[4:5] > 0.5, key, -1.0)
    for c in range(2):
        key_near[0, c:c + 1, :] = base + ids[c] * float(src_cap) + ranks[c]
    near[0:tok, :] = x_val
    for way in range(2):
        pack_rows(way, bounds[1], HOP_ROWS[0] - bounds[1])
    for way in range(2):
        key_copy(way, 0).start()
        for part in parts_of(0)[1:]:
            hop_copy(way, 0, part).start()
    kpx_copy.start()

    best, runner, first, second = top_two(logits, 1)
    chosen = as_one(first | second)
    lanes = 128
    count_send[...] = jnp.concatenate(
        [jnp.sum(chosen, axis=0, keepdims=True), jnp.zeros((1, lanes - experts), F32) + over], axis=1)
    count_all[me] = count_send[...]
    rank = dot(as_one(row_i > col_i).astype(BF), chosen.astype(BF))
    lane_e = iota_f((tok, experts), 1)
    norm = jnp.sum(jnp.exp(logits - best), axis=1, keepdims=True)
    gates = (1.0 / norm, jnp.exp(runner - best) / norm)
    tkeys = [jnp.sum(jnp.where(mask, lane_e * float(src_cap) + rank, 0.0), axis=1, keepdims=True) for mask in (first, second)]

    for step in range(1, n_ep):
        count_copy(step).start()

    for step in range(1, n_ep):
        count_copy(step).wait_recv()
    count_rows = jnp.concatenate([count_all[s] for s in range(n_ep)], axis=0)
    counts = count_rows[:, 0:experts]
    over = jnp.max(jnp.max(count_rows[:, experts:lanes], axis=1, keepdims=True), axis=0, keepdims=True)
    tri = as_one(lax.broadcasted_iota(jnp.int32, (n_ep, n_ep), 1) <= lax.broadcasted_iota(jnp.int32, (n_ep, n_ep), 0)).astype(BF)
    ends = dot(tri, counts.astype(BF))
    lane_ep = lax.broadcasted_iota(jnp.int32, (n_ep, experts), 1)
    slot = iota_f((n_ep, capacity), 1)
    for el in range(exp_dev):
        mine = lane_ep == me * exp_dev + el
        count_col = jnp.sum(jnp.where(mine, counts, 0.0), axis=1, keepdims=True)
        end_col = jnp.sum(jnp.where(mine, ends, 0.0), axis=1, keepdims=True)
        past = as_one(end_col <= slot)
        src = jnp.sum(past, axis=0, keepdims=True)
        rnk = slot[0:1] - jnp.sum(past * count_col, axis=0, keepdims=True)
        valid = src < float(n_ep)
        e_base = (me * exp_dev + el).astype(F32) * float(src_cap)
        key = jnp.where(valid, src * float(experts * src_cap) + e_base + rnk, -2.0)
        skey[el] = jnp.broadcast_to(key, (128, capacity)).T
        rkeys[el:el + 1, :] = jnp.where(valid, src * float(src_cap) + rnk, -1.0)

    def gather_rows(el, buf, keys, first_time=False):
        want = skey[el][:, 0:1]
        hit = as_one((want == keys[0:1]) | (want == keys[1:2])).astype(BF)
        part = dot(hit, buf[...])
        return part if first_time else acc[el] + part

    def gather_some(lo, hi, buf, keys, first_time=False):
        def body(el, carry):
            acc[el] = gather_rows(el, buf, keys, first_time)
            return carry
        lax.fori_loop(lo, hi, body, 0)

    def hop_keys(hop):
        for way in range(2):
            mirror_copy(way, hop).wait_recv()
            key_mirror(way, hop).wait_recv()
        size = HOP_ROWS[hop]
        return jnp.concatenate([keys[way, hop][:, 0:size] for keys in (key_ring, key_mir) for way in range(2)], axis=1)

    px_copy.wait_recv()
    kpx_copy.wait_recv()
    gather_some(0, exp_dev, near, jnp.concatenate([key_near[0], key_near[1]], axis=1), True)

    late = None
    for hop in range(half):
        for part in parts_of(hop):
            if part == 1 and late is not None:
                gather_some(exp_dev // 2, exp_dev, *late)
                late = None
            for way in range(2):
                hop_copy(way, hop, part).wait_recv()
                onward = hop + 1 < half
                if onward and part in parts_of(hop + 1):
                    hop_copy(way, hop + 1, part).start()
                if part == 0:
                    key_copy(way, hop).wait_recv()
                    key_mirror(way, hop).start()
                    if onward:
                        key_copy(way, hop + 1).start()
        for way in range(2):
            mirror_copy(way, hop).start()
        if late is not None:
            gather_some(exp_dev // 2, exp_dev, *late)
            late = None
        if hop + 1 < half:
            late = (hop_bufs[hop], hop_keys(hop))
            gather_some(0, exp_dev // 2, *late)
            if hop + 2 == half:
                gather_some(exp_dev // 2, exp_dev, *late)
                late = None
    last_keys = hop_keys(half - 1)

    flag_buf[0] = jnp.broadcast_to(over, (8, 128))

    def flag_copy(step):
        return pltpu.make_async_remote_copy(
            src_ref=flag_buf.at[0], dst_ref=flag_buf.at[step], send_sem=flag_ssem.at[step], recv_sem=flag_rsem.at[step],
            device_id={'dp': lax.rem(my_dp + step, n_dp)}, device_id_type=MESH)

    for step in range(1, n_dp):
        flag_copy(step).start()

    def ret_copy(el, step):
        dest = lax.rem(me + step, n_ep)
        return pltpu.make_async_remote_copy(
            src_ref=ret.at[el, pl.ds(pl.multiple_of(dest * src_cap, src_cap), src_cap)],
            dst_ref=back.at[el, pl.ds(pl.multiple_of(me * src_cap, src_cap), src_cap)],
            send_sem=ret_ssem.at[el, step], recv_sem=ret_rsem.at[el, step],
            device_id={'ep': dest}, device_id_type=MESH)

    ret_order = sorted(range(1, n_ep), key=lambda s: -min(s, n_ep - s))

    def expert_body(el, carry):
        spot = lax.rem(el, 2)
        for copy in weight_copies(el):
            copy.wait()
        rows = gather_rows(el, hop_bufs[half - 1], last_keys).astype(BF)
        z_acc[...] = jnp.zeros_like(z_acc)

        def ff_body(tile, inner):
            cols = pl.ds(pl.multiple_of(tile * FF_TILE, FF_TILE), FF_TILE)
            hidden = jax.nn.gelu(dot(rows, w1_buf[spot, :, cols]), approximate=True).astype(BF)
            z_acc[...] += dot(hidden, w2_buf[spot, cols, :])
            return inner

        lax.fori_loop(0, ff // FF_TILE, ff_body, 0)

        @pl.when(el + 2 < exp_dev)
        def _():
            for copy in weight_copies(el + 2):
                copy.start()

        spread = as_one(iota_f((n_ep * src_cap, capacity), 0) == rkeys[pl.ds(el, 1), :]).astype(BF)
        ret[el] = dot(spread, z_acc[...].astype(BF)).astype(BF)
        for step in ret_order:
            ret_copy(el, step).start()
        own = pl.ds(pl.multiple_of(me * src_cap, src_cap), src_cap)
        back[el, own, :] = ret[el, own, :]
        return carry

    lax.fori_loop(0, exp_dev, expert_body, 0)

    slot_i = lax.broadcasted_iota(jnp.int32, (1, n_ep * src_cap), 1)
    slot_src = lax.div(slot_i, src_cap)
    out_ref[...] = jnp.zeros_like(out_ref)

    def mix_body(el, carry):
        for step in ret_order:
            ret_copy(el, step).wait_recv()
        slot_key = ((slot_src * exp_dev + el) * src_cap + (slot_i - slot_src * src_cap)).astype(F32)
        for c in range(2):
            hit = as_one(tkeys[c] == slot_key).astype(BF)
            out_ref[...] += gates[c] * dot(hit, back[el])
        return carry

    lax.fori_loop(0, exp_dev, mix_body, 0)

    worst = flag_buf[0]
    for step in range(1, n_dp):
        flag_copy(step).wait_recv()
        worst = jnp.maximum(worst, flag_buf[step])
    flag_ref[0] = jnp.max(worst)

    px_copy.wait_send()
    kpx_copy.wait_send()
    for step in range(1, n_ep):
        count_copy(step).wait_send()
    for step in range(1, n_dp):
        flag_copy(step).wait_send()
    for hop in range(half):
        for way in range(2):
            mirror_copy(way, hop).wait_send()
            key_mirror(way, hop).wait_send()
            key_copy(way, hop).wait_send()
            for part in parts_of(hop):
                hop_copy(way, hop, part).wait_send()
    for el in range(exp_dev):
        for step in ret_order:
            ret_copy(el, step).wait_send()


def plain_step(n_ep, x_rows, logits, w_in, w_out):
    tok_dev, d_model = x_rows.shape
    experts = logits.shape[1]
    exp_dev = w_in.shape[0]
    capacity = CAP_FACTOR * tok_dev * n_ep // experts
    src_cap = 4 * tok_dev // experts
    my_index = lax.axis_index('ep')
    gate_probs = jax.nn.softmax(logits, axis=-1)
    top_vals, top_ids = lax.top_k(logits, 2)
    chosen = (logits >= top_vals[:, 1:2]).astype(jnp.int32)
    local_before = jnp.cumsum(chosen, axis=0) - chosen
    local_counts = jnp.sum(chosen, axis=0).astype(jnp.float32)
    all_counts = lax.all_gather(local_counts, 'ep').astype(jnp.int32)
    dev_offsets = jnp.cumsum(all_counts, axis=0) - all_counts
    local_pos = jnp.take_along_axis(local_before, top_ids, axis=1)
    kept_mask = local_pos + jnp.take(dev_offsets[my_index], top_ids) < capacity
    send_row = jnp.where(kept_mask, top_ids * src_cap + local_pos, experts * src_cap)
    tok_ids = jnp.broadcast_to(jnp.arange(tok_dev, dtype=jnp.int32)[:, None], (tok_dev, 2))
    slot_tok = jnp.full((experts * src_cap,), tok_dev, jnp.int32).at[send_row.reshape(-1)].set(tok_ids.reshape(-1), mode='drop')
    send_buf = jnp.take(x_rows, slot_tok, axis=0, mode='fill', fill_value=0)
    recv_buf = lax.all_to_all(send_buf, 'ep', 0, 0, tiled=True)

    own_counts = lax.dynamic_slice_in_dim(all_counts, my_index * exp_dev, exp_dev, axis=1)
    own_offsets = lax.dynamic_slice_in_dim(dev_offsets, my_index * exp_dev, exp_dev, axis=1)
    kept_counts = jnp.minimum(jnp.maximum(capacity - own_offsets, 0), own_counts)
    slot_ends = (own_offsets + kept_counts).T
    cap_ids = jnp.arange(capacity, dtype=jnp.int32)
    below_mask = slot_ends[:, None, :] <= cap_ids[None, :, None]
    src_dev = jnp.sum(below_mask.astype(jnp.int32), axis=2)
    slot_start = jnp.sum(jnp.where(below_mask, kept_counts.T[:, None, :], 0), axis=2)
    exp_local = jnp.arange(exp_dev, dtype=jnp.int32)
    recv_row = (src_dev * exp_dev + exp_local[:, None]) * src_cap + cap_ids[None, :] - slot_start
    recv_row = jnp.where(src_dev < n_ep, recv_row, n_ep * exp_dev * src_cap)
    expert_rows = jnp.take(recv_buf, recv_row.reshape(-1), axis=0, mode='fill', fill_value=0).reshape(exp_dev, capacity, d_model)
    hidden = jax.nn.gelu(jnp.einsum('ecd,edf->ecf', expert_rows, w_in, preferred_element_type=jnp.float32), approximate=True).astype(jnp.bfloat16)
    expert_out = jnp.einsum('ecf,efd->ecd', hidden, w_out, preferred_element_type=jnp.float32).astype(jnp.bfloat16).reshape(exp_dev * capacity, d_model)

    src_slots = jnp.arange(src_cap, dtype=jnp.int32)
    back_row = exp_local[None, :, None] * capacity + own_offsets[:, :, None] + src_slots[None, None, :]
    back_row = jnp.where(src_slots[None, None, :] < kept_counts[:, :, None], back_row, exp_dev * capacity)
    back_buf = jnp.take(expert_out, back_row.reshape(-1), axis=0, mode='fill', fill_value=0)
    ret_buf = lax.all_to_all(back_buf, 'ep', 0, 0, tiled=True)

    rows_back = jnp.take(ret_buf, send_row, axis=0, mode='fill', fill_value=0)
    pick_gate = jnp.take_along_axis(gate_probs, top_ids, axis=1)
    return jnp.sum(pick_gate[:, :, None] * rows_back.astype(jnp.float32), axis=1)


def solution(mesh):
    n_ep = mesh.shape['ep']
    n_dp = mesh.shape['dp']
    row_spec = P(('dp', 'ep'), None)
    expert_spec = P('ep', None, None)

    def local_step(x_rows, logits, w_in, w_out):
        tok, d_model = x_rows.shape
        experts = logits.shape[1]
        exp_dev, _, ff = w_in.shape
        capacity = CAP_FACTOR * tok * n_ep // experts
        src_cap = 4 * tok // experts
        half = n_ep // 4
        vmem = pl.BlockSpec(memory_space=pltpu.VMEM)
        smem = pl.BlockSpec(memory_space=pltpu.SMEM)
        hbm = pl.BlockSpec(memory_space=pl.ANY)
        dma = pltpu.SemaphoreType.DMA
        out, flag = pl.pallas_call(
            functools.partial(moe_kernel, n_ep, n_dp, capacity, src_cap),
            out_shape=(jax.ShapeDtypeStruct((tok, d_model), F32), jax.ShapeDtypeStruct((1,), F32)),
            in_specs=[vmem, vmem, hbm, hbm],
            out_specs=(vmem, smem),
            scratch_shapes=[
                pltpu.VMEM((2, d_model, ff), BF),
                pltpu.VMEM((2, ff, d_model), BF),
                pltpu.VMEM((2, HOP_ROWS[0], d_model), BF),
                pltpu.VMEM((2 * tok, d_model), BF),
                *[pltpu.VMEM((4 * rows, d_model), BF) for rows in HOP_ROWS],
                pltpu.VMEM((2, 2, tok), F32),
                pltpu.VMEM((2, 2, tok), F32),
                pltpu.VMEM((2, half, 2, tok), F32),
                pltpu.VMEM((2, half, 2, tok), F32),
                pltpu.VMEM((1, 128), F32),
                pltpu.VMEM((n_ep, 1, 128), F32),
                pltpu.VMEM((exp_dev, capacity, d_model), F32),
                pltpu.VMEM((capacity, d_model), F32),
                pltpu.VMEM((exp_dev, capacity, 128), F32),
                pltpu.VMEM((8, capacity), F32),
                pltpu.VMEM((exp_dev, n_ep * src_cap, d_model), BF),
                pltpu.VMEM((exp_dev, n_ep * src_cap, d_model), BF),
                pltpu.VMEM((n_dp, 8, 128), F32),
                dma((2, 2)),
                dma((2, half, half)), dma((2, half, half)),
                dma((2, half)), dma((2, half)),
                dma((2,)),
                dma((2, half)), dma((2, half)), dma((2, half)), dma((2, half)),
                dma((2,)),
                dma((n_ep,)), dma((n_ep,)),
                dma((exp_dev, n_ep)), dma((exp_dev, n_ep)),
                dma((n_dp,)), dma((n_dp,)),
            ],
            compiler_params=pltpu.CompilerParams(
                collective_id=0, has_side_effects=True, vmem_limit_bytes=62 * 1024 * 1024),
            name='moe_layer',
        )(x_rows, logits.T, w_in, w_out)
        mix_sum = lax.cond(flag[0] > 0.0, functools.partial(plain_step, n_ep), lambda *_: out, x_rows, logits, w_in, w_out)
        return (x_rows.astype(F32) + mix_sum).astype(BF)

    return jax.shard_map(local_step, mesh=mesh, in_specs=(row_spec, row_spec, expert_spec, expert_spec), out_specs=row_spec, check_vma=False)
```

```python
import functools

import jax
import jax.numpy as jnp
from jax import lax
from jax.experimental import pallas as pl
from jax.experimental.pallas import tpu as pltpu
from jax.sharding import PartitionSpec as P

CAP_FACTOR = 2
HOP_ROWS = (464, 384, 304, 160)
FF_TILE = 512
BF = jnp.bfloat16
F32 = jnp.float32
MESH = pl.DeviceIdType.MESH


def top_two(vals, axis):
    best = jnp.max(vals, axis=axis, keepdims=True)
    first = vals == best
    rest = jnp.where(first, -jnp.inf, vals)
    runner = jnp.max(rest, axis=axis, keepdims=True)
    return best, runner, first, rest == runner


def as_one(mask):
    return jnp.where(mask, 1.0, 0.0)


def iota_f(shape, dim):
    return lax.broadcasted_iota(jnp.int32, shape, dim).astype(F32)


def dot(lhs, rhs):
    return jnp.dot(lhs, rhs, preferred_element_type=F32)


def moe_kernel(n_ep, n_dp, capacity, src_cap, x_ref, lg_ref, w1_hbm, w2_hbm, out_ref, flag_ref,
               w1_buf, w2_buf, blk, near, hops_a, hops_b, hops_c, hops_d, key_send, key_near, key_ring, key_mir,
               count_send, count_all, acc, z_acc, skey, rkeys, ret, back, y_acc, flag_buf,
               w_sem, send_sem, recv_sem, mir_send, mir_recv, px_sem, ksend_sem, krecv_sem, kmir_send, kmir_recv,
               kpx_sem, count_ssem, count_rsem, ret_ssem, ret_rsem, flag_ssem, flag_rsem):
    tok, d_model = x_ref.shape
    experts = lg_ref.shape[0]
    exp_dev = experts // n_ep
    ff = w1_buf.shape[2]
    n_chip = n_ep // 2
    half = n_chip // 2
    me = lax.axis_index('ep')
    my_dp = lax.axis_index('dp')
    chip = lax.div(me, 2)
    core = lax.rem(me, 2)
    other = chip * 2 + 1 - core
    nxt = (lax.rem(chip + 1, n_chip) * 2 + core, lax.rem(chip + n_chip - 1, n_chip) * 2 + core)
    bounds = (0,) + HOP_ROWS[::-1]
    hop_bufs = (hops_a, hops_b, hops_c, hops_d)

    def weight_copies(el):
        slot = lax.rem(el, 2)
        return (pltpu.make_async_copy(w1_hbm.at[el], w1_buf.at[slot], w_sem.at[slot, 0]),
                pltpu.make_async_copy(w2_hbm.at[el], w2_buf.at[slot], w_sem.at[slot, 1]))

    for el in range(min(2, exp_dev)):
        for copy in weight_copies(el):
            copy.start()

    barrier = pltpu.get_barrier_semaphore()
    for step in range(1, n_ep):
        pl.semaphore_signal(barrier, inc=1, device_id={'ep': lax.rem(me + step, n_ep)}, device_id_type=MESH)
    for step in range(1, n_dp):
        pl.semaphore_signal(barrier, inc=1, device_id={'dp': lax.rem(my_dp + step, n_dp)}, device_id_type=MESH)

    logits_t = lg_ref[...]
    logits = logits_t.T
    _, _, first_t, second_t = top_two(logits_t, 0)
    row_i = lax.broadcasted_iota(jnp.int32, (tok, tok), 0)
    col_i = lax.broadcasted_iota(jnp.int32, (tok, tok), 1)
    upper = as_one(row_i < col_i).astype(BF)
    e_ids = iota_f((experts, tok), 0)
    ids = [jnp.sum(jnp.where(mask, e_ids, 0.0), axis=0, keepdims=True) for mask in (first_t, second_t)]
    chip_f = chip.astype(F32)
    base = me.astype(F32) * float(experts * src_cap)
    reach = [jnp.zeros((1, tok), F32), jnp.zeros((1, tok), F32)]
    opposite = jnp.zeros((1, tok), jnp.bool_)
    for expert_id in ids:
        delta = jnp.floor((expert_id + 0.5) * (1.0 / (2 * exp_dev))) - chip_f
        delta = jnp.where(delta < 0.0, delta + n_chip, delta)
        reach[0] = jnp.maximum(reach[0], jnp.where(delta < half, delta, 0.0))
        reach[1] = jnp.maximum(reach[1], jnp.where(delta > half, n_chip - delta, 0.0))
        opposite = opposite | (delta == half)
    odd = lax.rem(lax.broadcasted_iota(jnp.int32, (1, tok), 1) + core, 2) == 0
    forward = (reach[0] > reach[1]) | ((reach[0] == reach[1]) & odd)
    reach = [jnp.where(opposite & forward, float(half), reach[0]),
             jnp.where(opposite & jnp.logical_not(forward), float(half), reach[1])]

    zero_row = jnp.zeros((1, tok), F32)
    over = jnp.zeros((1, 1), F32)
    places = []
    for way in range(2):
        level = float(half) - iota_f((8, tok), 0)
        member = as_one((reach[way] == level) & (level > 0.5))
        inner = dot(member.astype(BF), upper)
        sizes = jnp.sum(member, axis=1, keepdims=True)
        place = zero_row - 1.0
        total = jnp.zeros((1, 1), F32)
        for lev in range(half):
            place = jnp.where(member[lev:lev + 1] > 0.5, inner[lev:lev + 1] + total, place)
            total = total + sizes[lev:lev + 1]
            over = jnp.maximum(over, as_one(total > float(bounds[lev + 1])))
        places.append(place)

    x_val = x_ref[...]

    def pick_rows(way, lo, size):
        return as_one(iota_f((size, tok), 0) + float(lo) == places[way]).astype(BF)

    def pack_rows(way, lo, size):
        blk[way, lo:lo + size, :] = dot(pick_rows(way, lo, size), x_val).astype(BF)

    lanes = 128
    chosen_t = as_one(first_t | second_t).astype(BF)
    tally = lax.dot_general(jnp.ones((8, tok), BF), chosen_t, (((1,), (1,)), ((), ())), preferred_element_type=F32)
    count_send[...] = jnp.concatenate([tally[0:1], jnp.zeros((1, lanes - experts), F32) + over], axis=1)
    count_all[me] = count_send[...]
    for way in range(2):
        pack_rows(way, 0, bounds[1])

    def remote(src, dst, send, recv, to):
        return pltpu.make_async_remote_copy(
            src_ref=src, dst_ref=dst, send_sem=send, recv_sem=recv, device_id=to, device_id_type=MESH)

    def count_copy(step):
        return remote(count_send, count_all.at[me], count_ssem.at[step], count_rsem.at[step],
                      {'ep': lax.rem(me + step, n_ep)})

    def ring_rows(way, hop, lo, size):
        return hop_bufs[hop].at[pl.ds(way * HOP_ROWS[hop] + lo, size)]

    def hop_copy(way, hop, part):
        lo, size = bounds[part], bounds[part + 1] - bounds[part]
        src = blk.at[way, pl.ds(lo, size)] if hop == 0 else ring_rows(way, hop - 1, lo, size)
        return remote(src, ring_rows(way, hop, lo, size), send_sem.at[way, hop, part], recv_sem.at[way, hop, part],
                      {'ep': nxt[way]})

    def key_copy(way, hop):
        src = key_send.at[way] if hop == 0 else key_ring.at[way, hop - 1]
        return remote(src, key_ring.at[way, hop], ksend_sem.at[way, hop], krecv_sem.at[way, hop], {'ep': nxt[way]})

    def mirror_copy(way, hop):
        return remote(ring_rows(way, hop, 0, HOP_ROWS[hop]), ring_rows(2 + way, hop, 0, HOP_ROWS[hop]),
                      mir_send.at[way, hop], mir_recv.at[way, hop], {'ep': other})

    def key_mirror(way, hop):
        return remote(key_ring.at[way, hop], key_mir.at[way, hop], kmir_send.at[way, hop], kmir_recv.at[way, hop],
                      {'ep': other})

    px_copy = remote(x_ref, near.at[pl.ds(tok, tok)], px_sem.at[0], px_sem.at[1], {'ep': other})
    kpx_copy = remote(key_near.at[0], key_near.at[1], kpx_sem.at[0], kpx_sem.at[1], {'ep': other})

    def parts_of(hop):
        return [p for p in range(half - hop) if bounds[p + 1] > bounds[p]]

    pl.semaphore_wait(barrier, n_ep - 1 + n_dp - 1)
    for step in range(1, n_ep):
        count_copy(step).start()
    for way in range(2):
        hop_copy(way, 0, 0).start()
    px_copy.start()
    for way in range(2):
        pack_rows(way, bounds[1], HOP_ROWS[0] - bounds[1])
    for part in parts_of(0)[1:]:
        for way in range(2):
            hop_copy(way, 0, part).start()

    rank_t = dot(chosen_t, upper)
    ranks = [jnp.sum(jnp.where(mask, rank_t, 0.0), axis=0, keepdims=True) for mask in (first_t, second_t)]
    info = jnp.concatenate([ids[0], ranks[0], ids[1], ranks[1], zero_row + 1.0, zero_row, zero_row, zero_row], axis=0).astype(BF)
    place_cols = jnp.concatenate(places + [zero_row] * 6, axis=0).T
    for way in range(2):
        pick_t = as_one(iota_f((tok, HOP_ROWS[0]), 1) == place_cols[:, way:way + 1]).astype(BF)
        keys = dot(info, pick_t)
        for c in range(2):
            key = base + keys[2 * c:2 * c + 1] * float(src_cap) + keys[2 * c + 1:2 * c + 2]
            key_send[way, c:c + 1, 0:HOP_ROWS[0]] = jnp.where(keys[4:5] > 0.5, key, -1.0)
        key_copy(way, 0).start()
    for c in range(2):
        key_near[0, c:c + 1, :] = base + ids[c] * float(src_cap) + ranks[c]
    kpx_copy.start()
    near[0:tok, :] = x_val

    best, runner, first, second = top_two(logits, 1)
    chosen = as_one(first | second)
    rank = dot(as_one(row_i > col_i).astype(BF), chosen.astype(BF))
    lane_e = iota_f((tok, experts), 1)
    norm = jnp.sum(jnp.exp(logits - best), axis=1, keepdims=True)
    gates = (1.0 / norm, jnp.exp(runner - best) / norm)
    tkeys = [jnp.sum(jnp.where(mask, lane_e * float(src_cap) + rank, 0.0), axis=1, keepdims=True) for mask in (first, second)]

    for step in range(1, n_ep):
        count_copy(step).wait_recv()
    count_rows = jnp.concatenate([count_all[s] for s in range(n_ep)], axis=0)
    counts = count_rows[:, 0:experts]
    over = jnp.max(jnp.max(count_rows[:, experts:lanes], axis=1, keepdims=True), axis=0, keepdims=True)
    tri = as_one(lax.broadcasted_iota(jnp.int32, (n_ep, n_ep), 1) <= lax.broadcasted_iota(jnp.int32, (n_ep, n_ep), 0)).astype(BF)
    ends = dot(tri, counts.astype(BF))
    lane_ep = lax.broadcasted_iota(jnp.int32, (n_ep, experts), 1)
    slot = iota_f((n_ep, capacity), 1)
    for el in range(exp_dev):
        mine = lane_ep == me * exp_dev + el
        count_col = jnp.sum(jnp.where(mine, counts, 0.0), axis=1, keepdims=True)
        end_col = jnp.sum(jnp.where(mine, ends, 0.0), axis=1, keepdims=True)
        past = as_one(end_col <= slot)
        src = jnp.sum(past, axis=0, keepdims=True)
        rnk = slot[0:1] - jnp.sum(past * count_col, axis=0, keepdims=True)
        valid = src < float(n_ep)
        e_base = (me * exp_dev + el).astype(F32) * float(src_cap)
        key = jnp.where(valid, src * float(experts * src_cap) + e_base + rnk, -2.0)
        skey[el] = jnp.broadcast_to(key, (128, capacity)).T
        rkeys[el:el + 1, :] = jnp.where(valid, src * float(src_cap) + rnk, -1.0)

    def gather_rows(el, buf, keys, first_time=False):
        want = skey[el][:, 0:1]
        hit = as_one((want == keys[0:1]) | (want == keys[1:2])).astype(BF)
        part = dot(hit, buf[...])
        return part if first_time else acc[el] + part

    def gather_some(lo, hi, buf, keys, first_time=False):
        def body(el, carry):
            acc[el] = gather_rows(el, buf, keys, first_time)
            return carry
        lax.fori_loop(lo, hi, body, 0)

    def hop_keys(hop):
        for way in range(2):
            mirror_copy(way, hop).wait_recv()
            key_mirror(way, hop).wait_recv()
        size = HOP_ROWS[hop]
        return jnp.concatenate([keys[way, hop][:, 0:size] for keys in (key_ring, key_mir) for way in range(2)], axis=1)

    px_copy.wait_recv()
    kpx_copy.wait_recv()
    gather_some(0, exp_dev, near, jnp.concatenate([key_near[0], key_near[1]], axis=1), True)

    late = None
    for hop in range(half):
        for part in parts_of(hop):
            if part == 1 and late is not None:
                gather_some(exp_dev // 2, exp_dev, *late)
                late = None
            for way in range(2):
                hop_copy(way, hop, part).wait_recv()
                onward = hop + 1 < half
                if onward and part in parts_of(hop + 1):
                    hop_copy(way, hop + 1, part).start()
                if part == 0:
                    key_copy(way, hop).wait_recv()
                    key_mirror(way, hop).start()
                    if onward:
                        key_copy(way, hop + 1).start()
        for way in range(2):
            mirror_copy(way, hop).start()
        if late is not None:
            gather_some(exp_dev // 2, exp_dev, *late)
            late = None
        if hop + 1 < half:
            late = (hop_bufs[hop], hop_keys(hop))
            gather_some(0, exp_dev // 2, *late)
            if hop + 2 == half:
                gather_some(exp_dev // 2, exp_dev, *late)
                late = None
    last_keys = hop_keys(half - 1)

    flag_buf[0] = jnp.broadcast_to(over, (8, 128))

    def flag_copy(step):
        return pltpu.make_async_remote_copy(
            src_ref=flag_buf.at[0], dst_ref=flag_buf.at[step], send_sem=flag_ssem.at[step], recv_sem=flag_rsem.at[step],
            device_id={'dp': lax.rem(my_dp + step, n_dp)}, device_id_type=MESH)

    for step in range(1, n_dp):
        flag_copy(step).start()

    def ret_copy(el, step):
        dest = lax.rem(me + step, n_ep)
        return pltpu.make_async_remote_copy(
            src_ref=ret.at[el, pl.ds(pl.multiple_of(dest * src_cap, src_cap), src_cap)],
            dst_ref=back.at[el, pl.ds(pl.multiple_of(me * src_cap, src_cap), src_cap)],
            send_sem=ret_ssem.at[el, step], recv_sem=ret_rsem.at[el, step],
            device_id={'ep': dest}, device_id_type=MESH)

    ret_order = sorted(range(1, n_ep), key=lambda s: -min(s, n_ep - s))

    def expert_body(el, carry):
        spot = lax.rem(el, 2)
        for copy in weight_copies(el):
            copy.wait()
        rows = gather_rows(el, hop_bufs[half - 1], last_keys).astype(BF)
        z_acc[...] = jnp.zeros_like(z_acc)

        def ff_body(tile, inner):
            cols = pl.ds(pl.multiple_of(tile * FF_TILE, FF_TILE), FF_TILE)
            hidden = jax.nn.gelu(dot(rows, w1_buf[spot, :, cols]), approximate=True).astype(BF)
            z_acc[...] += dot(hidden, w2_buf[spot, cols, :])
            return inner

        lax.fori_loop(0, ff // FF_TILE, ff_body, 0)

        @pl.when(el + 2 < exp_dev)
        def _():
            for copy in weight_copies(el + 2):
                copy.start()

        spread = as_one(iota_f((n_ep * src_cap, capacity), 0) == rkeys[pl.ds(el, 1), :]).astype(BF)
        ret[el] = dot(spread, z_acc[...].astype(BF)).astype(BF)
        for step in ret_order:
            ret_copy(el, step).start()
        own = pl.ds(pl.multiple_of(me * src_cap, src_cap), src_cap)
        back[el, own, :] = ret[el, own, :]
        return carry

    lax.fori_loop(0, exp_dev, expert_body, 0)

    slot_i = lax.broadcasted_iota(jnp.int32, (1, n_ep * src_cap), 1)
    slot_src = lax.div(slot_i, src_cap)
    y_acc[...] = jnp.zeros_like(y_acc)

    def mix_body(el, carry):
        for step in ret_order:
            ret_copy(el, step).wait_recv()
        slot_key = ((slot_src * exp_dev + el) * src_cap + (slot_i - slot_src * src_cap)).astype(F32)
        for c in range(2):
            hit = as_one(tkeys[c] == slot_key).astype(BF)
            y_acc[...] += gates[c] * dot(hit, back[el])
        return carry

    lax.fori_loop(0, exp_dev, mix_body, 0)

    out_ref[...] = (x_ref[...].astype(F32) + y_acc[...]).astype(BF)

    worst = flag_buf[0]
    for step in range(1, n_dp):
        flag_copy(step).wait_recv()
        worst = jnp.maximum(worst, flag_buf[step])
    flag_ref[0] = jnp.max(worst)

    px_copy.wait_send()
    kpx_copy.wait_send()
    for step in range(1, n_ep):
        count_copy(step).wait_send()
    for step in range(1, n_dp):
        flag_copy(step).wait_send()
    for hop in range(half):
        for way in range(2):
            mirror_copy(way, hop).wait_send()
            key_mirror(way, hop).wait_send()
            key_copy(way, hop).wait_send()
            for part in parts_of(hop):
                hop_copy(way, hop, part).wait_send()
    for el in range(exp_dev):
        for step in ret_order:
            ret_copy(el, step).wait_send()


def plain_step(n_ep, x_rows, logits, w_in, w_out):
    tok_dev, d_model = x_rows.shape
    experts = logits.shape[1]
    exp_dev = w_in.shape[0]
    capacity = CAP_FACTOR * tok_dev * n_ep // experts
    src_cap = 4 * tok_dev // experts
    my_index = lax.axis_index('ep')
    gate_probs = jax.nn.softmax(logits, axis=-1)
    top_vals, top_ids = lax.top_k(logits, 2)
    chosen = (logits >= top_vals[:, 1:2]).astype(jnp.int32)
    local_before = jnp.cumsum(chosen, axis=0) - chosen
    local_counts = jnp.sum(chosen, axis=0).astype(jnp.float32)
    all_counts = lax.all_gather(local_counts, 'ep').astype(jnp.int32)
    dev_offsets = jnp.cumsum(all_counts, axis=0) - all_counts
    local_pos = jnp.take_along_axis(local_before, top_ids, axis=1)
    kept_mask = local_pos + jnp.take(dev_offsets[my_index], top_ids) < capacity
    send_row = jnp.where(kept_mask, top_ids * src_cap + local_pos, experts * src_cap)
    tok_ids = jnp.broadcast_to(jnp.arange(tok_dev, dtype=jnp.int32)[:, None], (tok_dev, 2))
    slot_tok = jnp.full((experts * src_cap,), tok_dev, jnp.int32).at[send_row.reshape(-1)].set(tok_ids.reshape(-1), mode='drop')
    send_buf = jnp.take(x_rows, slot_tok, axis=0, mode='fill', fill_value=0)
    recv_buf = lax.all_to_all(send_buf, 'ep', 0, 0, tiled=True)

    own_counts = lax.dynamic_slice_in_dim(all_counts, my_index * exp_dev, exp_dev, axis=1)
    own_offsets = lax.dynamic_slice_in_dim(dev_offsets, my_index * exp_dev, exp_dev, axis=1)
    kept_counts = jnp.minimum(jnp.maximum(capacity - own_offsets, 0), own_counts)
    slot_ends = (own_offsets + kept_counts).T
    cap_ids = jnp.arange(capacity, dtype=jnp.int32)
    below_mask = slot_ends[:, None, :] <= cap_ids[None, :, None]
    src_dev = jnp.sum(below_mask.astype(jnp.int32), axis=2)
    slot_start = jnp.sum(jnp.where(below_mask, kept_counts.T[:, None, :], 0), axis=2)
    exp_local = jnp.arange(exp_dev, dtype=jnp.int32)
    recv_row = (src_dev * exp_dev + exp_local[:, None]) * src_cap + cap_ids[None, :] - slot_start
    recv_row = jnp.where(src_dev < n_ep, recv_row, n_ep * exp_dev * src_cap)
    expert_rows = jnp.take(recv_buf, recv_row.reshape(-1), axis=0, mode='fill', fill_value=0).reshape(exp_dev, capacity, d_model)
    hidden = jax.nn.gelu(jnp.einsum('ecd,edf->ecf', expert_rows, w_in, preferred_element_type=jnp.float32), approximate=True).astype(jnp.bfloat16)
    expert_out = jnp.einsum('ecf,efd->ecd', hidden, w_out, preferred_element_type=jnp.float32).astype(jnp.bfloat16).reshape(exp_dev * capacity, d_model)

    src_slots = jnp.arange(src_cap, dtype=jnp.int32)
    back_row = exp_local[None, :, None] * capacity + own_offsets[:, :, None] + src_slots[None, None, :]
    back_row = jnp.where(src_slots[None, None, :] < kept_counts[:, :, None], back_row, exp_dev * capacity)
    back_buf = jnp.take(expert_out, back_row.reshape(-1), axis=0, mode='fill', fill_value=0)
    ret_buf = lax.all_to_all(back_buf, 'ep', 0, 0, tiled=True)

    rows_back = jnp.take(ret_buf, send_row, axis=0, mode='fill', fill_value=0)
    pick_gate = jnp.take_along_axis(gate_probs, top_ids, axis=1)
    mix_sum = jnp.sum(pick_gate[:, :, None] * rows_back.astype(jnp.float32), axis=1)
    return (x_rows.astype(jnp.float32) + mix_sum).astype(jnp.bfloat16)


def solution(mesh):
    n_ep = mesh.shape['ep']
    n_dp = mesh.shape['dp']
    row_spec = P(('dp', 'ep'), None)
    expert_spec = P('ep', None, None)

    def local_step(x_rows, logits, w_in, w_out):
        tok, d_model = x_rows.shape
        experts = logits.shape[1]
        exp_dev, _, ff = w_in.shape
        capacity = CAP_FACTOR * tok * n_ep // experts
        src_cap = 4 * tok // experts
        half = n_ep // 4
        vmem = pl.BlockSpec(memory_space=pltpu.VMEM)
        smem = pl.BlockSpec(memory_space=pltpu.SMEM)
        hbm = pl.BlockSpec(memory_space=pl.ANY)
        dma = pltpu.SemaphoreType.DMA
        out, flag = pl.pallas_call(
            functools.partial(moe_kernel, n_ep, n_dp, capacity, src_cap),
            out_shape=(jax.ShapeDtypeStruct((tok, d_model), BF), jax.ShapeDtypeStruct((1,), F32)),
            in_specs=[vmem, vmem, hbm, hbm],
            out_specs=(vmem, smem),
            scratch_shapes=[
                pltpu.VMEM((2, d_model, ff), BF),
                pltpu.VMEM((2, ff, d_model), BF),
                pltpu.VMEM((2, HOP_ROWS[0], d_model), BF),
                pltpu.VMEM((2 * tok, d_model), BF),
                *[pltpu.VMEM((4 * rows, d_model), BF) for rows in HOP_ROWS],
                pltpu.VMEM((2, 2, tok), F32),
                pltpu.VMEM((2, 2, tok), F32),
                pltpu.VMEM((2, half, 2, tok), F32),
                pltpu.VMEM((2, half, 2, tok), F32),
                pltpu.VMEM((1, 128), F32),
                pltpu.VMEM((n_ep, 1, 128), F32),
                pltpu.VMEM((exp_dev, capacity, d_model), F32),
                pltpu.VMEM((capacity, d_model), F32),
                pltpu.VMEM((exp_dev, capacity, 128), F32),
                pltpu.VMEM((8, capacity), F32),
                pltpu.VMEM((exp_dev, n_ep * src_cap, d_model), BF),
                pltpu.VMEM((exp_dev, n_ep * src_cap, d_model), BF),
                pltpu.VMEM((tok, d_model), F32),
                pltpu.VMEM((n_dp, 8, 128), F32),
                dma((2, 2)),
                dma((2, half, half)), dma((2, half, half)),
                dma((2, half)), dma((2, half)),
                dma((2,)),
                dma((2, half)), dma((2, half)), dma((2, half)), dma((2, half)),
                dma((2,)),
                dma((n_ep,)), dma((n_ep,)),
                dma((exp_dev, n_ep)), dma((exp_dev, n_ep)),
                dma((n_dp,)), dma((n_dp,)),
            ],
            compiler_params=pltpu.CompilerParams(
                collective_id=0, has_side_effects=True, vmem_limit_bytes=62 * 1024 * 1024),
            name='moe_layer',
        )(x_rows, logits.T, w_in, w_out)
        return lax.cond(flag[0] > 0.0, functools.partial(plain_step, n_ep), lambda *_: out, x_rows, logits, w_in, w_out)

    return jax.shard_map(local_step, mesh=mesh, in_specs=(row_spec, row_spec, expert_spec, expert_spec), out_specs=row_spec, check_vma=False)
```

```python
import functools

import jax
import jax.numpy as jnp
from jax import lax
from jax.experimental import pallas as pl
from jax.experimental.pallas import tpu as pltpu
from jax.sharding import PartitionSpec as P

CAP_FACTOR = 2
HOP_ROWS = (464, 384, 304, 160)
RET_ROWS = (272, 192, 128, 64)
FF_TILE = 512
BF = jnp.bfloat16
F32 = jnp.float32
MESH = pl.DeviceIdType.MESH


def top_two(vals, axis):
    best = jnp.max(vals, axis=axis, keepdims=True)
    first = vals == best
    rest = jnp.where(first, -jnp.inf, vals)
    runner = jnp.max(rest, axis=axis, keepdims=True)
    return best, runner, first, rest == runner


def as_one(mask):
    return jnp.where(mask, 1.0, 0.0)


def iota_f(shape, dim):
    return lax.broadcasted_iota(jnp.int32, shape, dim).astype(F32)


def dot(lhs, rhs):
    return jnp.dot(lhs, rhs, preferred_element_type=F32)


def moe_kernel(n_ep, n_dp, capacity, src_cap, x_ref, lg_ref, w1_hbm, w2_hbm, out_ref, flag_ref,
               w1_buf, w2_buf, blk, near, hops_a, hops_b, hops_c, hops_d, key_send, key_near, key_ring, key_mir,
               count_send, count_all, acc, z_acc, skey, rkeys, ret, back, y_acc, flag_buf,
               z_all, ov_place, ov_blk, ov_a, ov_b, ov_c, ov_d, okey_send, okey_ring, okey_mir,
               w_sem, send_sem, recv_sem, mir_send, mir_recv, px_sem, ksend_sem, krecv_sem, kmir_send, kmir_recv,
               kpx_sem, count_ssem, count_rsem, ret_ssem, ret_rsem, flag_ssem, flag_rsem, z_sem, extra_sem,
               osend_sem, orecv_sem, omir_sem, okey_sem):
    tok, d_model = x_ref.shape
    experts = lg_ref.shape[0]
    exp_dev = experts // n_ep
    ff = w1_buf.shape[2]
    n_chip = n_ep // 2
    half = n_chip // 2
    me = lax.axis_index('ep')
    my_dp = lax.axis_index('dp')
    chip = lax.div(me, 2)
    core = lax.rem(me, 2)
    other = chip * 2 + 1 - core
    nxt = (lax.rem(chip + 1, n_chip) * 2 + core, lax.rem(chip + n_chip - 1, n_chip) * 2 + core)
    bounds = (0,) + HOP_ROWS[::-1]
    hop_bufs = (hops_a, hops_b, hops_c, hops_d)
    ov_bufs = (ov_a, ov_b, ov_c, ov_d)
    ov_bounds = (0,) + RET_ROWS[::-1]
    direct = src_cap // 2
    packed = (n_ep + 2) * direct
    slots = exp_dev * capacity

    def weight_copies(el):
        slot = lax.rem(el, 2)
        return (pltpu.make_async_copy(w1_hbm.at[el], w1_buf.at[slot], w_sem.at[slot, 0]),
                pltpu.make_async_copy(w2_hbm.at[el], w2_buf.at[slot], w_sem.at[slot, 1]))

    for el in range(min(2, exp_dev)):
        for copy in weight_copies(el):
            copy.start()

    barrier = pltpu.get_barrier_semaphore()
    for step in range(1, n_ep):
        pl.semaphore_signal(barrier, inc=1, device_id={'ep': lax.rem(me + step, n_ep)}, device_id_type=MESH)
    for step in range(1, n_dp):
        pl.semaphore_signal(barrier, inc=1, device_id={'dp': lax.rem(my_dp + step, n_dp)}, device_id_type=MESH)

    logits_t = lg_ref[...]
    logits = logits_t.T
    _, _, first_t, second_t = top_two(logits_t, 0)
    row_i = lax.broadcasted_iota(jnp.int32, (tok, tok), 0)
    col_i = lax.broadcasted_iota(jnp.int32, (tok, tok), 1)
    upper = as_one(row_i < col_i).astype(BF)
    e_ids = iota_f((experts, tok), 0)
    ids = [jnp.sum(jnp.where(mask, e_ids, 0.0), axis=0, keepdims=True) for mask in (first_t, second_t)]
    chip_f = chip.astype(F32)
    base = me.astype(F32) * float(experts * src_cap)
    reach = [jnp.zeros((1, tok), F32), jnp.zeros((1, tok), F32)]
    opposite = jnp.zeros((1, tok), jnp.bool_)
    for expert_id in ids:
        delta = jnp.floor((expert_id + 0.5) * (1.0 / (2 * exp_dev))) - chip_f
        delta = jnp.where(delta < 0.0, delta + n_chip, delta)
        reach[0] = jnp.maximum(reach[0], jnp.where(delta < half, delta, 0.0))
        reach[1] = jnp.maximum(reach[1], jnp.where(delta > half, n_chip - delta, 0.0))
        opposite = opposite | (delta == half)
    odd = lax.rem(lax.broadcasted_iota(jnp.int32, (1, tok), 1) + core, 2) == 0
    forward = (reach[0] > reach[1]) | ((reach[0] == reach[1]) & odd)
    reach = [jnp.where(opposite & forward, float(half), reach[0]),
             jnp.where(opposite & jnp.logical_not(forward), float(half), reach[1])]

    zero_row = jnp.zeros((1, tok), F32)
    over = jnp.zeros((1, 1), F32)
    places = []
    for way in range(2):
        level = float(half) - iota_f((8, tok), 0)
        member = as_one((reach[way] == level) & (level > 0.5))
        inner = dot(member.astype(BF), upper)
        sizes = jnp.sum(member, axis=1, keepdims=True)
        place = zero_row - 1.0
        total = jnp.zeros((1, 1), F32)
        for lev in range(half):
            place = jnp.where(member[lev:lev + 1] > 0.5, inner[lev:lev + 1] + total, place)
            total = total + sizes[lev:lev + 1]
            over = jnp.maximum(over, as_one(total > float(bounds[lev + 1])))
        places.append(place)

    x_val = x_ref[...]

    def pick_rows(way, lo, size):
        return as_one(iota_f((size, tok), 0) + float(lo) == places[way]).astype(BF)

    def pack_rows(way, lo, size):
        blk[way, lo:lo + size, :] = dot(pick_rows(way, lo, size), x_val).astype(BF)

    lanes = 128
    chosen_t = as_one(first_t | second_t).astype(BF)
    tally = lax.dot_general(jnp.ones((8, tok), BF), chosen_t, (((1,), (1,)), ((), ())), preferred_element_type=F32)
    count_send[...] = jnp.concatenate([tally[0:1], jnp.zeros((1, lanes - experts), F32) + over], axis=1)
    count_all[me] = count_send[...]
    for way in range(2):
        pack_rows(way, 0, bounds[1])

    def remote(src, dst, send, recv, to):
        return pltpu.make_async_remote_copy(
            src_ref=src, dst_ref=dst, send_sem=send, recv_sem=recv, device_id=to, device_id_type=MESH)

    def count_copy(step):
        return remote(count_send, count_all.at[me], count_ssem.at[step], count_rsem.at[step],
                      {'ep': lax.rem(me + step, n_ep)})

    def ring_rows(way, hop, lo, size):
        return hop_bufs[hop].at[pl.ds(way * HOP_ROWS[hop] + lo, size)]

    def hop_copy(way, hop, part):
        lo, size = bounds[part], bounds[part + 1] - bounds[part]
        src = blk.at[way, pl.ds(lo, size)] if hop == 0 else ring_rows(way, hop - 1, lo, size)
        return remote(src, ring_rows(way, hop, lo, size), send_sem.at[way, hop, part], recv_sem.at[way, hop, part],
                      {'ep': nxt[way]})

    def key_copy(way, hop):
        src = key_send.at[way] if hop == 0 else key_ring.at[way, hop - 1]
        return remote(src, key_ring.at[way, hop], ksend_sem.at[way, hop], krecv_sem.at[way, hop], {'ep': nxt[way]})

    def mirror_copy(way, hop):
        return remote(ring_rows(way, hop, 0, HOP_ROWS[hop]), ring_rows(2 + way, hop, 0, HOP_ROWS[hop]),
                      mir_send.at[way, hop], mir_recv.at[way, hop], {'ep': other})

    def key_mirror(way, hop):
        return remote(key_ring.at[way, hop], key_mir.at[way, hop], kmir_send.at[way, hop], kmir_recv.at[way, hop],
                      {'ep': other})

    px_copy = remote(x_ref, near.at[pl.ds(tok, tok)], px_sem.at[0], px_sem.at[1], {'ep': other})
    kpx_copy = remote(key_near.at[0], key_near.at[1], kpx_sem.at[0], kpx_sem.at[1], {'ep': other})

    def parts_of(hop):
        return [p for p in range(half - hop) if bounds[p + 1] > bounds[p]]

    pl.semaphore_wait(barrier, n_ep - 1 + n_dp - 1)
    for step in range(1, n_ep):
        count_copy(step).start()
    for way in range(2):
        hop_copy(way, 0, 0).start()
    px_copy.start()
    rank_t = dot(chosen_t, upper)
    ranks = [jnp.sum(jnp.where(mask, rank_t, 0.0), axis=0, keepdims=True) for mask in (first_t, second_t)]
    info = jnp.concatenate([ids[0], ranks[0], ids[1], ranks[1], zero_row + 1.0, zero_row, zero_row, zero_row], axis=0).astype(BF)
    place_cols = jnp.concatenate(places + [zero_row] * 6, axis=0).T
    for way in range(2):
        pick_t = as_one(iota_f((tok, HOP_ROWS[0]), 1) == place_cols[:, way:way + 1]).astype(BF)
        keys = dot(info, pick_t)
        for c in range(2):
            key = base + keys[2 * c:2 * c + 1] * float(src_cap) + keys[2 * c + 1:2 * c + 2]
            key_send[way, c:c + 1, 0:HOP_ROWS[0]] = jnp.where(keys[4:5] > 0.5, key, -1.0)
        key_copy(way, 0).start()
    for c in range(2):
        key_near[0, c:c + 1, :] = base + ids[c] * float(src_cap) + ranks[c]
    kpx_copy.start()
    near[0:tok, :] = x_val
    for way in range(2):
        pack_rows(way, bounds[1], HOP_ROWS[0] - bounds[1])
    for part in parts_of(0)[1:]:
        for way in range(2):
            hop_copy(way, 0, part).start()

    best, runner, first, second = top_two(logits, 1)
    chosen = as_one(first | second)
    rank = dot(as_one(row_i > col_i).astype(BF), chosen.astype(BF))
    lane_e = iota_f((tok, experts), 1)
    norm = jnp.sum(jnp.exp(logits - best), axis=1, keepdims=True)
    gates = (1.0 / norm, jnp.exp(runner - best) / norm)
    tkeys = [jnp.sum(jnp.where(mask, lane_e * float(src_cap) + rank, 0.0), axis=1, keepdims=True) for mask in (first, second)]

    for step in range(1, n_ep):
        count_copy(step).wait_recv()
    count_rows = jnp.concatenate([count_all[s] for s in range(n_ep)], axis=0)
    counts = count_rows[:, 0:experts]
    over = jnp.max(jnp.max(count_rows[:, experts:lanes], axis=1, keepdims=True), axis=0, keepdims=True)
    tri = as_one(lax.broadcasted_iota(jnp.int32, (n_ep, n_ep), 1) <= lax.broadcasted_iota(jnp.int32, (n_ep, n_ep), 0)).astype(BF)
    ends = dot(tri, counts.astype(BF))
    lane_ep = lax.broadcasted_iota(jnp.int32, (n_ep, experts), 1)
    slot = iota_f((n_ep, capacity), 1)
    for el in range(exp_dev):
        mine = lane_ep == me * exp_dev + el
        count_col = jnp.sum(jnp.where(mine, counts, 0.0), axis=1, keepdims=True)
        end_col = jnp.sum(jnp.where(mine, ends, 0.0), axis=1, keepdims=True)
        past = as_one(end_col <= slot)
        src = jnp.sum(past, axis=0, keepdims=True)
        rnk = slot[0:1] - jnp.sum(past * count_col, axis=0, keepdims=True)
        valid = src < float(n_ep)
        e_base = (me * exp_dev + el).astype(F32) * float(src_cap)
        key = jnp.where(valid, src * float(experts * src_cap) + e_base + rnk, -2.0)
        skey[el] = jnp.broadcast_to(key, (128, capacity)).T
        beyond = jnp.where(src == me.astype(F32), 0.0, float(direct)) + float((n_ep - 1) * direct)
        home = (src == me.astype(F32)) | (src == other.astype(F32))
        spot = jnp.where(rnk < float(direct), src * float(direct) + rnk, jnp.where(home, beyond + rnk, -1.0))
        rkeys[el:el + 1, :] = jnp.where(valid, spot, -1.0)

    kept = jnp.clip(float(capacity) - (ends - counts), 0.0, counts)
    to_chip = as_one(jnp.floor((iota_f((experts, lanes), 0) + 0.5) * (1.0 / (2 * exp_dev))) == iota_f((experts, lanes), 1)).astype(BF)
    pooled = dot(jnp.maximum(kept - float(direct), 0.0).astype(BF), to_chip)

    def distances(src, origin):
        dest = jnp.floor((src + 0.5) * 0.5)
        delta = dest - origin
        delta = jnp.where(delta < 0.0, delta + n_chip, delta)
        at_half = delta == float(half)
        even = src == 2.0 * dest
        return (jnp.where((delta < half) | (at_half & even), delta, 0.0),
                jnp.where((delta > half) | (at_half & jnp.logical_not(even)), n_chip - delta, 0.0))

    for dist in distances(iota_f((n_ep, lanes), 0), iota_f((n_ep, lanes), 1)):
        for hop in range(half):
            load = jnp.sum(jnp.where(dist >= float(hop + 1), pooled, 0.0), axis=0, keepdims=True)
            over = jnp.maximum(over, jnp.max(as_one(load > float(2 * RET_ROWS[hop])), axis=1, keepdims=True))

    def plan_overflow():
        row_c = lax.broadcasted_iota(jnp.int32, (capacity, capacity), 0)
        col_c = lax.broadcasted_iota(jnp.int32, (capacity, capacity), 1)
        upper_c = as_one(row_c < col_c).astype(BF)
        infos, members = [], ([], [])
        level = float(half) - iota_f((8, capacity), 0)
        zero_c = jnp.zeros((1, capacity), F32)
        for b in range(2 * exp_dev):
            expert_id = chip * 2 * exp_dev + b
            mine = lane_ep == expert_id
            count_col = jnp.sum(jnp.where(mine, counts, 0.0), axis=1, keepdims=True)
            end_col = jnp.sum(jnp.where(mine, ends, 0.0), axis=1, keepdims=True)
            past = as_one(end_col <= slot)
            src = jnp.sum(past, axis=0, keepdims=True)
            rnk = slot[0:1] - jnp.sum(past * count_col, axis=0, keepdims=True)
            live = (src < float(n_ep)) & (rnk >= float(direct))
            infos.append(jnp.concatenate([src, zero_c + expert_id.astype(F32), rnk, zero_c + 1.0] + [zero_c] * 4, axis=0).astype(BF))
            for way, dist in enumerate(distances(src, chip_f)):
                members[way].append(as_one((jnp.where(live, dist, 0.0) == level) & (level > 0.5)))
        for way in range(2):
            inner = dot(jnp.concatenate(members[way], axis=0).astype(BF), upper_c)
            run = jnp.zeros((8, 1), F32)
            inners = []
            for b in range(2 * exp_dev):
                inners.append(inner[8 * b:8 * b + 8] + run)
                run = run + jnp.sum(members[way][b], axis=1, keepdims=True)
            for b in range(2 * exp_dev):
                place, total = zero_c - 1.0, jnp.zeros((1, 1), F32)
                for lev in range(half):
                    place = jnp.where(members[way][b][lev:lev + 1] > 0.5, inners[b][lev:lev + 1] + total, place)
                    total = total + run[lev:lev + 1]
                ov_place[way, b:b + 1, :] = place
            columns = ov_place[way].T
            keys = jnp.zeros((8, RET_ROWS[0]), F32)
            turn = 2.0 * iota_f((capacity, RET_ROWS[0]), 1) + core.astype(F32)
            for b in range(2 * exp_dev):
                keys = keys + dot(infos[b], as_one(turn == columns[:, b:b + 1]).astype(BF))
            key = keys[0:1] * float(experts * src_cap) + keys[1:2] * float(src_cap) + keys[2:3]
            okey_send[way, 0:1, 0:RET_ROWS[0]] = jnp.where(keys[3:4] > 0.5, key, -1.0)

    def ov_rows(way, hop, lo, size):
        return ov_bufs[hop].at[pl.ds(way * RET_ROWS[hop] + lo, size)]

    def ov_copy(way, hop, part):
        lo, size = ov_bounds[part], ov_bounds[part + 1] - ov_bounds[part]
        src = ov_blk.at[way, pl.ds(lo, size)] if hop == 0 else ov_rows(way, hop - 1, lo, size)
        return remote(src, ov_rows(way, hop, lo, size), osend_sem.at[way, hop, part], orecv_sem.at[way, hop, part],
                      {'ep': nxt[way]})

    def okey_copy(way, hop):
        src = okey_send.at[way] if hop == 0 else okey_ring.at[way, hop - 1]
        return remote(src, okey_ring.at[way, hop], okey_sem.at[way, hop, 0], okey_sem.at[way, hop, 1], {'ep': nxt[way]})

    def ov_mirror(way, hop):
        return remote(ov_rows(way, hop, 0, RET_ROWS[hop]), ov_rows(2 + way, hop, 0, RET_ROWS[hop]),
                      omir_sem.at[way, hop, 0], omir_sem.at[way, hop, 1], {'ep': other})

    def okey_mirror(way, hop):
        return remote(okey_ring.at[way, hop], okey_mir.at[way, hop], okey_sem.at[way, hop, 2], okey_sem.at[way, hop, 3],
                      {'ep': other})

    def ov_parts(hop):
        return list(range(half - hop))

    def gather_rows(el, buf, keys, first_time=False):
        want = skey[el][:, 0:1]
        hit = as_one((want == keys[0:1]) | (want == keys[1:2])).astype(BF)
        part = dot(hit, buf[...])
        return part if first_time else acc[el] + part

    def gather_all(buf, keys, first_time=False):
        def body(el, carry):
            acc[el] = gather_rows(el, buf, keys, first_time)
            return carry
        lax.fori_loop(0, exp_dev, body, 0)

    def hop_keys(hop):
        for way in range(2):
            mirror_copy(way, hop).wait_recv()
            key_mirror(way, hop).wait_recv()
        size = HOP_ROWS[hop]
        return jnp.concatenate([keys[way, hop][:, 0:size] for keys in (key_ring, key_mir) for way in range(2)], axis=1)

    px_copy.wait_recv()
    kpx_copy.wait_recv()
    gather_all(near, jnp.concatenate([key_near[0], key_near[1]], axis=1), True)

    late = None
    for hop in range(half):
        for part in parts_of(hop):
            if hop == 1 and part == parts_of(1)[-1]:
                plan_overflow()
            if part == 1 and late is not None:
                gather_all(*late)
                late = None
            for way in range(2):
                hop_copy(way, hop, part).wait_recv()
                onward = hop + 1 < half
                if onward and part in parts_of(hop + 1):
                    hop_copy(way, hop + 1, part).start()
                if part == 0:
                    key_copy(way, hop).wait_recv()
                    key_mirror(way, hop).start()
                    if onward:
                        key_copy(way, hop + 1).start()
        for way in range(2):
            mirror_copy(way, hop).start()
        if hop + 1 < half:
            late = (hop_bufs[hop], hop_keys(hop))
            if hop + 2 == half:
                gather_all(*late)
                late = None
    last_keys = hop_keys(half - 1)

    flag_buf[0] = jnp.broadcast_to(over, (8, 128))

    def flag_copy(step):
        return pltpu.make_async_remote_copy(
            src_ref=flag_buf.at[0], dst_ref=flag_buf.at[step], send_sem=flag_ssem.at[step], recv_sem=flag_rsem.at[step],
            device_id={'dp': lax.rem(my_dp + step, n_dp)}, device_id_type=MESH)

    for step in range(1, n_dp):
        flag_copy(step).start()

    def ret_copy(el, step):
        dest = lax.rem(me + step, n_ep)
        return pltpu.make_async_remote_copy(
            src_ref=ret.at[el, pl.ds(pl.multiple_of(dest * direct, direct), direct)],
            dst_ref=back.at[el, pl.ds(pl.multiple_of(me * direct, direct), direct)],
            send_sem=ret_ssem.at[el, step], recv_sem=ret_rsem.at[el, step],
            device_id={'ep': dest}, device_id_type=MESH)

    def extra_copy(el):
        rows = pl.ds(packed - direct, direct)
        return remote(ret.at[el, rows], back.at[el, rows], extra_sem.at[el, 0], extra_sem.at[el, 1], {'ep': other})

    def z_copy(el):
        rows = pl.ds(pl.multiple_of(core * slots + el * capacity, capacity), capacity)
        return remote(z_all.at[rows], z_all.at[rows], z_sem.at[el, 0], z_sem.at[el, 1], {'ep': other})

    def z_arrival(el):
        rows = pl.ds(pl.multiple_of((1 - core) * slots + el * capacity, capacity), capacity)
        return remote(z_all.at[rows], z_all.at[rows], z_sem.at[el, 0], z_sem.at[el, 1], {'ep': other})

    ret_order = sorted(range(1, n_ep), key=lambda s: -min(s, n_ep - s))

    def expert_body(el, carry):
        spot = lax.rem(el, 2)
        for copy in weight_copies(el):
            copy.wait()
        rows = gather_rows(el, hop_bufs[half - 1], last_keys).astype(BF)
        z_acc[...] = jnp.zeros_like(z_acc)

        def ff_body(tile, inner):
            cols = pl.ds(pl.multiple_of(tile * FF_TILE, FF_TILE), FF_TILE)
            hidden = jax.nn.gelu(dot(rows, w1_buf[spot, :, cols]), approximate=True).astype(BF)
            z_acc[...] += dot(hidden, w2_buf[spot, cols, :])
            return inner

        lax.fori_loop(0, ff // FF_TILE, ff_body, 0)

        @pl.when(el + 2 < exp_dev)
        def _():
            for copy in weight_copies(el + 2):
                copy.start()

        spread = as_one(iota_f((packed, capacity), 0) == rkeys[pl.ds(el, 1), :]).astype(BF)
        z_rows = z_acc[...].astype(BF)
        z_all[pl.ds(pl.multiple_of(core * slots + el * capacity, capacity), capacity), :] = z_rows
        ret[el] = dot(spread, z_rows).astype(BF)
        for step in ret_order:
            ret_copy(el, step).start()
        extra_copy(el).start()
        z_copy(el).start()
        own = pl.ds(pl.multiple_of(me * direct, direct), direct)
        back[el, own, :] = ret[el, own, :]
        back[el, n_ep * direct:(n_ep + 1) * direct, :] = ret[el, n_ep * direct:(n_ep + 1) * direct, :]
        return carry

    lax.fori_loop(0, exp_dev, expert_body, 0)

    for el in range(exp_dev):
        z_arrival(el).wait_recv()
    turn = 2.0 * iota_f((RET_ROWS[0], capacity), 0) + core.astype(F32)
    for way in range(2):
        take = jnp.concatenate([as_one(turn == ov_place[way, b:b + 1, :]).astype(BF) for b in range(2 * exp_dev)], axis=1)
        ov_blk[way] = dot(take, z_all[...]).astype(BF)
    for way in range(2):
        ov_copy(way, 0, 0).start()
        okey_copy(way, 0).start()
    for part in ov_parts(0)[1:]:
        for way in range(2):
            ov_copy(way, 0, part).start()

    slot_i = lax.broadcasted_iota(jnp.int32, (1, packed), 1)
    slot_src = lax.div(slot_i, direct)
    slot_rank = slot_i - slot_src * direct
    slot_rank = jnp.where(slot_src < n_ep, slot_rank, slot_rank + direct)
    slot_src = jnp.where(slot_src < n_ep, slot_src, jnp.where(slot_src == n_ep, me, other))
    y_acc[...] = jnp.zeros_like(y_acc)

    def mix_body(el, carry):
        for step in ret_order:
            ret_copy(el, step).wait_recv()
        extra_copy(el).wait_recv()
        slot_key = ((slot_src * exp_dev + el) * src_cap + slot_rank).astype(F32)
        for c in range(2):
            hit = as_one(tkeys[c] == slot_key).astype(BF)
            y_acc[...] += gates[c] * dot(hit, back[el])
        return carry

    lax.fori_loop(0, exp_dev, mix_body, 0)

    def mix_overflow(hop):
        for way in range(2):
            ov_mirror(way, hop).wait_recv()
            okey_mirror(way, hop).wait_recv()
        size = RET_ROWS[hop]
        keys = jnp.concatenate([buf[way, hop][:, 0:size] for buf in (okey_ring, okey_mir) for way in range(2)], axis=1)
        for c in range(2):
            hit = as_one(base + tkeys[c] == keys).astype(BF)
            y_acc[...] += gates[c] * dot(hit, ov_bufs[hop][...])

    for hop in range(half):
        onward = hop + 1 < half
        for part in ov_parts(hop):
            for way in range(2):
                ov_copy(way, hop, part).wait_recv()
                if onward and part in ov_parts(hop + 1):
                    ov_copy(way, hop + 1, part).start()
                if part == 0:
                    okey_copy(way, hop).wait_recv()
                    okey_mirror(way, hop).start()
                    if onward:
                        okey_copy(way, hop + 1).start()
            if part == 0 and hop > 0:
                mix_overflow(hop - 1)
        for way in range(2):
            ov_mirror(way, hop).start()
    mix_overflow(half - 1)
    out_ref[...] = (x_ref[...].astype(F32) + y_acc[...]).astype(BF)

    worst = flag_buf[0]
    for step in range(1, n_dp):
        flag_copy(step).wait_recv()
        worst = jnp.maximum(worst, flag_buf[step])
    flag_ref[0] = jnp.max(worst)

    px_copy.wait_send()
    kpx_copy.wait_send()
    for step in range(1, n_ep):
        count_copy(step).wait_send()
    for step in range(1, n_dp):
        flag_copy(step).wait_send()
    for hop in range(half):
        for way in range(2):
            mirror_copy(way, hop).wait_send()
            key_mirror(way, hop).wait_send()
            key_copy(way, hop).wait_send()
            for part in parts_of(hop):
                hop_copy(way, hop, part).wait_send()
    for el in range(exp_dev):
        extra_copy(el).wait_send()
        z_copy(el).wait_send()
        for step in ret_order:
            ret_copy(el, step).wait_send()
    for hop in range(half):
        for way in range(2):
            ov_mirror(way, hop).wait_send()
            okey_mirror(way, hop).wait_send()
            okey_copy(way, hop).wait_send()
            for part in ov_parts(hop):
                ov_copy(way, hop, part).wait_send()


def plain_step(n_ep, x_rows, logits, w_in, w_out):
    tok, d_model = x_rows.shape
    experts = logits.shape[1]
    exp_dev = w_in.shape[0]
    capacity = CAP_FACTOR * tok * n_ep // experts
    src_cap = 4 * tok // experts
    me = lax.axis_index('ep')
    best, runner, first, second = top_two(logits, 1)
    norm = jnp.sum(jnp.exp(logits - best), axis=1, keepdims=True)
    gates = (1.0 / norm, jnp.exp(runner - best) / norm)
    chosen = as_one(first | second)
    lower = as_one(iota_f((tok, tok), 0) > iota_f((tok, tok), 1)).astype(BF)
    rank = dot(lower, chosen.astype(BF))
    counts = lax.all_gather(jnp.sum(chosen, axis=0), 'ep')
    tri = as_one(iota_f((n_ep, n_ep), 0) > iota_f((n_ep, n_ep), 1)).astype(BF)
    before = dot(tri, counts.astype(BF))
    mine = jnp.sum(jnp.where(iota_f((n_ep, experts), 0) == me.astype(F32), before, 0.0), axis=0, keepdims=True)
    slot_of = jnp.where(rank + mine < capacity, iota_f((tok, experts), 1) * src_cap + rank, -1.0)
    rows = [jnp.sum(jnp.where(mask, slot_of, 0.0), axis=1, keepdims=True) for mask in (first, second)]
    slots = iota_f((tok, experts * src_cap), 1)
    hits = [as_one(row == slots).astype(BF) for row in rows]
    send_buf = lax.dot_general(hits[0] + hits[1], x_rows, (((0,), (0,)), ((), ())), preferred_element_type=F32).astype(BF)
    recv_buf = lax.all_to_all(send_buf, 'ep', 0, 0, tiled=True)
    own = lax.dynamic_slice_in_dim(jnp.stack([before, counts]), me * exp_dev, exp_dev, axis=2)
    start = jnp.transpose(own[0])[:, :, None]
    size = jnp.transpose(own[1])[:, :, None]
    order = jnp.arange(src_cap, dtype=F32)[None, None, :]
    place = jnp.where((order < size) & (start + order < capacity), start + order, -1.0)
    place = jnp.where(place >= 0.0, place + capacity * jnp.arange(exp_dev, dtype=F32)[:, None, None], -1.0)
    place = jnp.transpose(place, (1, 0, 2)).reshape(1, experts * src_cap)
    move = as_one(iota_f((exp_dev * capacity, experts * src_cap), 0) == place).astype(BF)
    expert_rows = dot(move, recv_buf).astype(BF).reshape(exp_dev, capacity, d_model)
    hidden = jax.nn.gelu(jnp.einsum('ecd,edf->ecf', expert_rows, w_in, preferred_element_type=F32), approximate=True).astype(BF)
    expert_out = jnp.einsum('ecf,efd->ecd', hidden, w_out, preferred_element_type=F32).astype(BF).reshape(exp_dev * capacity, d_model)
    back_buf = lax.dot_general(move, expert_out, (((0,), (0,)), ((), ())), preferred_element_type=F32).astype(BF)
    ret_buf = lax.all_to_all(back_buf, 'ep', 0, 0, tiled=True)
    mix_sum = gates[0] * dot(hits[0], ret_buf) + gates[1] * dot(hits[1], ret_buf)
    return (x_rows.astype(F32) + mix_sum).astype(BF)


def solution(mesh):
    n_ep = mesh.shape['ep']
    n_dp = mesh.shape['dp']
    row_spec = P(('dp', 'ep'), None)
    expert_spec = P('ep', None, None)

    def local_step(x_rows, logits, w_in, w_out):
        tok, d_model = x_rows.shape
        experts = logits.shape[1]
        exp_dev, _, ff = w_in.shape
        capacity = CAP_FACTOR * tok * n_ep // experts
        src_cap = 4 * tok // experts
        half = n_ep // 4
        packed = (n_ep + 2) * (src_cap // 2)
        vmem = pl.BlockSpec(memory_space=pltpu.VMEM)
        smem = pl.BlockSpec(memory_space=pltpu.SMEM)
        hbm = pl.BlockSpec(memory_space=pl.ANY)
        dma = pltpu.SemaphoreType.DMA
        out, flag = pl.pallas_call(
            functools.partial(moe_kernel, n_ep, n_dp, capacity, src_cap),
            out_shape=(jax.ShapeDtypeStruct((tok, d_model), BF), jax.ShapeDtypeStruct((1,), F32)),
            in_specs=[vmem, vmem, hbm, hbm],
            out_specs=(vmem, smem),
            scratch_shapes=[
                pltpu.VMEM((2, d_model, ff), BF),
                pltpu.VMEM((2, ff, d_model), BF),
                pltpu.VMEM((2, HOP_ROWS[0], d_model), BF),
                pltpu.VMEM((2 * tok, d_model), BF),
                *[pltpu.VMEM((4 * rows, d_model), BF) for rows in HOP_ROWS],
                pltpu.VMEM((2, 2, tok), F32),
                pltpu.VMEM((2, 2, tok), F32),
                pltpu.VMEM((2, half, 2, tok), F32),
                pltpu.VMEM((2, half, 2, tok), F32),
                pltpu.VMEM((1, 128), F32),
                pltpu.VMEM((n_ep, 1, 128), F32),
                pltpu.VMEM((exp_dev, capacity, d_model), F32),
                pltpu.VMEM((capacity, d_model), F32),
                pltpu.VMEM((exp_dev, capacity, 128), F32),
                pltpu.VMEM((8, capacity), F32),
                pltpu.VMEM((exp_dev, packed, d_model), BF),
                pltpu.VMEM((exp_dev, packed, d_model), BF),
                pltpu.VMEM((tok, d_model), F32),
                pltpu.VMEM((n_dp, 8, 128), F32),
                pltpu.VMEM((2 * exp_dev * capacity, d_model), BF),
                pltpu.VMEM((2, 2 * exp_dev, capacity), F32),
                pltpu.VMEM((2, RET_ROWS[0], d_model), BF),
                *[pltpu.VMEM((4 * rows, d_model), BF) for rows in RET_ROWS],
                pltpu.VMEM((2, 1, tok), F32),
                pltpu.VMEM((2, half, 1, tok), F32),
                pltpu.VMEM((2, half, 1, tok), F32),
                dma((2, 2)),
                dma((2, half, half)), dma((2, half, half)),
                dma((2, half)), dma((2, half)),
                dma((2,)),
                dma((2, half)), dma((2, half)), dma((2, half)), dma((2, half)),
                dma((2,)),
                dma((n_ep,)), dma((n_ep,)),
                dma((exp_dev, n_ep)), dma((exp_dev, n_ep)),
                dma((n_dp,)), dma((n_dp,)),
                dma((exp_dev, 2)), dma((exp_dev, 2)),
                dma((2, half, half)), dma((2, half, half)),
                dma((2, half, 2)), dma((2, half, 4)),
            ],
            compiler_params=pltpu.CompilerParams(
                collective_id=0, has_side_effects=True, vmem_limit_bytes=62 * 1024 * 1024),
            name='moe_layer',
        )(x_rows, logits.T, w_in, w_out)
        return lax.cond(flag[0] > 0.0, functools.partial(plain_step, n_ep), lambda *_: out, x_rows, logits, w_in, w_out)

    return jax.shard_map(local_step, mesh=mesh, in_specs=(row_spec, row_spec, expert_spec, expert_spec), out_specs=row_spec, check_vma=False)
```

```python
import functools

import jax
import jax.numpy as jnp
from jax import lax
from jax.experimental import pallas as pl
from jax.experimental.pallas import tpu as pltpu
from jax.sharding import PartitionSpec as P

CAP_FACTOR = 2
HOP_ROWS = (464, 384, 304, 160)
RET_ROWS = (416, 320, 208, 80)
DIRECT_PART = 4
FF_TILE = 512
BF = jnp.bfloat16
F32 = jnp.float32
MESH = pl.DeviceIdType.MESH


def top_two(vals, axis):
    best = jnp.max(vals, axis=axis, keepdims=True)
    first = vals == best
    rest = jnp.where(first, -jnp.inf, vals)
    runner = jnp.max(rest, axis=axis, keepdims=True)
    return best, runner, first, rest == runner


def as_one(mask):
    return jnp.where(mask, 1.0, 0.0)


def iota_f(shape, dim):
    return lax.broadcasted_iota(jnp.int32, shape, dim).astype(F32)


def dot(lhs, rhs):
    return jnp.dot(lhs, rhs, preferred_element_type=F32)


def moe_kernel(n_ep, n_dp, capacity, src_cap, x_ref, lg_ref, w1_hbm, w2_hbm, out_ref, flag_ref,
               w1_buf, w2_buf, blk, near, hops_a, hops_b, hops_c, hops_d, key_send, key_near, key_ring, key_mir,
               count_send, count_all, acc, z_acc, skey, rkeys, ret, back, y_acc, flag_buf,
               z_all, ov_place, ov_blk, ov_a, ov_b, ov_c, ov_d, okey_send, okey_ring, okey_mir,
               w_sem, send_sem, recv_sem, mir_send, mir_recv, px_sem, ksend_sem, krecv_sem, kmir_send, kmir_recv,
               kpx_sem, count_ssem, count_rsem, ret_ssem, ret_rsem, flag_ssem, flag_rsem, z_sem, extra_sem,
               osend_sem, orecv_sem, omir_sem, okey_sem):
    tok, d_model = x_ref.shape
    experts = lg_ref.shape[0]
    exp_dev = experts // n_ep
    ff = w1_buf.shape[2]
    n_chip = n_ep // 2
    half = n_chip // 2
    me = lax.axis_index('ep')
    my_dp = lax.axis_index('dp')
    chip = lax.div(me, 2)
    core = lax.rem(me, 2)
    other = chip * 2 + 1 - core
    nxt = (lax.rem(chip + 1, n_chip) * 2 + core, lax.rem(chip + n_chip - 1, n_chip) * 2 + core)
    bounds = (0,) + HOP_ROWS[::-1]
    hop_bufs = (hops_a, hops_b, hops_c, hops_d)
    ov_bufs = (ov_a, ov_b, ov_c, ov_d)
    ov_bounds = (0,) + RET_ROWS[::-1]
    direct = src_cap // DIRECT_PART
    extra = src_cap - direct
    packed = n_ep * direct + 2 * extra
    slots = exp_dev * capacity

    def weight_copies(el):
        slot = lax.rem(el, 2)
        return (pltpu.make_async_copy(w1_hbm.at[el], w1_buf.at[slot], w_sem.at[slot, 0]),
                pltpu.make_async_copy(w2_hbm.at[el], w2_buf.at[slot], w_sem.at[slot, 1]))

    for el in range(min(2, exp_dev)):
        for copy in weight_copies(el):
            copy.start()

    barrier = pltpu.get_barrier_semaphore()
    for step in range(1, n_ep):
        pl.semaphore_signal(barrier, inc=1, device_id={'ep': lax.rem(me + step, n_ep)}, device_id_type=MESH)
    for step in range(1, n_dp):
        pl.semaphore_signal(barrier, inc=1, device_id={'dp': lax.rem(my_dp + step, n_dp)}, device_id_type=MESH)

    logits_t = lg_ref[...]
    logits = logits_t.T
    _, _, first_t, second_t = top_two(logits_t, 0)
    row_i = lax.broadcasted_iota(jnp.int32, (tok, tok), 0)
    col_i = lax.broadcasted_iota(jnp.int32, (tok, tok), 1)
    upper = as_one(row_i < col_i).astype(BF)
    e_ids = iota_f((experts, tok), 0)
    ids = [jnp.sum(jnp.where(mask, e_ids, 0.0), axis=0, keepdims=True) for mask in (first_t, second_t)]
    chip_f = chip.astype(F32)
    base = me.astype(F32) * float(experts * src_cap)
    reach = [jnp.zeros((1, tok), F32), jnp.zeros((1, tok), F32)]
    opposite = jnp.zeros((1, tok), jnp.bool_)
    for expert_id in ids:
        delta = jnp.floor((expert_id + 0.5) * (1.0 / (2 * exp_dev))) - chip_f
        delta = jnp.where(delta < 0.0, delta + n_chip, delta)
        reach[0] = jnp.maximum(reach[0], jnp.where(delta < half, delta, 0.0))
        reach[1] = jnp.maximum(reach[1], jnp.where(delta > half, n_chip - delta, 0.0))
        opposite = opposite | (delta == half)
    odd = lax.rem(lax.broadcasted_iota(jnp.int32, (1, tok), 1) + core, 2) == 0
    forward = (reach[0] > reach[1]) | ((reach[0] == reach[1]) & odd)
    reach = [jnp.where(opposite & forward, float(half), reach[0]),
             jnp.where(opposite & jnp.logical_not(forward), float(half), reach[1])]

    zero_row = jnp.zeros((1, tok), F32)
    over = jnp.zeros((1, 1), F32)
    places = []
    for way in range(2):
        level = float(half) - iota_f((8, tok), 0)
        member = as_one((reach[way] == level) & (level > 0.5))
        inner = dot(member.astype(BF), upper)
        sizes = jnp.sum(member, axis=1, keepdims=True)
        place = zero_row - 1.0
        total = jnp.zeros((1, 1), F32)
        for lev in range(half):
            place = jnp.where(member[lev:lev + 1] > 0.5, inner[lev:lev + 1] + total, place)
            total = total + sizes[lev:lev + 1]
            over = jnp.maximum(over, as_one(total > float(bounds[lev + 1])))
        places.append(place)

    x_val = x_ref[...]

    def pick_rows(way, lo, size):
        return as_one(iota_f((size, tok), 0) + float(lo) == places[way]).astype(BF)

    def pack_rows(way, lo, size):
        blk[way, lo:lo + size, :] = dot(pick_rows(way, lo, size), x_val).astype(BF)

    lanes = 128
    chosen_t = as_one(first_t | second_t).astype(BF)
    tally = lax.dot_general(jnp.ones((8, tok), BF), chosen_t, (((1,), (1,)), ((), ())), preferred_element_type=F32)
    count_send[...] = jnp.concatenate([tally[0:1], jnp.zeros((1, lanes - experts), F32) + over], axis=1)
    count_all[me] = count_send[...]
    for way in range(2):
        pack_rows(way, 0, bounds[1])

    def remote(src, dst, send, recv, to):
        return pltpu.make_async_remote_copy(
            src_ref=src, dst_ref=dst, send_sem=send, recv_sem=recv, device_id=to, device_id_type=MESH)

    def count_copy(step):
        return remote(count_send, count_all.at[me], count_ssem.at[step], count_rsem.at[step],
                      {'ep': lax.rem(me + step, n_ep)})

    def ring_rows(way, hop, lo, size):
        return hop_bufs[hop].at[pl.ds(way * HOP_ROWS[hop] + lo, size)]

    def hop_copy(way, hop, part):
        lo, size = bounds[part], bounds[part + 1] - bounds[part]
        src = blk.at[way, pl.ds(lo, size)] if hop == 0 else ring_rows(way, hop - 1, lo, size)
        return remote(src, ring_rows(way, hop, lo, size), send_sem.at[way, hop, part], recv_sem.at[way, hop, part],
                      {'ep': nxt[way]})

    def key_copy(way, hop):
        src = key_send.at[way] if hop == 0 else key_ring.at[way, hop - 1]
        return remote(src, key_ring.at[way, hop], ksend_sem.at[way, hop], krecv_sem.at[way, hop], {'ep': nxt[way]})

    def mirror_copy(way, hop):
        return remote(ring_rows(way, hop, 0, HOP_ROWS[hop]), ring_rows(2 + way, hop, 0, HOP_ROWS[hop]),
                      mir_send.at[way, hop], mir_recv.at[way, hop], {'ep': other})

    def key_mirror(way, hop):
        return remote(key_ring.at[way, hop], key_mir.at[way, hop], kmir_send.at[way, hop], kmir_recv.at[way, hop],
                      {'ep': other})

    px_copy = remote(x_ref, near.at[pl.ds(tok, tok)], px_sem.at[0], px_sem.at[1], {'ep': other})
    kpx_copy = remote(key_near.at[0], key_near.at[1], kpx_sem.at[0], kpx_sem.at[1], {'ep': other})

    def parts_of(hop):
        return [p for p in range(half - hop) if bounds[p + 1] > bounds[p]]

    pl.semaphore_wait(barrier, n_ep - 1 + n_dp - 1)
    for step in range(1, n_ep):
        count_copy(step).start()
    for way in range(2):
        hop_copy(way, 0, 0).start()
    px_copy.start()
    rank_t = dot(chosen_t, upper)
    ranks = [jnp.sum(jnp.where(mask, rank_t, 0.0), axis=0, keepdims=True) for mask in (first_t, second_t)]
    info = jnp.concatenate([ids[0], ranks[0], ids[1], ranks[1], zero_row + 1.0, zero_row, zero_row, zero_row], axis=0).astype(BF)
    place_cols = jnp.concatenate(places + [zero_row] * 6, axis=0).T
    for way in range(2):
        pick_t = as_one(iota_f((tok, HOP_ROWS[0]), 1) == place_cols[:, way:way + 1]).astype(BF)
        keys = dot(info, pick_t)
        for c in range(2):
            key = base + keys[2 * c:2 * c + 1] * float(src_cap) + keys[2 * c + 1:2 * c + 2]
            key_send[way, c:c + 1, 0:HOP_ROWS[0]] = jnp.where(keys[4:5] > 0.5, key, -1.0)
        key_copy(way, 0).start()
    for c in range(2):
        key_near[0, c:c + 1, :] = base + ids[c] * float(src_cap) + ranks[c]
    kpx_copy.start()
    near[0:tok, :] = x_val
    for way in range(2):
        pack_rows(way, bounds[1], HOP_ROWS[0] - bounds[1])
    for part in parts_of(0)[1:]:
        for way in range(2):
            hop_copy(way, 0, part).start()

    best, runner, first, second = top_two(logits, 1)
    chosen = as_one(first | second)
    rank = dot(as_one(row_i > col_i).astype(BF), chosen.astype(BF))
    lane_e = iota_f((tok, experts), 1)
    norm = jnp.sum(jnp.exp(logits - best), axis=1, keepdims=True)
    gates = (1.0 / norm, jnp.exp(runner - best) / norm)
    tkeys = [jnp.sum(jnp.where(mask, lane_e * float(src_cap) + rank, 0.0), axis=1, keepdims=True) for mask in (first, second)]

    for step in range(1, n_ep):
        count_copy(step).wait_recv()
    count_rows = jnp.concatenate([count_all[s] for s in range(n_ep)], axis=0)
    counts = count_rows[:, 0:experts]
    over = jnp.max(jnp.max(count_rows[:, experts:lanes], axis=1, keepdims=True), axis=0, keepdims=True)
    tri = as_one(lax.broadcasted_iota(jnp.int32, (n_ep, n_ep), 1) <= lax.broadcasted_iota(jnp.int32, (n_ep, n_ep), 0)).astype(BF)
    ends = dot(tri, counts.astype(BF))
    lane_ep = lax.broadcasted_iota(jnp.int32, (n_ep, experts), 1)
    slot = iota_f((n_ep, capacity), 1)
    for el in range(exp_dev):
        mine = lane_ep == me * exp_dev + el
        count_col = jnp.sum(jnp.where(mine, counts, 0.0), axis=1, keepdims=True)
        end_col = jnp.sum(jnp.where(mine, ends, 0.0), axis=1, keepdims=True)
        past = as_one(end_col <= slot)
        src = jnp.sum(past, axis=0, keepdims=True)
        rnk = slot[0:1] - jnp.sum(past * count_col, axis=0, keepdims=True)
        valid = src < float(n_ep)
        e_base = (me * exp_dev + el).astype(F32) * float(src_cap)
        key = jnp.where(valid, src * float(experts * src_cap) + e_base + rnk, -2.0)
        skey[el] = jnp.broadcast_to(key, (128, capacity)).T
        beyond = jnp.where(src == me.astype(F32), 0.0, float(extra)) + float((n_ep - 1) * direct)
        home = (src == me.astype(F32)) | (src == other.astype(F32))
        spot = jnp.where(rnk < float(direct), src * float(direct) + rnk, jnp.where(home, beyond + rnk, -1.0))
        rkeys[el:el + 1, :] = jnp.where(valid, spot, -1.0)

    kept = jnp.clip(float(capacity) - (ends - counts), 0.0, counts)
    to_chip = as_one(jnp.floor((iota_f((experts, lanes), 0) + 0.5) * (1.0 / (2 * exp_dev))) == iota_f((experts, lanes), 1)).astype(BF)
    pooled = dot(jnp.maximum(kept - float(direct), 0.0).astype(BF), to_chip)

    def distances(src, origin):
        dest = jnp.floor((src + 0.5) * 0.5)
        delta = dest - origin
        delta = jnp.where(delta < 0.0, delta + n_chip, delta)
        at_half = delta == float(half)
        even = src == 2.0 * dest
        return (jnp.where((delta < half) | (at_half & even), delta, 0.0),
                jnp.where((delta > half) | (at_half & jnp.logical_not(even)), n_chip - delta, 0.0))

    for dist in distances(iota_f((n_ep, lanes), 0), iota_f((n_ep, lanes), 1)):
        for hop in range(half):
            load = jnp.sum(jnp.where(dist >= float(hop + 1), pooled, 0.0), axis=0, keepdims=True)
            over = jnp.maximum(over, jnp.max(as_one(load > float(2 * RET_ROWS[hop])), axis=1, keepdims=True))

    def plan_overflow():
        row_c = lax.broadcasted_iota(jnp.int32, (capacity, capacity), 0)
        col_c = lax.broadcasted_iota(jnp.int32, (capacity, capacity), 1)
        upper_c = as_one(row_c < col_c).astype(BF)
        infos, members = [], ([], [])
        level = float(half) - iota_f((8, capacity), 0)
        zero_c = jnp.zeros((1, capacity), F32)
        for b in range(2 * exp_dev):
            expert_id = chip * 2 * exp_dev + b
            mine = lane_ep == expert_id
            count_col = jnp.sum(jnp.where(mine, counts, 0.0), axis=1, keepdims=True)
            end_col = jnp.sum(jnp.where(mine, ends, 0.0), axis=1, keepdims=True)
            past = as_one(end_col <= slot)
            src = jnp.sum(past, axis=0, keepdims=True)
            rnk = slot[0:1] - jnp.sum(past * count_col, axis=0, keepdims=True)
            live = (src < float(n_ep)) & (rnk >= float(direct))
            infos.append(jnp.concatenate([src, zero_c + expert_id.astype(F32), rnk, zero_c + 1.0] + [zero_c] * 4, axis=0).astype(BF))
            for way, dist in enumerate(distances(src, chip_f)):
                members[way].append(as_one((jnp.where(live, dist, 0.0) == level) & (level > 0.5)))
        for way in range(2):
            inner = dot(jnp.concatenate(members[way], axis=0).astype(BF), upper_c)
            run = jnp.zeros((8, 1), F32)
            inners = []
            for b in range(2 * exp_dev):
                inners.append(inner[8 * b:8 * b + 8] + run)
                run = run + jnp.sum(members[way][b], axis=1, keepdims=True)
            for b in range(2 * exp_dev):
                place, total = zero_c - 1.0, jnp.zeros((1, 1), F32)
                for lev in range(half):
                    place = jnp.where(members[way][b][lev:lev + 1] > 0.5, inners[b][lev:lev + 1] + total, place)
                    total = total + run[lev:lev + 1]
                ov_place[way, b:b + 1, :] = place
            columns = ov_place[way].T
            keys = jnp.zeros((8, RET_ROWS[0]), F32)
            turn = 2.0 * iota_f((capacity, RET_ROWS[0]), 1) + core.astype(F32)
            for b in range(2 * exp_dev):
                keys = keys + dot(infos[b], as_one(turn == columns[:, b:b + 1]).astype(BF))
            key = keys[0:1] * float(experts * src_cap) + keys[1:2] * float(src_cap) + keys[2:3]
            okey_send[way, 0:1, 0:RET_ROWS[0]] = jnp.where(keys[3:4] > 0.5, key, -1.0)

    def ov_rows(way, hop, lo, size):
        return ov_bufs[hop].at[pl.ds(way * RET_ROWS[hop] + lo, size)]

    def ov_copy(way, hop, part):
        lo, size = ov_bounds[part], ov_bounds[part + 1] - ov_bounds[part]
        src = ov_blk.at[way, pl.ds(lo, size)] if hop == 0 else ov_rows(way, hop - 1, lo, size)
        return remote(src, ov_rows(way, hop, lo, size), osend_sem.at[way, hop, part], orecv_sem.at[way, hop, part],
                      {'ep': nxt[way]})

    def okey_copy(way, hop):
        src = okey_send.at[way] if hop == 0 else okey_ring.at[way, hop - 1]
        return remote(src, okey_ring.at[way, hop], okey_sem.at[way, hop, 0], okey_sem.at[way, hop, 1], {'ep': nxt[way]})

    def ov_mirror(way, hop):
        return remote(ov_rows(way, hop, 0, RET_ROWS[hop]), ov_rows(2 + way, hop, 0, RET_ROWS[hop]),
                      omir_sem.at[way, hop, 0], omir_sem.at[way, hop, 1], {'ep': other})

    def okey_mirror(way, hop):
        return remote(okey_ring.at[way, hop], okey_mir.at[way, hop], okey_sem.at[way, hop, 2], okey_sem.at[way, hop, 3],
                      {'ep': other})

    def ov_parts(hop):
        return list(range(half - hop))

    def gather_rows(el, buf, keys, first_time=False):
        want = skey[el][:, 0:1]
        hit = as_one((want == keys[0:1]) | (want == keys[1:2])).astype(BF)
        part = dot(hit, buf[...])
        return part if first_time else acc[el] + part

    def gather_all(buf, keys, first_time=False):
        def body(el, carry):
            acc[el] = gather_rows(el, buf, keys, first_time)
            return carry
        lax.fori_loop(0, exp_dev, body, 0)

    def hop_keys(hop):
        for way in range(2):
            mirror_copy(way, hop).wait_recv()
            key_mirror(way, hop).wait_recv()
        size = HOP_ROWS[hop]
        return jnp.concatenate([keys[way, hop][:, 0:size] for keys in (key_ring, key_mir) for way in range(2)], axis=1)

    px_copy.wait_recv()
    kpx_copy.wait_recv()
    gather_all(near, jnp.concatenate([key_near[0], key_near[1]], axis=1), True)

    late = None
    for hop in range(half):
        for part in parts_of(hop):
            if hop == 1 and part == parts_of(1)[-1]:
                plan_overflow()
            if part == 1 and late is not None:
                gather_all(*late)
                late = None
            for way in range(2):
                hop_copy(way, hop, part).wait_recv()
                onward = hop + 1 < half
                if onward and part in parts_of(hop + 1):
                    hop_copy(way, hop + 1, part).start()
                if part == 0:
                    key_copy(way, hop).wait_recv()
                    key_mirror(way, hop).start()
                    if onward:
                        key_copy(way, hop + 1).start()
        for way in range(2):
            mirror_copy(way, hop).start()
        if hop + 1 < half:
            late = (hop_bufs[hop], hop_keys(hop))
            if hop + 2 == half:
                gather_all(*late)
                late = None
    last_keys = hop_keys(half - 1)

    flag_buf[0] = jnp.broadcast_to(over, (8, 128))

    def flag_copy(step):
        return pltpu.make_async_remote_copy(
            src_ref=flag_buf.at[0], dst_ref=flag_buf.at[step], send_sem=flag_ssem.at[step], recv_sem=flag_rsem.at[step],
            device_id={'dp': lax.rem(my_dp + step, n_dp)}, device_id_type=MESH)

    for step in range(1, n_dp):
        flag_copy(step).start()

    def ret_copy(el, step):
        dest = lax.rem(me + step, n_ep)
        return pltpu.make_async_remote_copy(
            src_ref=ret.at[el, pl.ds(pl.multiple_of(dest * direct, direct), direct)],
            dst_ref=back.at[el, pl.ds(pl.multiple_of(me * direct, direct), direct)],
            send_sem=ret_ssem.at[el, step], recv_sem=ret_rsem.at[el, step],
            device_id={'ep': dest}, device_id_type=MESH)

    def extra_copy(el):
        rows = pl.ds(packed - extra, extra)
        return remote(ret.at[el, rows], back.at[el, rows], extra_sem.at[el, 0], extra_sem.at[el, 1], {'ep': other})

    def z_copy(el):
        rows = pl.ds(pl.multiple_of(core * slots + el * capacity, capacity), capacity)
        return remote(z_all.at[rows], z_all.at[rows], z_sem.at[el, 0], z_sem.at[el, 1], {'ep': other})

    def z_arrival(el):
        rows = pl.ds(pl.multiple_of((1 - core) * slots + el * capacity, capacity), capacity)
        return remote(z_all.at[rows], z_all.at[rows], z_sem.at[el, 0], z_sem.at[el, 1], {'ep': other})

    ret_order = sorted(range(1, n_ep), key=lambda s: -min(s, n_ep - s))

    def expert_body(el, carry):
        spot = lax.rem(el, 2)
        for copy in weight_copies(el):
            copy.wait()
        rows = gather_rows(el, hop_bufs[half - 1], last_keys).astype(BF)
        z_acc[...] = jnp.zeros_like(z_acc)

        def ff_body(tile, inner):
            cols = pl.ds(pl.multiple_of(tile * FF_TILE, FF_TILE), FF_TILE)
            hidden = jax.nn.gelu(dot(rows, w1_buf[spot, :, cols]), approximate=True).astype(BF)
            z_acc[...] += dot(hidden, w2_buf[spot, cols, :])
            return inner

        lax.fori_loop(0, ff // FF_TILE, ff_body, 0)

        @pl.when(el + 2 < exp_dev)
        def _():
            for copy in weight_copies(el + 2):
                copy.start()

        spread = as_one(iota_f((packed, capacity), 0) == rkeys[pl.ds(el, 1), :]).astype(BF)
        z_rows = z_acc[...].astype(BF)
        z_all[pl.ds(pl.multiple_of(core * slots + el * capacity, capacity), capacity), :] = z_rows
        ret[el] = dot(spread, z_rows).astype(BF)
        for step in ret_order:
            ret_copy(el, step).start()
        extra_copy(el).start()
        z_copy(el).start()
        own = pl.ds(pl.multiple_of(me * direct, direct), direct)
        back[el, own, :] = ret[el, own, :]
        back[el, packed - 2 * extra:packed - extra, :] = ret[el, packed - 2 * extra:packed - extra, :]
        return carry

    lax.fori_loop(0, exp_dev, expert_body, 0)

    for el in range(exp_dev):
        z_arrival(el).wait_recv()
    turn = 2.0 * iota_f((RET_ROWS[0], capacity), 0) + core.astype(F32)
    for way in range(2):
        take = jnp.concatenate([as_one(turn == ov_place[way, b:b + 1, :]).astype(BF) for b in range(2 * exp_dev)], axis=1)
        ov_blk[way] = dot(take, z_all[...]).astype(BF)
    for way in range(2):
        ov_copy(way, 0, 0).start()
        okey_copy(way, 0).start()
    for part in ov_parts(0)[1:]:
        for way in range(2):
            ov_copy(way, 0, part).start()

    slot_i = lax.broadcasted_iota(jnp.int32, (1, packed), 1)
    slot_src = lax.div(slot_i, direct)
    slot_rank = slot_i - slot_src * direct
    past_own = slot_i - n_ep * direct
    past_other = past_own - extra
    slot_src = jnp.where(past_own < 0, slot_src, jnp.where(past_other < 0, me, other))
    slot_rank = jnp.where(past_own < 0, slot_rank, jnp.where(past_other < 0, past_own, past_other) + direct)
    y_acc[...] = jnp.zeros_like(y_acc)

    def mix_body(el, carry):
        for step in ret_order:
            ret_copy(el, step).wait_recv()
        extra_copy(el).wait_recv()
        slot_key = ((slot_src * exp_dev + el) * src_cap + slot_rank).astype(F32)
        for c in range(2):
            hit = as_one(tkeys[c] == slot_key).astype(BF)
            y_acc[...] += gates[c] * dot(hit, back[el])
        return carry

    lax.fori_loop(0, exp_dev, mix_body, 0)

    def mix_overflow(hop):
        for way in range(2):
            ov_mirror(way, hop).wait_recv()
            okey_mirror(way, hop).wait_recv()
        size = RET_ROWS[hop]
        keys = jnp.concatenate([buf[way, hop][:, 0:size] for buf in (okey_ring, okey_mir) for way in range(2)], axis=1)
        for c in range(2):
            hit = as_one(base + tkeys[c] == keys).astype(BF)
            y_acc[...] += gates[c] * dot(hit, ov_bufs[hop][...])

    for hop in range(half):
        onward = hop + 1 < half
        for part in ov_parts(hop):
            for way in range(2):
                ov_copy(way, hop, part).wait_recv()
                if onward and part in ov_parts(hop + 1):
                    ov_copy(way, hop + 1, part).start()
                if part == 0:
                    okey_copy(way, hop).wait_recv()
                    okey_mirror(way, hop).start()
                    if onward:
                        okey_copy(way, hop + 1).start()
            if part == 0 and hop > 0 and onward:
                mix_overflow(hop - 1)
        for way in range(2):
            ov_mirror(way, hop).start()
        if not onward:
            mix_overflow(hop - 1)
    mix_overflow(half - 1)
    out_ref[...] = (x_ref[...].astype(F32) + y_acc[...]).astype(BF)

    worst = flag_buf[0]
    for step in range(1, n_dp):
        flag_copy(step).wait_recv()
        worst = jnp.maximum(worst, flag_buf[step])
    flag_ref[0] = jnp.max(worst)

    px_copy.wait_send()
    kpx_copy.wait_send()
    for step in range(1, n_ep):
        count_copy(step).wait_send()
    for step in range(1, n_dp):
        flag_copy(step).wait_send()
    for hop in range(half):
        for way in range(2):
            mirror_copy(way, hop).wait_send()
            key_mirror(way, hop).wait_send()
            key_copy(way, hop).wait_send()
            for part in parts_of(hop):
                hop_copy(way, hop, part).wait_send()
    for el in range(exp_dev):
        extra_copy(el).wait_send()
        z_copy(el).wait_send()
        for step in ret_order:
            ret_copy(el, step).wait_send()
    for hop in range(half):
        for way in range(2):
            ov_mirror(way, hop).wait_send()
            okey_mirror(way, hop).wait_send()
            okey_copy(way, hop).wait_send()
            for part in ov_parts(hop):
                ov_copy(way, hop, part).wait_send()


def plain_step(n_ep, x_rows, logits, w_in, w_out):
    tok, d_model = x_rows.shape
    experts = logits.shape[1]
    exp_dev = w_in.shape[0]
    capacity = CAP_FACTOR * tok * n_ep // experts
    src_cap = 4 * tok // experts
    me = lax.axis_index('ep')
    best, runner, first, second = top_two(logits, 1)
    norm = jnp.sum(jnp.exp(logits - best), axis=1, keepdims=True)
    gates = (1.0 / norm, jnp.exp(runner - best) / norm)
    chosen = as_one(first | second)
    lower = as_one(iota_f((tok, tok), 0) > iota_f((tok, tok), 1)).astype(BF)
    rank = dot(lower, chosen.astype(BF))
    counts = lax.all_gather(jnp.sum(chosen, axis=0), 'ep')
    tri = as_one(iota_f((n_ep, n_ep), 0) > iota_f((n_ep, n_ep), 1)).astype(BF)
    before = dot(tri, counts.astype(BF))
    mine = jnp.sum(jnp.where(iota_f((n_ep, experts), 0) == me.astype(F32), before, 0.0), axis=0, keepdims=True)
    slot_of = jnp.where(rank + mine < capacity, iota_f((tok, experts), 1) * src_cap + rank, -1.0)
    rows = [jnp.sum(jnp.where(mask, slot_of, 0.0), axis=1, keepdims=True) for mask in (first, second)]
    slots = iota_f((tok, experts * src_cap), 1)
    hits = [as_one(row == slots).astype(BF) for row in rows]
    send_buf = lax.dot_general(hits[0] + hits[1], x_rows, (((0,), (0,)), ((), ())), preferred_element_type=F32).astype(BF)
    recv_buf = lax.all_to_all(send_buf, 'ep', 0, 0, tiled=True)
    own = lax.dynamic_slice_in_dim(jnp.stack([before, counts]), me * exp_dev, exp_dev, axis=2)
    start = jnp.transpose(own[0])[:, :, None]
    size = jnp.transpose(own[1])[:, :, None]
    order = jnp.arange(src_cap, dtype=F32)[None, None, :]
    place = jnp.where((order < size) & (start + order < capacity), start + order, -1.0)
    place = jnp.where(place >= 0.0, place + capacity * jnp.arange(exp_dev, dtype=F32)[:, None, None], -1.0)
    place = jnp.transpose(place, (1, 0, 2)).reshape(1, experts * src_cap)
    move = as_one(iota_f((exp_dev * capacity, experts * src_cap), 0) == place).astype(BF)
    expert_rows = dot(move, recv_buf).astype(BF).reshape(exp_dev, capacity, d_model)
    hidden = jax.nn.gelu(jnp.einsum('ecd,edf->ecf', expert_rows, w_in, preferred_element_type=F32), approximate=True).astype(BF)
    expert_out = jnp.einsum('ecf,efd->ecd', hidden, w_out, preferred_element_type=F32).astype(BF).reshape(exp_dev * capacity, d_model)
    back_buf = lax.dot_general(move, expert_out, (((0,), (0,)), ((), ())), preferred_element_type=F32).astype(BF)
    ret_buf = lax.all_to_all(back_buf, 'ep', 0, 0, tiled=True)
    mix_sum = gates[0] * dot(hits[0], ret_buf) + gates[1] * dot(hits[1], ret_buf)
    return (x_rows.astype(F32) + mix_sum).astype(BF)


def solution(mesh):
    n_ep = mesh.shape['ep']
    n_dp = mesh.shape['dp']
    row_spec = P(('dp', 'ep'), None)
    expert_spec = P('ep', None, None)

    def local_step(x_rows, logits, w_in, w_out):
        tok, d_model = x_rows.shape
        experts = logits.shape[1]
        exp_dev, _, ff = w_in.shape
        capacity = CAP_FACTOR * tok * n_ep // experts
        src_cap = 4 * tok // experts
        half = n_ep // 4
        packed = n_ep * (src_cap // DIRECT_PART) + 2 * (src_cap - src_cap // DIRECT_PART)
        vmem = pl.BlockSpec(memory_space=pltpu.VMEM)
        smem = pl.BlockSpec(memory_space=pltpu.SMEM)
        hbm = pl.BlockSpec(memory_space=pl.ANY)
        dma = pltpu.SemaphoreType.DMA
        out, flag = pl.pallas_call(
            functools.partial(moe_kernel, n_ep, n_dp, capacity, src_cap),
            out_shape=(jax.ShapeDtypeStruct((tok, d_model), BF), jax.ShapeDtypeStruct((1,), F32)),
            in_specs=[vmem, vmem, hbm, hbm],
            out_specs=(vmem, smem),
            scratch_shapes=[
                pltpu.VMEM((2, d_model, ff), BF),
                pltpu.VMEM((2, ff, d_model), BF),
                pltpu.VMEM((2, HOP_ROWS[0], d_model), BF),
                pltpu.VMEM((2 * tok, d_model), BF),
                *[pltpu.VMEM((4 * rows, d_model), BF) for rows in HOP_ROWS],
                pltpu.VMEM((2, 2, tok), F32),
                pltpu.VMEM((2, 2, tok), F32),
                pltpu.VMEM((2, half, 2, tok), F32),
                pltpu.VMEM((2, half, 2, tok), F32),
                pltpu.VMEM((1, 128), F32),
                pltpu.VMEM((n_ep, 1, 128), F32),
                pltpu.VMEM((exp_dev, capacity, d_model), F32),
                pltpu.VMEM((capacity, d_model), F32),
                pltpu.VMEM((exp_dev, capacity, 128), F32),
                pltpu.VMEM((8, capacity), F32),
                pltpu.VMEM((exp_dev, packed, d_model), BF),
                pltpu.VMEM((exp_dev, packed, d_model), BF),
                pltpu.VMEM((tok, d_model), F32),
                pltpu.VMEM((n_dp, 8, 128), F32),
                pltpu.VMEM((2 * exp_dev * capacity, d_model), BF),
                pltpu.VMEM((2, 2 * exp_dev, capacity), F32),
                pltpu.VMEM((2, RET_ROWS[0], d_model), BF),
                *[pltpu.VMEM((4 * rows, d_model), BF) for rows in RET_ROWS],
                pltpu.VMEM((2, 1, tok), F32),
                pltpu.VMEM((2, half, 1, tok), F32),
                pltpu.VMEM((2, half, 1, tok), F32),
                dma((2, 2)),
                dma((2, half, half)), dma((2, half, half)),
                dma((2, half)), dma((2, half)),
                dma((2,)),
                dma((2, half)), dma((2, half)), dma((2, half)), dma((2, half)),
                dma((2,)),
                dma((n_ep,)), dma((n_ep,)),
                dma((exp_dev, n_ep)), dma((exp_dev, n_ep)),
                dma((n_dp,)), dma((n_dp,)),
                dma((exp_dev, 2)), dma((exp_dev, 2)),
                dma((2, half, half)), dma((2, half, half)),
                dma((2, half, 2)), dma((2, half, 4)),
            ],
            compiler_params=pltpu.CompilerParams(
                collective_id=0, has_side_effects=True, vmem_limit_bytes=62 * 1024 * 1024),
            name='moe_layer',
        )(x_rows, logits.T, w_in, w_out)
        return lax.cond(flag[0] > 0.0, functools.partial(plain_step, n_ep), lambda *_: out, x_rows, logits, w_in, w_out)

    return jax.shard_map(local_step, mesh=mesh, in_specs=(row_spec, row_spec, expert_spec, expert_spec), out_specs=row_spec, check_vma=False)
```

```python
import functools

import jax
import jax.numpy as jnp
from jax import lax
from jax.experimental import pallas as pl
from jax.experimental.pallas import tpu as pltpu
from jax.sharding import PartitionSpec as P

CAP_FACTOR = 2
HOP_ROWS = (464, 384, 304, 160)
RET_ROWS = (272, 192, 128, 64)
FF_TILE = 512
BF = jnp.bfloat16
F32 = jnp.float32
MESH = pl.DeviceIdType.MESH


def top_two(vals, axis):
    best = jnp.max(vals, axis=axis, keepdims=True)
    first = vals == best
    rest = jnp.where(first, -jnp.inf, vals)
    runner = jnp.max(rest, axis=axis, keepdims=True)
    return best, runner, first, rest == runner


def as_one(mask):
    return jnp.where(mask, 1.0, 0.0)


def iota_f(shape, dim):
    return lax.broadcasted_iota(jnp.int32, shape, dim).astype(F32)


def dot(lhs, rhs):
    return jnp.dot(lhs, rhs, preferred_element_type=F32)


def moe_kernel(n_ep, n_dp, capacity, src_cap, x_ref, lg_ref, w1_hbm, w2_hbm, out_ref, flag_ref,
               w1_buf, w2_buf, blk, near, hops_a, hops_b, hops_c, hops_d, key_send, key_near, key_ring, key_mir,
               count_send, count_all, acc, z_acc, skey, rkeys, ret, back, y_acc, flag_buf,
               z_all, ov_place, ov_blk, ov_a, ov_b, ov_c, ov_d, okey_send, okey_ring, okey_mir,
               w_sem, send_sem, recv_sem, mir_send, mir_recv, px_sem, ksend_sem, krecv_sem, kmir_send, kmir_recv,
               kpx_sem, count_ssem, count_rsem, ret_ssem, ret_rsem, flag_ssem, flag_rsem, z_sem, extra_sem,
               osend_sem, orecv_sem, omir_sem, okey_sem):
    tok, d_model = x_ref.shape
    experts = lg_ref.shape[0]
    exp_dev = experts // n_ep
    ff = w1_buf.shape[2]
    n_chip = n_ep // 2
    half = n_chip // 2
    me = lax.axis_index('ep')
    my_dp = lax.axis_index('dp')
    chip = lax.div(me, 2)
    core = lax.rem(me, 2)
    other = chip * 2 + 1 - core
    nxt = (lax.rem(chip + 1, n_chip) * 2 + core, lax.rem(chip + n_chip - 1, n_chip) * 2 + core)
    bounds = (0,) + HOP_ROWS[::-1]
    hop_bufs = (hops_a, hops_b, hops_c, hops_d)
    ov_bufs = (ov_a, ov_b, ov_c, ov_d)
    ov_bounds = (0,) + RET_ROWS[::-1]
    direct = src_cap // 2
    packed = (n_ep + 2) * direct
    slots = exp_dev * capacity

    def weight_copies(el):
        slot = lax.rem(el, 2)
        return (pltpu.make_async_copy(w1_hbm.at[el], w1_buf.at[slot], w_sem.at[slot, 0]),
                pltpu.make_async_copy(w2_hbm.at[el], w2_buf.at[slot], w_sem.at[slot, 1]))

    for el in range(min(2, exp_dev)):
        for copy in weight_copies(el):
            copy.start()

    barrier = pltpu.get_barrier_semaphore()
    for step in range(1, n_ep):
        pl.semaphore_signal(barrier, inc=1, device_id={'ep': lax.rem(me + step, n_ep)}, device_id_type=MESH)
    for step in range(1, n_dp):
        pl.semaphore_signal(barrier, inc=1, device_id={'dp': lax.rem(my_dp + step, n_dp)}, device_id_type=MESH)

    logits_t = lg_ref[...]
    logits = logits_t.T
    _, _, first_t, second_t = top_two(logits_t, 0)
    row_i = lax.broadcasted_iota(jnp.int32, (tok, tok), 0)
    col_i = lax.broadcasted_iota(jnp.int32, (tok, tok), 1)
    upper = as_one(row_i < col_i).astype(BF)
    e_ids = iota_f((experts, tok), 0)
    ids = [jnp.sum(jnp.where(mask, e_ids, 0.0), axis=0, keepdims=True) for mask in (first_t, second_t)]
    chip_f = chip.astype(F32)
    base = me.astype(F32) * float(experts * src_cap)
    reach = [jnp.zeros((1, tok), F32), jnp.zeros((1, tok), F32)]
    opposite = jnp.zeros((1, tok), jnp.bool_)
    for expert_id in ids:
        delta = jnp.floor((expert_id + 0.5) * (1.0 / (2 * exp_dev))) - chip_f
        delta = jnp.where(delta < 0.0, delta + n_chip, delta)
        reach[0] = jnp.maximum(reach[0], jnp.where(delta < half, delta, 0.0))
        reach[1] = jnp.maximum(reach[1], jnp.where(delta > half, n_chip - delta, 0.0))
        opposite = opposite | (delta == half)
    odd = lax.rem(lax.broadcasted_iota(jnp.int32, (1, tok), 1) + core, 2) == 0
    forward = (reach[0] > reach[1]) | ((reach[0] == reach[1]) & odd)
    reach = [jnp.where(opposite & forward, float(half), reach[0]),
             jnp.where(opposite & jnp.logical_not(forward), float(half), reach[1])]

    zero_row = jnp.zeros((1, tok), F32)
    over = jnp.zeros((1, 1), F32)
    places = []
    for way in range(2):
        level = float(half) - iota_f((8, tok), 0)
        member = as_one((reach[way] == level) & (level > 0.5))
        inner = dot(member.astype(BF), upper)
        sizes = jnp.sum(member, axis=1, keepdims=True)
        place = zero_row - 1.0
        total = jnp.zeros((1, 1), F32)
        for lev in range(half):
            place = jnp.where(member[lev:lev + 1] > 0.5, inner[lev:lev + 1] + total, place)
            total = total + sizes[lev:lev + 1]
            over = jnp.maximum(over, as_one(total > float(bounds[lev + 1])))
        places.append(place)

    x_val = x_ref[...]

    def pick_rows(way, lo, size):
        return as_one(iota_f((size, tok), 0) + float(lo) == places[way]).astype(BF)

    def pack_rows(way, lo, size):
        blk[way, lo:lo + size, :] = dot(pick_rows(way, lo, size), x_val).astype(BF)

    lanes = 128
    chosen_t = as_one(first_t | second_t).astype(BF)
    tally = lax.dot_general(jnp.ones((8, tok), BF), chosen_t, (((1,), (1,)), ((), ())), preferred_element_type=F32)
    count_send[...] = jnp.concatenate([tally[0:1], jnp.zeros((1, lanes - experts), F32) + over], axis=1)
    count_all[me] = count_send[...]
    for way in range(2):
        pack_rows(way, 0, bounds[1])

    def remote(src, dst, send, recv, to):
        return pltpu.make_async_remote_copy(
            src_ref=src, dst_ref=dst, send_sem=send, recv_sem=recv, device_id=to, device_id_type=MESH)

    def count_copy(step):
        return remote(count_send, count_all.at[me], count_ssem.at[step], count_rsem.at[step],
                      {'ep': lax.rem(me + step, n_ep)})

    def ring_rows(way, hop, lo, size):
        return hop_bufs[hop].at[pl.ds(way * HOP_ROWS[hop] + lo, size)]

    def hop_copy(way, hop, part):
        lo, size = bounds[part], bounds[part + 1] - bounds[part]
        src = blk.at[way, pl.ds(lo, size)] if hop == 0 else ring_rows(way, hop - 1, lo, size)
        return remote(src, ring_rows(way, hop, lo, size), send_sem.at[way, hop, part], recv_sem.at[way, hop, part],
                      {'ep': nxt[way]})

    def key_copy(way, hop):
        src = key_send.at[way] if hop == 0 else key_ring.at[way, hop - 1]
        return remote(src, key_ring.at[way, hop], ksend_sem.at[way, hop], krecv_sem.at[way, hop], {'ep': nxt[way]})

    def mirror_copy(way, hop):
        return remote(ring_rows(way, hop, 0, HOP_ROWS[hop]), ring_rows(2 + way, hop, 0, HOP_ROWS[hop]),
                      mir_send.at[way, hop], mir_recv.at[way, hop], {'ep': other})

    def key_mirror(way, hop):
        return remote(key_ring.at[way, hop], key_mir.at[way, hop], kmir_send.at[way, hop], kmir_recv.at[way, hop],
                      {'ep': other})

    px_copy = remote(x_ref, near.at[pl.ds(tok, tok)], px_sem.at[0], px_sem.at[1], {'ep': other})
    kpx_copy = remote(key_near.at[0], key_near.at[1], kpx_sem.at[0], kpx_sem.at[1], {'ep': other})

    def parts_of(hop):
        return [p for p in range(half - hop) if bounds[p + 1] > bounds[p]]

    pl.semaphore_wait(barrier, n_ep - 1 + n_dp - 1)
    for step in range(1, n_ep):
        count_copy(step).start()
    for way in range(2):
        hop_copy(way, 0, 0).start()
    px_copy.start()
    rank_t = dot(chosen_t, upper)
    ranks = [jnp.sum(jnp.where(mask, rank_t, 0.0), axis=0, keepdims=True) for mask in (first_t, second_t)]
    info = jnp.concatenate([ids[0], ranks[0], ids[1], ranks[1], zero_row + 1.0, zero_row, zero_row, zero_row], axis=0).astype(BF)
    place_cols = jnp.concatenate(places + [zero_row] * 6, axis=0).T
    for way in range(2):
        pick_t = as_one(iota_f((tok, HOP_ROWS[0]), 1) == place_cols[:, way:way + 1]).astype(BF)
        keys = dot(info, pick_t)
        for c in range(2):
            key = base + keys[2 * c:2 * c + 1] * float(src_cap) + keys[2 * c + 1:2 * c + 2]
            key_send[way, c:c + 1, 0:HOP_ROWS[0]] = jnp.where(keys[4:5] > 0.5, key, -1.0)
        key_copy(way, 0).start()
    for c in range(2):
        key_near[0, c:c + 1, :] = base + ids[c] * float(src_cap) + ranks[c]
    kpx_copy.start()
    near[0:tok, :] = x_val
    for way in range(2):
        pack_rows(way, bounds[1], HOP_ROWS[0] - bounds[1])
    for part in parts_of(0)[1:]:
        for way in range(2):
            hop_copy(way, 0, part).start()

    best, runner, first, second = top_two(logits, 1)
    chosen = as_one(first | second)
    rank = dot(as_one(row_i > col_i).astype(BF), chosen.astype(BF))
    lane_e = iota_f((tok, experts), 1)
    norm = jnp.sum(jnp.exp(logits - best), axis=1, keepdims=True)
    gates = (1.0 / norm, jnp.exp(runner - best) / norm)
    tkeys = [jnp.sum(jnp.where(mask, lane_e * float(src_cap) + rank, 0.0), axis=1, keepdims=True) for mask in (first, second)]

    for step in range(1, n_ep):
        count_copy(step).wait_recv()
    count_rows = jnp.concatenate([count_all[s] for s in range(n_ep)], axis=0)
    counts = count_rows[:, 0:experts]
    over = jnp.max(jnp.max(count_rows[:, experts:lanes], axis=1, keepdims=True), axis=0, keepdims=True)
    tri = as_one(lax.broadcasted_iota(jnp.int32, (n_ep, n_ep), 1) <= lax.broadcasted_iota(jnp.int32, (n_ep, n_ep), 0)).astype(BF)
    ends = dot(tri, counts.astype(BF))
    lane_ep = lax.broadcasted_iota(jnp.int32, (n_ep, experts), 1)
    slot = iota_f((n_ep, capacity), 1)
    for el in range(exp_dev):
        mine = lane_ep == me * exp_dev + el
        count_col = jnp.sum(jnp.where(mine, counts, 0.0), axis=1, keepdims=True)
        end_col = jnp.sum(jnp.where(mine, ends, 0.0), axis=1, keepdims=True)
        past = as_one(end_col <= slot)
        src = jnp.sum(past, axis=0, keepdims=True)
        rnk = slot[0:1] - jnp.sum(past * count_col, axis=0, keepdims=True)
        valid = src < float(n_ep)
        e_base = (me * exp_dev + el).astype(F32) * float(src_cap)
        key = jnp.where(valid, src * float(experts * src_cap) + e_base + rnk, -2.0)
        skey[el] = jnp.broadcast_to(key, (128, capacity)).T
        beyond = jnp.where(src == me.astype(F32), 0.0, float(direct)) + float((n_ep - 1) * direct)
        home = (src == me.astype(F32)) | (src == other.astype(F32))
        spot = jnp.where(rnk < float(direct), src * float(direct) + rnk, jnp.where(home, beyond + rnk, -1.0))
        rkeys[el:el + 1, :] = jnp.where(valid, spot, -1.0)

    kept = jnp.clip(float(capacity) - (ends - counts), 0.0, counts)
    to_chip = as_one(jnp.floor((iota_f((experts, lanes), 0) + 0.5) * (1.0 / (2 * exp_dev))) == iota_f((experts, lanes), 1)).astype(BF)
    pooled = dot(jnp.maximum(kept - float(direct), 0.0).astype(BF), to_chip)

    def distances(src, origin):
        dest = jnp.floor((src + 0.5) * 0.5)
        delta = dest - origin
        delta = jnp.where(delta < 0.0, delta + n_chip, delta)
        at_half = delta == float(half)
        even = src == 2.0 * dest
        return (jnp.where((delta < half) | (at_half & even), delta, 0.0),
                jnp.where((delta > half) | (at_half & jnp.logical_not(even)), n_chip - delta, 0.0))

    for dist in distances(iota_f((n_ep, lanes), 0), iota_f((n_ep, lanes), 1)):
        for hop in range(half):
            load = jnp.sum(jnp.where(dist >= float(hop + 1), pooled, 0.0), axis=0, keepdims=True)
            over = jnp.maximum(over, jnp.max(as_one(load > float(2 * RET_ROWS[hop])), axis=1, keepdims=True))

    def plan_overflow():
        row_c = lax.broadcasted_iota(jnp.int32, (capacity, capacity), 0)
        col_c = lax.broadcasted_iota(jnp.int32, (capacity, capacity), 1)
        upper_c = as_one(row_c < col_c).astype(BF)
        infos, members = [], ([], [])
        level = float(half) - iota_f((8, capacity), 0)
        zero_c = jnp.zeros((1, capacity), F32)
        for b in range(2 * exp_dev):
            expert_id = chip * 2 * exp_dev + b
            mine = lane_ep == expert_id
            count_col = jnp.sum(jnp.where(mine, counts, 0.0), axis=1, keepdims=True)
            end_col = jnp.sum(jnp.where(mine, ends, 0.0), axis=1, keepdims=True)
            past = as_one(end_col <= slot)
            src = jnp.sum(past, axis=0, keepdims=True)
            rnk = slot[0:1] - jnp.sum(past * count_col, axis=0, keepdims=True)
            live = (src < float(n_ep)) & (rnk >= float(direct))
            infos.append(jnp.concatenate([src, zero_c + expert_id.astype(F32), rnk, zero_c + 1.0] + [zero_c] * 4, axis=0).astype(BF))
            for way, dist in enumerate(distances(src, chip_f)):
                members[way].append(as_one((jnp.where(live, dist, 0.0) == level) & (level > 0.5)))
        for way in range(2):
            inner = dot(jnp.concatenate(members[way], axis=0).astype(BF), upper_c)
            run = jnp.zeros((8, 1), F32)
            inners = []
            for b in range(2 * exp_dev):
                inners.append(inner[8 * b:8 * b + 8] + run)
                run = run + jnp.sum(members[way][b], axis=1, keepdims=True)
            for b in range(2 * exp_dev):
                place, total = zero_c - 1.0, jnp.zeros((1, 1), F32)
                for lev in range(half):
                    place = jnp.where(members[way][b][lev:lev + 1] > 0.5, inners[b][lev:lev + 1] + total, place)
                    total = total + run[lev:lev + 1]
                ov_place[way, b:b + 1, :] = place
            columns = ov_place[way].T
            keys = jnp.zeros((8, RET_ROWS[0]), F32)
            turn = 2.0 * iota_f((capacity, RET_ROWS[0]), 1) + core.astype(F32)
            for b in range(2 * exp_dev):
                keys = keys + dot(infos[b], as_one(turn == columns[:, b:b + 1]).astype(BF))
            key = keys[0:1] * float(experts * src_cap) + keys[1:2] * float(src_cap) + keys[2:3]
            okey_send[way, 0:1, 0:RET_ROWS[0]] = jnp.where(keys[3:4] > 0.5, key, -1.0)

    def ov_rows(way, hop, lo, size):
        return ov_bufs[hop].at[pl.ds(way * RET_ROWS[hop] + lo, size)]

    def ov_copy(way, hop, part):
        lo, size = ov_bounds[part], ov_bounds[part + 1] - ov_bounds[part]
        src = ov_blk.at[way, pl.ds(lo, size)] if hop == 0 else ov_rows(way, hop - 1, lo, size)
        return remote(src, ov_rows(way, hop, lo, size), osend_sem.at[way, hop, part], orecv_sem.at[way, hop, part],
                      {'ep': nxt[way]})

    def okey_copy(way, hop):
        src = okey_send.at[way] if hop == 0 else okey_ring.at[way, hop - 1]
        return remote(src, okey_ring.at[way, hop], okey_sem.at[way, hop, 0], okey_sem.at[way, hop, 1], {'ep': nxt[way]})

    def ov_mirror(way, hop):
        return remote(ov_rows(way, hop, 0, RET_ROWS[hop]), ov_rows(2 + way, hop, 0, RET_ROWS[hop]),
                      omir_sem.at[way, hop, 0], omir_sem.at[way, hop, 1], {'ep': other})

    def okey_mirror(way, hop):
        return remote(okey_ring.at[way, hop], okey_mir.at[way, hop], okey_sem.at[way, hop, 2], okey_sem.at[way, hop, 3],
                      {'ep': other})

    def ov_parts(hop):
        return list(range(half - hop))

    def gather_rows(el, buf, keys, first_time=False):
        want = skey[el][:, 0:1]
        hit = as_one((want == keys[0:1]) | (want == keys[1:2])).astype(BF)
        part = dot(hit, buf[...])
        return part if first_time else acc[el] + part

    def gather_all(buf, keys, first_time=False):
        def body(el, carry):
            acc[el] = gather_rows(el, buf, keys, first_time)
            return carry
        lax.fori_loop(0, exp_dev, body, 0)

    def hop_keys(hop):
        for way in range(2):
            mirror_copy(way, hop).wait_recv()
            key_mirror(way, hop).wait_recv()
        size = HOP_ROWS[hop]
        return jnp.concatenate([keys[way, hop][:, 0:size] for keys in (key_ring, key_mir) for way in range(2)], axis=1)

    px_copy.wait_recv()
    kpx_copy.wait_recv()

    late = (near, jnp.concatenate([key_near[0], key_near[1]], axis=1), True)
    for hop in range(half):
        for part in parts_of(hop):
            if hop == 1 and part == parts_of(1)[-1]:
                plan_overflow()
            if part == 1 and late is not None:
                gather_all(*late)
                late = None
            for way in range(2):
                hop_copy(way, hop, part).wait_recv()
                onward = hop + 1 < half
                if onward and part in parts_of(hop + 1):
                    hop_copy(way, hop + 1, part).start()
                if part == 0:
                    key_copy(way, hop).wait_recv()
                    key_mirror(way, hop).start()
                    if onward:
                        key_copy(way, hop + 1).start()
        for way in range(2):
            mirror_copy(way, hop).start()
        if hop + 1 < half:
            late = (hop_bufs[hop], hop_keys(hop))
            if hop + 2 == half:
                gather_all(*late)
                late = None
    last_keys = hop_keys(half - 1)

    flag_buf[0] = jnp.broadcast_to(over, (8, 128))

    def flag_copy(step):
        return pltpu.make_async_remote_copy(
            src_ref=flag_buf.at[0], dst_ref=flag_buf.at[step], send_sem=flag_ssem.at[step], recv_sem=flag_rsem.at[step],
            device_id={'dp': lax.rem(my_dp + step, n_dp)}, device_id_type=MESH)

    for step in range(1, n_dp):
        flag_copy(step).start()

    def ret_copy(el, step):
        dest = lax.rem(me + step, n_ep)
        return pltpu.make_async_remote_copy(
            src_ref=ret.at[el, pl.ds(pl.multiple_of(dest * direct, direct), direct)],
            dst_ref=back.at[el, pl.ds(pl.multiple_of(me * direct, direct), direct)],
            send_sem=ret_ssem.at[el, step], recv_sem=ret_rsem.at[el, step],
            device_id={'ep': dest}, device_id_type=MESH)

    def extra_copy(el):
        rows = pl.ds(packed - direct, direct)
        return remote(ret.at[el, rows], back.at[el, rows], extra_sem.at[el, 0], extra_sem.at[el, 1], {'ep': other})

    def z_copy(el):
        rows = pl.ds(pl.multiple_of(core * slots + el * capacity, capacity), capacity)
        return remote(z_all.at[rows], z_all.at[rows], z_sem.at[el, 0], z_sem.at[el, 1], {'ep': other})

    def z_arrival(el):
        rows = pl.ds(pl.multiple_of((1 - core) * slots + el * capacity, capacity), capacity)
        return remote(z_all.at[rows], z_all.at[rows], z_sem.at[el, 0], z_sem.at[el, 1], {'ep': other})

    ret_order = sorted(range(1, n_ep), key=lambda s: -min(s, n_ep - s))

    def expert_body(el, carry):
        spot = lax.rem(el, 2)
        for copy in weight_copies(el):
            copy.wait()
        rows = gather_rows(el, hop_bufs[half - 1], last_keys).astype(BF)
        z_acc[...] = jnp.zeros_like(z_acc)

        def ff_body(tile, inner):
            cols = pl.ds(pl.multiple_of(tile * FF_TILE, FF_TILE), FF_TILE)
            hidden = jax.nn.gelu(dot(rows, w1_buf[spot, :, cols]), approximate=True).astype(BF)
            z_acc[...] += dot(hidden, w2_buf[spot, cols, :])
            return inner

        lax.fori_loop(0, ff // FF_TILE, ff_body, 0)

        @pl.when(el + 2 < exp_dev)
        def _():
            for copy in weight_copies(el + 2):
                copy.start()

        spread = as_one(iota_f((packed, capacity), 0) == rkeys[pl.ds(el, 1), :]).astype(BF)
        z_rows = z_acc[...].astype(BF)
        z_all[pl.ds(pl.multiple_of(core * slots + el * capacity, capacity), capacity), :] = z_rows
        ret[el] = dot(spread, z_rows).astype(BF)
        for step in ret_order:
            ret_copy(el, step).start()
        extra_copy(el).start()
        z_copy(el).start()
        own = pl.ds(pl.multiple_of(me * direct, direct), direct)
        back[el, own, :] = ret[el, own, :]
        back[el, n_ep * direct:(n_ep + 1) * direct, :] = ret[el, n_ep * direct:(n_ep + 1) * direct, :]
        return carry

    lax.fori_loop(0, exp_dev, expert_body, 0)

    for el in range(exp_dev):
        z_arrival(el).wait_recv()
    turn = 2.0 * iota_f((RET_ROWS[0], capacity), 0) + core.astype(F32)
    for way in range(2):
        take = jnp.concatenate([as_one(turn == ov_place[way, b:b + 1, :]).astype(BF) for b in range(2 * exp_dev)], axis=1)
        ov_blk[way] = dot(take, z_all[...]).astype(BF)
    for way in range(2):
        ov_copy(way, 0, 0).start()
        okey_copy(way, 0).start()
    for part in ov_parts(0)[1:]:
        for way in range(2):
            ov_copy(way, 0, part).start()

    slot_i = lax.broadcasted_iota(jnp.int32, (1, packed), 1)
    slot_src = lax.div(slot_i, direct)
    slot_rank = slot_i - slot_src * direct
    slot_rank = jnp.where(slot_src < n_ep, slot_rank, slot_rank + direct)
    slot_src = jnp.where(slot_src < n_ep, slot_src, jnp.where(slot_src == n_ep, me, other))
    y_acc[...] = jnp.zeros_like(y_acc)

    def mix_body(el, carry):
        for step in ret_order:
            ret_copy(el, step).wait_recv()
        extra_copy(el).wait_recv()
        slot_key = ((slot_src * exp_dev + el) * src_cap + slot_rank).astype(F32)
        for c in range(2):
            hit = as_one(tkeys[c] == slot_key).astype(BF)
            y_acc[...] += gates[c] * dot(hit, back[el])
        return carry

    lax.fori_loop(0, exp_dev, mix_body, 0)

    def mix_overflow(hop):
        for way in range(2):
            ov_mirror(way, hop).wait_recv()
            okey_mirror(way, hop).wait_recv()
        size = RET_ROWS[hop]
        keys = jnp.concatenate([buf[way, hop][:, 0:size] for buf in (okey_ring, okey_mir) for way in range(2)], axis=1)
        for c in range(2):
            hit = as_one(base + tkeys[c] == keys).astype(BF)
            y_acc[...] += gates[c] * dot(hit, ov_bufs[hop][...])

    for hop in range(half):
        onward = hop + 1 < half
        for part in ov_parts(hop):
            for way in range(2):
                ov_copy(way, hop, part).wait_recv()
                if onward and part in ov_parts(hop + 1):
                    ov_copy(way, hop + 1, part).start()
                if part == 0:
                    okey_copy(way, hop).wait_recv()
                    okey_mirror(way, hop).start()
                    if onward:
                        okey_copy(way, hop + 1).start()
            if part == 0 and hop > 0 and onward:
                mix_overflow(hop - 1)
        for way in range(2):
            ov_mirror(way, hop).start()
        if not onward:
            mix_overflow(hop - 1)
    mix_overflow(half - 1)
    out_ref[...] = (x_ref[...].astype(F32) + y_acc[...]).astype(BF)

    worst = flag_buf[0]
    for step in range(1, n_dp):
        flag_copy(step).wait_recv()
        worst = jnp.maximum(worst, flag_buf[step])
    flag_ref[0] = jnp.max(worst)

    px_copy.wait_send()
    kpx_copy.wait_send()
    for step in range(1, n_ep):
        count_copy(step).wait_send()
    for step in range(1, n_dp):
        flag_copy(step).wait_send()
    for hop in range(half):
        for way in range(2):
            mirror_copy(way, hop).wait_send()
            key_mirror(way, hop).wait_send()
            key_copy(way, hop).wait_send()
            for part in parts_of(hop):
                hop_copy(way, hop, part).wait_send()
    for el in range(exp_dev):
        extra_copy(el).wait_send()
        z_copy(el).wait_send()
        for step in ret_order:
            ret_copy(el, step).wait_send()
    for hop in range(half):
        for way in range(2):
            ov_mirror(way, hop).wait_send()
            okey_mirror(way, hop).wait_send()
            okey_copy(way, hop).wait_send()
            for part in ov_parts(hop):
                ov_copy(way, hop, part).wait_send()


def plain_step(n_ep, x_rows, logits, w_in, w_out):
    tok, d_model = x_rows.shape
    experts = logits.shape[1]
    exp_dev = w_in.shape[0]
    capacity = CAP_FACTOR * tok * n_ep // experts
    src_cap = 4 * tok // experts
    me = lax.axis_index('ep')
    best, runner, first, second = top_two(logits, 1)
    norm = jnp.sum(jnp.exp(logits - best), axis=1, keepdims=True)
    gates = (1.0 / norm, jnp.exp(runner - best) / norm)
    chosen = as_one(first | second)
    lower = as_one(iota_f((tok, tok), 0) > iota_f((tok, tok), 1)).astype(BF)
    rank = dot(lower, chosen.astype(BF))
    counts = lax.all_gather(jnp.sum(chosen, axis=0), 'ep')
    tri = as_one(iota_f((n_ep, n_ep), 0) > iota_f((n_ep, n_ep), 1)).astype(BF)
    before = dot(tri, counts.astype(BF))
    mine = jnp.sum(jnp.where(iota_f((n_ep, experts), 0) == me.astype(F32), before, 0.0), axis=0, keepdims=True)
    slot_of = jnp.where(rank + mine < capacity, iota_f((tok, experts), 1) * src_cap + rank, -1.0)
    rows = [jnp.sum(jnp.where(mask, slot_of, 0.0), axis=1, keepdims=True) for mask in (first, second)]
    slots = iota_f((tok, experts * src_cap), 1)
    hits = [as_one(row == slots).astype(BF) for row in rows]
    send_buf = lax.dot_general(hits[0] + hits[1], x_rows, (((0,), (0,)), ((), ())), preferred_element_type=F32).astype(BF)
    recv_buf = lax.all_to_all(send_buf, 'ep', 0, 0, tiled=True)
    own = lax.dynamic_slice_in_dim(jnp.stack([before, counts]), me * exp_dev, exp_dev, axis=2)
    start = jnp.transpose(own[0])[:, :, None]
    size = jnp.transpose(own[1])[:, :, None]
    order = jnp.arange(src_cap, dtype=F32)[None, None, :]
    place = jnp.where((order < size) & (start + order < capacity), start + order, -1.0)
    place = jnp.where(place >= 0.0, place + capacity * jnp.arange(exp_dev, dtype=F32)[:, None, None], -1.0)
    place = jnp.transpose(place, (1, 0, 2)).reshape(1, experts * src_cap)
    move = as_one(iota_f((exp_dev * capacity, experts * src_cap), 0) == place).astype(BF)
    expert_rows = dot(move, recv_buf).astype(BF).reshape(exp_dev, capacity, d_model)
    hidden = jax.nn.gelu(jnp.einsum('ecd,edf->ecf', expert_rows, w_in, preferred_element_type=F32), approximate=True).astype(BF)
    expert_out = jnp.einsum('ecf,efd->ecd', hidden, w_out, preferred_element_type=F32).astype(BF).reshape(exp_dev * capacity, d_model)
    back_buf = lax.dot_general(move, expert_out, (((0,), (0,)), ((), ())), preferred_element_type=F32).astype(BF)
    ret_buf = lax.all_to_all(back_buf, 'ep', 0, 0, tiled=True)
    mix_sum = gates[0] * dot(hits[0], ret_buf) + gates[1] * dot(hits[1], ret_buf)
    return (x_rows.astype(F32) + mix_sum).astype(BF)


def solution(mesh):
    n_ep = mesh.shape['ep']
    n_dp = mesh.shape['dp']
    row_spec = P(('dp', 'ep'), None)
    expert_spec = P('ep', None, None)

    def local_step(x_rows, logits, w_in, w_out):
        tok, d_model = x_rows.shape
        experts = logits.shape[1]
        exp_dev, _, ff = w_in.shape
        capacity = CAP_FACTOR * tok * n_ep // experts
        src_cap = 4 * tok // experts
        half = n_ep // 4
        packed = (n_ep + 2) * (src_cap // 2)
        vmem = pl.BlockSpec(memory_space=pltpu.VMEM)
        smem = pl.BlockSpec(memory_space=pltpu.SMEM)
        hbm = pl.BlockSpec(memory_space=pl.ANY)
        dma = pltpu.SemaphoreType.DMA
        out, flag = pl.pallas_call(
            functools.partial(moe_kernel, n_ep, n_dp, capacity, src_cap),
            out_shape=(jax.ShapeDtypeStruct((tok, d_model), BF), jax.ShapeDtypeStruct((1,), F32)),
            in_specs=[vmem, vmem, hbm, hbm],
            out_specs=(vmem, smem),
            scratch_shapes=[
                pltpu.VMEM((2, d_model, ff), BF),
                pltpu.VMEM((2, ff, d_model), BF),
                pltpu.VMEM((2, HOP_ROWS[0], d_model), BF),
                pltpu.VMEM((2 * tok, d_model), BF),
                *[pltpu.VMEM((4 * rows, d_model), BF) for rows in HOP_ROWS],
                pltpu.VMEM((2, 2, tok), F32),
                pltpu.VMEM((2, 2, tok), F32),
                pltpu.VMEM((2, half, 2, tok), F32),
                pltpu.VMEM((2, half, 2, tok), F32),
                pltpu.VMEM((1, 128), F32),
                pltpu.VMEM((n_ep, 1, 128), F32),
                pltpu.VMEM((exp_dev, capacity, d_model), F32),
                pltpu.VMEM((capacity, d_model), F32),
                pltpu.VMEM((exp_dev, capacity, 128), F32),
                pltpu.VMEM((8, capacity), F32),
                pltpu.VMEM((exp_dev, packed, d_model), BF),
                pltpu.VMEM((exp_dev, packed, d_model), BF),
                pltpu.VMEM((tok, d_model), F32),
                pltpu.VMEM((n_dp, 8, 128), F32),
                pltpu.VMEM((2 * exp_dev * capacity, d_model), BF),
                pltpu.VMEM((2, 2 * exp_dev, capacity), F32),
                pltpu.VMEM((2, RET_ROWS[0], d_model), BF),
                *[pltpu.VMEM((4 * rows, d_model), BF) for rows in RET_ROWS],
                pltpu.VMEM((2, 1, tok), F32),
                pltpu.VMEM((2, half, 1, tok), F32),
                pltpu.VMEM((2, half, 1, tok), F32),
                dma((2, 2)),
                dma((2, half, half)), dma((2, half, half)),
                dma((2, half)), dma((2, half)),
                dma((2,)),
                dma((2, half)), dma((2, half)), dma((2, half)), dma((2, half)),
                dma((2,)),
                dma((n_ep,)), dma((n_ep,)),
                dma((exp_dev, n_ep)), dma((exp_dev, n_ep)),
                dma((n_dp,)), dma((n_dp,)),
                dma((exp_dev, 2)), dma((exp_dev, 2)),
                dma((2, half, half)), dma((2, half, half)),
                dma((2, half, 2)), dma((2, half, 4)),
            ],
            compiler_params=pltpu.CompilerParams(
                collective_id=0, has_side_effects=True, vmem_limit_bytes=62 * 1024 * 1024),
            name='moe_layer',
        )(x_rows, logits.T, w_in, w_out)
        return lax.cond(flag[0] > 0.0, functools.partial(plain_step, n_ep), lambda *_: out, x_rows, logits, w_in, w_out)

    return jax.shard_map(local_step, mesh=mesh, in_specs=(row_spec, row_spec, expert_spec, expert_spec), out_specs=row_spec, check_vma=False)
```
